32 devices in a mesh: chord: 4 (over z), span: 8 (over y, x, core).
Axes of the slice: x: 2, y: 2, z: 4, core: 2. Of those that a mesh axis runs over, the one named last changes fastest.
Arguments:
- state: float32 [5, 125, 16, 16, 128], P(None, None, 'chord', 'span'), may hold values from -10 to 10
Outputs:
- residual: float32 [5, 125, 16, 16, 128], P(None, None, 'chord', 'span')
- viscosity: float32 [125, 16, 16, 128], P(None, 'chord', 'span')
The draws below stay inside these ranges and needn't reach their ends.
All inputs are finite; a program needn't handle non-finite values.
Results may differ from the reference program's by a relative error of at most 0.0001.
Values sent between devices are 32-bit elements; how exact they have to be, the bound alone decides.
A program may use at most 128 MiB of HBM per device.

```python
import math
import jax
import jax.numpy as jnp
import numpy as np
from jax import lax

NVAR = 5
NPTS = 125
NORMAL_ELEMENTS = 128
CHORD_ELEMENTS = 16
SPAN_ELEMENTS = 16


def draw_state(key, part):
    element_lattice = (CHORD_ELEMENTS, SPAN_ELEMENTS, NORMAL_ELEMENTS)
    variable = jnp.arange(NVAR).reshape(NVAR, 1, 1, 1, 1)
    level_base = jax.random.normal(jax.random.fold_in(key, 1), (NVAR, 1) + element_lattice, jnp.float32)
    density_base = jax.random.uniform(jax.random.fold_in(key, 2), (NVAR, 1) + element_lattice, jnp.float32, 0.5, 1.5)
    base = jnp.where(variable == 0, density_base, level_base)
    log_amp = jax.random.uniform(jax.random.fold_in(key, 3), (NVAR, 1) + element_lattice, jnp.float32, math.log(0.001), math.log(1.0))
    noise = jax.random.normal(jax.random.fold_in(key, 4), (NVAR, NPTS) + element_lattice, jnp.float32)
    return jnp.clip(base + jnp.exp(log_amp) * noise, -10.0, 10.0)


def setup_inputs(seed: int = 0) -> dict:
    key_of = jax.random.split(jax.random.key(seed), 2)
    return {
        "state": draw_state(jax.random.fold_in(key_of[1], 71), 0),
    }


EPS_SCALE = 0.01
SENSOR_CENTRE = -3.0
SENSOR_WIDTH = 1.5
RATIO_FLOOR = 1e-06
ENERGY_EPS = 1e-06
GAUSS_NODES = [-0.906179845938664, -0.5384693101056831, 0.0, 0.5384693101056831, 0.906179845938664]
GAUSS_WEIGHTS = [0.2369268850561891, 0.4786286704993665, 0.5688888888888889, 0.4786286704993665, 0.2369268850561891]

def legendre_values(points):
    values = [np.ones(points.shape), np.array(points)]
    for order in range(1, 5):
        values.append(((2 * order + 1) * points * values[order] - order * values[order - 1]) / (order + 1))
    return values

def line_tables():
    line_nodes = np.array(GAUSS_NODES)
    quadrature_weights = np.array(GAUSS_WEIGHTS)
    barycentric = np.array([1.0 / np.prod([line_nodes[j] - line_nodes[k] for k in range(5) if k != j]) for j in range(5)])
    derivative = np.zeros((5, 5))
    for i in range(5):
        for j in range(5):
            if i != j:
                derivative[i, j] = barycentric[j] / barycentric[i] / (line_nodes[i] - line_nodes[j])
        derivative[i, i] = -np.sum(derivative[i])
    left_values = np.ones(5)
    right_values = np.ones(5)
    for j in range(5):
        for k in range(5):
            if k != j:
                left_values[j] *= (-1.0 - line_nodes[k]) / (line_nodes[j] - line_nodes[k])
                right_values[j] *= (1.0 - line_nodes[k]) / (line_nodes[j] - line_nodes[k])
    legendre = legendre_values(line_nodes)
    fourth_slope = 7.0 * legendre[3] + 3.0 * legendre[1]
    fifth_slope = 9.0 * legendre[4] + 5.0 * legendre[2] + legendre[0]
    left_corr = 0.5 * (fourth_slope - fifth_slope)
    right_corr = 0.5 * (fourth_slope + fifth_slope)
    modal = np.zeros((5, 5))
    for k in range(5):
        modal[k, :] = quadrature_weights * math.sqrt((2 * k + 1) / 2.0) * legendre[k]
    return (line_nodes, derivative, left_values, right_values, left_corr, right_corr, modal)

def along_axis(operator_matrix, axis):
    factors = [np.eye(5), np.eye(5), np.eye(5)]
    factors[axis] = operator_matrix
    return np.kron(np.kron(factors[0], factors[1]), factors[2])

def build_tables():
    line_nodes, derivative, left_values, right_values, left_corr, right_corr, modal = line_tables()
    operators = []
    for axis in range(3):
        group = (along_axis(derivative, axis), along_axis(left_values[None, :], axis), along_axis(right_values[None, :], axis), along_axis(left_corr[:, None], axis), along_axis(right_corr[:, None], axis))
        operators.append(tuple((jnp.asarray(entry, dtype=jnp.float32) for entry in group)))
    modal_3d = jnp.asarray(np.kron(np.kron(modal, modal), modal), dtype=jnp.float32)
    point_index = np.arange(125)
    high_np = np.where((point_index // 25 == 4) | (point_index // 5 % 5 == 4) | (point_index % 5 == 4), 1.0, 0.0)
    high_mask = jnp.asarray(high_np, dtype=jnp.float32)
    halves = [(1.0 - line_nodes) / 2.0, (1.0 + line_nodes) / 2.0]
    trilinear_np = np.zeros((125, 8))
    for corner in range(8):
        trilinear_np[:, corner] = np.kron(np.kron(halves[corner // 4], halves[corner // 2 % 2]), halves[corner % 2])
    trilinear = jnp.asarray(trilinear_np, dtype=jnp.float32)
    return (operators, modal_3d, high_mask, trilinear)

def single_points(operator_matrix, field):
    return jnp.einsum('qp,pxyz->qxyz', operator_matrix, field, precision=lax.Precision.HIGHEST)

def sensor_viscosity(density, modal_3d, high_mask):
    coeffs = single_points(modal_3d, density)
    energy = coeffs * coeffs
    high_part = lax.optimization_barrier(jnp.sum(energy * high_mask[:, None, None, None], axis=0))
    total = lax.optimization_barrier(jnp.sum(energy, axis=0)) + ENERGY_EPS
    level = jnp.log10(jnp.maximum(high_part / total, RATIO_FLOOR))
    ramp = jnp.clip((level - SENSOR_CENTRE) / SENSOR_WIDTH, -1.0, 1.0)
    return EPS_SCALE * 0.5 * (1.0 + jnp.sin(0.5 * math.pi * ramp))

def boundary_masks(length, dim, rank, is_first, is_last):
    shape = [1] * rank
    shape[dim] = length
    place = lax.broadcasted_iota(jnp.int32, tuple(shape), dim)
    lower_open = jnp.logical_or(place > 0, jnp.logical_not(is_first))
    upper_open = jnp.logical_or(place < length - 1, jnp.logical_not(is_last))
    return (lower_open.astype(jnp.float32), upper_open.astype(jnp.float32))

def variable_residual(field, viscosity, operators):
    total = jnp.zeros_like(field)
    for axis in range(3):
        derivative, to_left, to_right, lift_left, lift_right = operators[axis]
        dim = axis + 1
        closed = axis != 1
        lower_open, upper_open = boundary_masks(field.shape[dim], dim, 4, closed, closed)
        left_tr = single_points(to_left, field)
        right_tr = single_points(to_right, field)
        prev_right = jnp.roll(right_tr, 1, axis=dim)
        following_left = jnp.roll(left_tr, -1, axis=dim)
        gradient = single_points(derivative, field) + single_points(lift_left, 0.5 * (prev_right - left_tr) * lower_open) + single_points(lift_right, 0.5 * (following_left - right_tr) * upper_open)
        flux = viscosity * gradient
        flux_left = single_points(to_left, flux)
        flux_right = single_points(to_right, flux)
        flux_prev = jnp.roll(flux_right, 1, axis=dim)
        flux_next = jnp.roll(flux_left, -1, axis=dim)
        total = total + single_points(derivative, flux) + single_points(lift_left, 0.5 * (flux_prev + flux_left) * lower_open - flux_left) + single_points(lift_right, 0.5 * (flux_next + flux_right) * upper_open - flux_right)
    return total

def reference(state):
    operators, modal_3d, high_mask, trilinear = build_tables()
    element_eps = sensor_viscosity(state[0], modal_3d, high_mask)
    padded = jnp.pad(element_eps, ((1, 1), (0, 0), (1, 1)))
    along_chord = jnp.maximum(padded[:-1], padded[1:])
    along_span = jnp.maximum(along_chord, jnp.roll(along_chord, 1, axis=1))
    vertex = jnp.maximum(along_span[:, :, :-1], along_span[:, :, 1:])
    shifted = jnp.roll(vertex, -1, axis=1)
    chord_count = element_eps.shape[0]
    normal_count = element_eps.shape[2]
    corner_list = []
    for corner in range(8):
        step_x = corner // 4
        step_y = corner // 2 % 2
        step_z = corner % 2
        source = shifted if step_y == 1 else vertex
        corner_list.append(source[step_x:step_x + chord_count, :, step_z:step_z + normal_count])
    corners = jnp.stack(corner_list, axis=0)
    viscosity = jnp.einsum('qc,cxyz->qxyz', trilinear, corners, precision=lax.Precision.HIGHEST)

    def one_variable(field):
        return variable_residual(field, viscosity, operators)
    residual = lax.map(one_variable, state)
    return (residual, viscosity)
```

```python
import functools
import math

import jax
import jax.numpy as jnp
import numpy as np
from jax import lax
from jax.experimental import pallas as pl
from jax.experimental.pallas import tpu as pltpu
from jax.sharding import PartitionSpec as P

VMEM_BYTES = 52_500_000
FINISH_BYTES = 8_000_000
EPS_SCALE = 0.01
SENSOR_CENTRE = -3.0
SENSOR_WIDTH = 1.5
RATIO_FLOOR = 1e-06
ENERGY_EPS = 1e-06
GAUSS_NODES = [-0.906179845938664, -0.5384693101056831, 0.0, 0.5384693101056831, 0.906179845938664]
GAUSS_WEIGHTS = [
    0.2369268850561891,
    0.4786286704993665,
    0.5688888888888889,
    0.4786286704993665,
    0.2369268850561891,
]


def legendre_values(points):
    values = [np.ones(points.shape), np.array(points)]
    for order in range(1, 5):
        values.append(
            ((2 * order + 1) * points * values[order] - order * values[order - 1]) / (order + 1)
        )
    return values


def line_tables():
    line_nodes = np.array(GAUSS_NODES)
    quadrature_weights = np.array(GAUSS_WEIGHTS)
    barycentric = np.array(
        [
            1.0 / np.prod([line_nodes[j] - line_nodes[k] for k in range(5) if k != j])
            for j in range(5)
        ]
    )
    derivative = np.zeros((5, 5))
    for i in range(5):
        for j in range(5):
            if i != j:
                derivative[i, j] = barycentric[j] / barycentric[i] / (line_nodes[i] - line_nodes[j])
        derivative[i, i] = -np.sum(derivative[i])
    left_values = np.ones(5)
    right_values = np.ones(5)
    for j in range(5):
        for k in range(5):
            if k != j:
                left_values[j] *= (-1.0 - line_nodes[k]) / (line_nodes[j] - line_nodes[k])
                right_values[j] *= (1.0 - line_nodes[k]) / (line_nodes[j] - line_nodes[k])
    legendre = legendre_values(line_nodes)
    fourth_slope = 7.0 * legendre[3] + 3.0 * legendre[1]
    fifth_slope = 9.0 * legendre[4] + 5.0 * legendre[2] + legendre[0]
    left_corr = 0.5 * (fourth_slope - fifth_slope)
    right_corr = 0.5 * (fourth_slope + fifth_slope)
    modal = np.zeros((5, 5))
    for k in range(5):
        modal[k, :] = quadrature_weights * math.sqrt((2 * k + 1) / 2.0) * legendre[k]
    return (line_nodes, derivative, left_values, right_values, left_corr, right_corr, modal)


NODES, DERIV, LEFT, RIGHT, LIFT_LEFT, LIFT_RIGHT, MODAL = line_tables()
HALF_LEFT = 0.5 * LIFT_LEFT
HALF_RIGHT = 0.5 * LIFT_RIGHT


def fold(u):
    return (u[0] + u[4], u[1] + u[3], u[2], u[0] - u[4], u[1] - u[3])


def traces(parts):
    s0, s1, mid, d0, d1 = parts
    r = [float(x) for x in RIGHT]
    even = 0.5 * (r[0] + r[4]) * s0 + 0.5 * (r[1] + r[3]) * s1 + r[2] * mid
    odd = 0.5 * (r[0] - r[4]) * d0 + 0.5 * (r[1] - r[3]) * d1
    return even - odd, even + odd


def slope(parts, before, after):
    s0, s1, mid, d0, d1 = parts
    h = [float(x) for x in HALF_LEFT]
    r = [float(x) for x in RIGHT]
    if before is not None:
        diff, both = before - after, before + after
    even, odd = [], []
    for i in range(3):
        lift = 0.5 * (h[i] + h[4 - i])
        value = (
            float(0.5 * (DERIV[i, 0] - DERIV[i, 4]) + lift * (r[0] - r[4])) * d0
            + float(0.5 * (DERIV[i, 1] - DERIV[i, 3]) + lift * (r[1] - r[3])) * d1
        )
        even.append(value if before is None else value + lift * diff)
    for i in range(2):
        lift = 0.5 * (h[i] - h[4 - i])
        value = (
            float(0.5 * (DERIV[i, 0] + DERIV[i, 4]) - lift * (r[0] + r[4])) * s0
            + float(0.5 * (DERIV[i, 1] + DERIV[i, 3]) - lift * (r[1] + r[3])) * s1
            + float(DERIV[i, 2] - 2.0 * lift * r[2]) * mid
        )
        odd.append(value if before is None else value + lift * both)
    return [even[0] + odd[0], even[1] + odd[1], even[2], even[1] - odd[1], even[0] - odd[0]]


def points(axis, q, j):
    if axis == 0:
        return [25 * i + 5 * q + j for i in range(5)]
    if axis == 1:
        return [25 * q + 5 * i + j for i in range(5)]
    return [25 * q + 5 * j + i for i in range(5)]


def modal_line(u):
    s0, s1, mid, d0, d1 = fold(u)
    out = []
    for k in range(5):
        m = [float(x) for x in MODAL[k]]
        out.append(m[0] * s0 + m[1] * s1 + m[2] * mid if k % 2 == 0 else m[0] * d0 + m[1] * d1)
    return out


def sensor(load, work):
    def first(q, carry):
        for j in range(5):
            pts = points(0, q, j)
            for i, value in zip(pts, modal_line([load(p) for p in pts])):
                work[i] = value
        return carry

    lax.fori_loop(0, 5, first, 0)

    def second(q, carry):
        total, high = carry
        plane = {}
        for c in range(5):
            for b, value in enumerate(modal_line([work[25 * q + 5 * b + c] for b in range(5)])):
                plane[b, c] = value
        low = jnp.zeros_like(total)
        edge = jnp.zeros_like(total)
        for b in range(5):
            line = modal_line([plane[b, c] for c in range(5)])
            squares = [x * x for x in line]
            if b < 4:
                low = low + ((squares[0] + squares[1]) + (squares[2] + squares[3]))
                edge = edge + squares[4]
            else:
                edge = edge + ((squares[0] + squares[1]) + (squares[2] + squares[3])) + squares[4]
        plane_total = low + edge
        return total + plane_total, high + jnp.where(q == 4, plane_total, edge)

    zero = jnp.zeros(work.shape[1:], jnp.float32)
    total, high = lax.fori_loop(0, 5, second, (zero, zero))
    level = jnp.log(jnp.maximum(high / (total + ENERGY_EPS), RATIO_FLOOR)) * (1.0 / math.log(10.0))
    ramp = jnp.clip((level - SENSOR_CENTRE) / SENSOR_WIDTH, -1.0, 1.0)
    return EPS_SCALE * 0.5 * (1.0 + jnp.sin(0.5 * math.pi * ramp))


def rolled(value, shift, axis):
    size = value.shape[axis]
    return pltpu.roll(value, shift % size, axis)


LOWER = [float((1.0 - x) / 2.0) for x in NODES]
UPPER = [float((1.0 + x) / 2.0) for x in NODES]


def along_lanes(line):
    lanes = line.shape[1]
    lane = lax.broadcasted_iota(jnp.int32, line.shape, 1)
    before = jnp.where(lane == 0, 0.0, rolled(line, 1, 1))
    after = jnp.where(lane == lanes - 1, 0.0, rolled(line, -1, 1))
    return jnp.maximum(line, before), jnp.maximum(line, after)


def interpolate(neighbours, nu):
    corner = {}
    for x in range(2):
        for y in range(2):
            line = jnp.maximum(
                jnp.maximum(neighbours[x][y], neighbours[x + 1][y]),
                jnp.maximum(neighbours[x][y + 1], neighbours[x + 1][y + 1]),
            )
            corner[x, y, 0], corner[x, y, 1] = along_lanes(line)
    lower, upper = LOWER, UPPER
    for a in range(5):
        face = {
            (y, z): lower[a] * corner[0, y, z] + upper[a] * corner[1, y, z]
            for y in range(2)
            for z in range(2)
        }
        for b in range(5):
            edge = [lower[b] * face[0, z] + upper[b] * face[1, z] for z in range(2)]
            for c in range(5):
                nu[25 * a + 5 * b + c] = lower[c] * edge[0] + upper[c] * edge[1]
    return corner


def row_masks(axis, chords, spans, lanes):
    row = lax.broadcasted_iota(jnp.int32, (chords * spans, lanes), 0)
    if axis == 0:
        return row < spans, row >= (chords - 1) * spans
    place = row % spans
    return place == 0, place == spans - 1


def outer_rows(axis, chords, spans, last):
    if axis == 0:
        return pl.ds((chords - 1) * spans if last else 0, spans)
    return pl.ds(spans - 1 if last else 0, chords, spans)


def store_pair(work, slot, left, right, down, up, index, rows_low, rows_high):
    work[2 * slot] = left
    work[2 * slot + 1] = right
    down[index] = work[2 * slot, rows_low]
    up[index] = work[2 * slot + 1, rows_high]


def local_kernel(sizes, count, chords, spans, *refs):
    state_hbm = refs[0]
    nu, acc = refs[1:3]
    (
        state, grad, around, work, eps_out, faces_c, faces_s, gain, edge, beta, outside, alpha,
        t0, t1, t2, t3, f0, f1, f2, f3,
    ) = refs[3:23]
    ghosts, flux_ghosts = refs[23:27], refs[27:31]
    load_sem, eps_send, eps_recv, send_sem, recv_sem = refs[31:]
    sends = ((t0, t1, t2, t3), (f0, f1, f2, f3))
    lands = (ghosts, flux_ghosts)
    rows, lanes = nu.shape[1:]
    chord_size, span_size = sizes
    me_c, me_s = lax.axis_index("chord"), lax.axis_index("span")
    mesh_id = pl.DeviceIdType.MESH

    def load(v):
        return pltpu.make_async_copy(state_hbm.at[v], state.at[v], load_sem.at[v])

    for v in range(count):
        load(v).start()

    def reachable(dx):
        if dx == 0:
            return None
        return me_c + 1 < chord_size if dx == 1 else me_c > 0

    def guarded(cond, run):
        if cond is None:
            run()
        else:
            pl.when(cond)(run)

    def partner(dx, dy):
        return (me_c + dx, lax.rem(me_s + dy + span_size, span_size))

    offsets = [(dx, dy) for dx in (0, -1, 1) for dy in (-1, 0, 1) if (dx, dy) != (0, 0)]
    barrier = pltpu.get_barrier_semaphore()
    for dx, dy in offsets:

        def greet(dx=dx, dy=dy):
            pl.semaphore_signal(barrier, inc=1, device_id=partner(dx, dy), device_id_type=mesh_id)

        guarded(reachable(dx), greet)

    def eps_copy(dx, dy):
        slot = 3 * (dx + 1) + dy + 1
        return pltpu.make_async_remote_copy(
            src_ref=eps_out, dst_ref=around.at[1 - dx, 1 - dy],
            send_sem=eps_send.at[slot], recv_sem=eps_recv.at[8 - slot],
            device_id=partner(dx, dy), device_id_type=mesh_id,
        )

    ways = ((1, 0), (-1, 0), (0, 1), (0, -1))

    def message(stage, k, v):
        dx, dy = ways[k]
        return pltpu.make_async_remote_copy(
            src_ref=sends[stage][k].at[v], dst_ref=lands[stage][k].at[v],
            send_sem=send_sem.at[stage, k, v], recv_sem=recv_sem.at[stage, k, v],
            device_id=partner(dx, dy), device_id_type=mesh_id,
        )

    def launch(stage, axis, v):
        for k in (2 * axis, 2 * axis + 1):
            guarded(reachable(ways[k][0]), lambda k=k: message(stage, k, v).start())

    masks = [row_masks(axis, chords, spans, lanes) for axis in range(2)]
    outer = [[outer_rows(axis, chords, spans, last) for last in (False, True)] for axis in range(2)]

    def send_traces(axis, v):
        up, down = sends[0][2 * axis], sends[0][2 * axis + 1]
        faces = (faces_c, faces_s)[axis]

        def body(q, carry):
            for j in range(5):
                left, right = traces(fold([state[v, p] for p in points(axis, q, j)]))
                faces[v, 5 * q + j] = jnp.where(masks[axis][0], left, right)
                store_pair(work, j, left, right, down, up, (v, 5 * q + j), *outer[axis])
            return carry

        lax.fori_loop(0, 5, body, 0)

    load(0).wait()
    send_traces(1, 0)
    sides = jnp.where(me_c > 0, 1, 0) + jnp.where(me_c + 1 < chord_size, 1, 0)
    pl.semaphore_wait(barrier, 2 + 3 * sides)
    launch(0, 1, 0)
    eps = sensor(lambda p: state[0, p], work)
    eps_out[...] = eps
    around[1, 1] = eps
    for dx, dy in offsets:
        guarded(reachable(dx), lambda dx=dx, dy=dy: eps_copy(dx, dy).start())

    send_traces(0, 0)
    launch(0, 0, 0)

    def later_traces(v, carry):
        load(v).wait()
        for axis in (1, 0):
            send_traces(axis, v)
            launch(0, axis, v)
        return carry

    lax.fori_loop(1, count, later_traces, 0)

    lane = lax.broadcasted_iota(jnp.int32, (rows, lanes), 1)
    first, last = lane == 0, lane == lanes - 1

    def normal_gradient(v, carry):
        def body(q, carry):
            for j in range(5):
                pts = points(2, q, j)
                parts = fold([state[v, p] for p in pts])
                left, right = traces(parts)
                before = jnp.where(first, left, rolled(right, 1, 1))
                after = jnp.where(last, right, rolled(left, -1, 1))
                for p, value in zip(pts, slope(parts, before, after)):
                    grad[v, p] = value
            return carry

        lax.fori_loop(0, 5, body, 0, unroll=True)
        return carry

    lax.fori_loop(0, count, normal_gradient, 0)

    row = lax.broadcasted_iota(jnp.int32, (rows, lanes), 0)
    for dx, dy in offsets:
        guarded(reachable(-dx), lambda dx=dx, dy=dy: eps_copy(dx, dy).wait_recv())

    have_low = jnp.where(me_c > 0, spans, 0)
    have_high = jnp.where(me_c + 1 < chord_size, rows, rows - spans)
    low_s, high_s = masks[1]
    low_c, high_c = masks[0]
    column = []
    for x in range(3):
        mine, left, right = around[x, 1], around[x, 0], around[x, 2]
        column.append([
            jnp.where(low_s, rolled(left, 1 - spans, 0), rolled(mine, 1, 0)),
            mine,
            jnp.where(high_s, rolled(right, spans - 1, 0), rolled(mine, -1, 0)),
            jnp.where(low_s, rolled(left, 2 - spans, 0), rolled(right, spans - 2, 0)),
        ])
    closed_low = row < spans - have_low
    closed_high = row >= have_high
    neighbours = [[], [], [], []]
    for y in range(4):
        inner = column[1][y]
        below = jnp.where(low_c, rolled(column[0][y], spans, 0), rolled(inner, spans, 0))
        above = jnp.where(high_c, rolled(column[2][y], -spans, 0), rolled(inner, -spans, 0))
        beyond = jnp.where(
            low_c, rolled(column[0][y], 2 * spans, 0), rolled(column[2][y], -2 * spans, 0)
        )
        neighbours[0].append(jnp.where(closed_low, 0.0, below))
        neighbours[1].append(inner)
        neighbours[2].append(jnp.where(closed_high, 0.0, above))
        neighbours[3].append(beyond)
    corner = interpolate(neighbours, nu)
    near_weight = sum(float(LEFT[i] * HALF_LEFT[i] * (1.0 - NODES[i]) / 2.0) for i in range(5))
    far_weight = sum(float(LEFT[i] * HALF_LEFT[i] * (1.0 + NODES[i]) / 2.0) for i in range(5))
    for axis in range(2):
        low = masks[axis][0]
        sign = jnp.where(low, -1.0, 1.0)
        weight = {}
        for t in range(2):
            pair = []
            for o in (t, t + 1):
                if axis == 0:
                    pair += [jnp.where(low, neighbours[0][o], neighbours[2][o]), neighbours[3][o]]
                else:
                    pair += [jnp.where(low, neighbours[o][0], neighbours[o][2]), neighbours[o][3]]
            line = jnp.maximum(jnp.maximum(pair[0], pair[1]), jnp.maximum(pair[2], pair[3]))
            far = along_lanes(line)
            for z in range(2):
                if axis == 0:
                    near = jnp.where(low, corner[0, t, z], corner[1, t, z])
                else:
                    near = jnp.where(low, corner[t, 0, z], corner[t, 1, z])
                weight[t, z] = sign * (near_weight * near + far_weight * far[z])
        for m in range(5):
            ends = [LOWER[m] * weight[0, z] + UPPER[m] * weight[1, z] for z in range(2)]
            for c in range(5):
                beta[axis, 5 * m + c] = LOWER[c] * ends[0] + UPPER[c] * ends[1]

    for axis in (1, 0):

        def variable(v, carry):
            up, down = sends[1][2 * axis], sends[1][2 * axis + 1]
            low, high = masks[axis]
            step = spans if axis == 0 else 1

            def body(q, carry):
                for j in range(5):
                    pts = points(axis, q, j)
                    parts = fold([state[v, p] for p in pts])
                    left, right = traces(parts)
                    before = jnp.where(low, 0.0, rolled(right, step, 0))
                    after = jnp.where(high, 0.0, rolled(left, -step, 0))
                    if axis == 0:
                        before = jnp.where(closed_low, left, before)
                        after = jnp.where(closed_high, right, after)
                    gradient = slope(parts, before, after)
                    parts = fold([nu[p] * g for p, g in zip(pts, gradient)])
                    left, right = traces(parts)
                    store_pair(work, j, left, right, down, up, (v, 5 * q + j), *outer[axis])
                    before = jnp.where(low, 0.0, rolled(right, step, 0))
                    after = jnp.where(high, 0.0, rolled(left, -step, 0))
                    if axis == 0:
                        before = jnp.where(closed_low, -left, before)
                        after = jnp.where(closed_high, -right, after)
                    for p, value in zip(pts, slope(parts, before, after)):
                        if axis == 1:
                            acc[v, p] = value
                        else:
                            acc[v, p] += value
                return carry

            lax.fori_loop(0, 5, body, 0, unroll=True)
            launch(1, axis, v)
            return carry

        lax.fori_loop(0, count, variable, 0)

    for axis in range(2):
        low, high = masks[axis]

        def gains(q, carry):
            for j in range(5):
                f = 5 * q + j
                spread = []
                for i, p in enumerate(points(axis, q, j)):
                    lift = jnp.where(high, float(HALF_RIGHT[i]), 0.0)
                    spread.append(nu[p] * jnp.where(low, float(HALF_LEFT[i]), lift))
                parts = fold(spread)
                left, right = traces(parts)
                edge[axis, 2 * f] = left
                edge[axis, 2 * f + 1] = right
                for i, value in enumerate(slope(parts, None, None)):
                    gain[axis, 5 * f + i] = value
            return carry

        lax.fori_loop(0, 5, gains, 0)

    def normal(v, carry):
        def body(q, carry):
            for j in range(5):
                pts = points(2, q, j)
                parts = fold([nu[p] * grad[v, p] for p in pts])
                left, right = traces(parts)
                before = jnp.where(first, -left, rolled(right, 1, 1))
                after = jnp.where(last, -right, rolled(left, -1, 1))
                for p, value in zip(pts, slope(parts, before, after)):
                    acc[v, p] += value
            return carry

        lax.fori_loop(0, 5, body, 0, unroll=True)
        return carry

    lax.fori_loop(0, count, normal, 0)

    def arrived(axis, v):
        for k in (2 * axis, 2 * axis + 1):
            for stage in range(2):
                guarded(
                    reachable(-ways[k][0]),
                    lambda k=k, stage=stage: message(stage, k, v).wait_recv(),
                )

    for axis in (0, 1):

        def correct(v, carry):
            arrived(axis, v)
            up, down = ghosts[2 * axis], ghosts[2 * axis + 1]
            f_up, f_down = flux_ghosts[2 * axis], flux_ghosts[2 * axis + 1]
            faces = (faces_c, faces_s)[axis]
            low, high = masks[axis]
            rows_low, rows_high = outer[axis]
            step = spans if axis == 0 else 1
            opened = low | high
            if axis == 0:
                opened = opened & jnp.logical_not(closed_low | closed_high)

            def gather(q, carry):
                for j in range(5):
                    f = 5 * q + j
                    outside[f, rows_low] = up[v, f]
                    outside[f, rows_high] = down[v, f]
                    alpha[f, rows_low] = f_up[v, f]
                    alpha[f, rows_high] = f_down[v, f]
                return carry

            lax.fori_loop(0, 5, gather, 0)

            def body(q, carry):
                for j in range(5):
                    f = 5 * q + j
                    ghost = jnp.where(opened, outside[f], 0.0)
                    flux = jnp.where(opened, alpha[f] + beta[axis, f] * faces[v, f], 0.0)
                    before = jnp.where(low, flux, rolled(edge[axis, 2 * f + 1] * ghost, step, 0))
                    after = jnp.where(high, flux, rolled(edge[axis, 2 * f] * ghost, -step, 0))
                    h = [float(x) for x in HALF_LEFT]
                    diff, both = before - after, before + after
                    even = [0.5 * (h[i] + h[4 - i]) * diff for i in range(3)]
                    odd = [0.5 * (h[i] - h[4 - i]) * both for i in range(2)]
                    lifts = [
                        even[0] + odd[0], even[1] + odd[1], even[2],
                        even[1] - odd[1], even[0] - odd[0],
                    ]
                    for i, p in enumerate(points(axis, q, j)):
                        acc[v, p] += gain[axis, 5 * f + i] * ghost + lifts[i]
                return carry

            lax.fori_loop(0, 5, body, 0, unroll=True)
            return carry

        lax.fori_loop(0, count, correct, 0)

    for dx, dy in offsets:
        guarded(reachable(dx), lambda dx=dx, dy=dy: eps_copy(dx, dy).wait_send())
    for stage in range(2):
        for k in range(4):
            for v in range(count):
                guarded(
                    reachable(ways[k][0]),
                    lambda stage=stage, k=k, v=v: message(stage, k, v).wait_send(),
                )


def finish_kernel(acc, nu, residual_out, nu_out, sems):
    copies = [
        pltpu.make_async_copy(acc.at[v], residual_out.at[v], sems.at[v])
        for v in range(acc.shape[0])
    ]
    copies.append(pltpu.make_async_copy(nu, nu_out, sems.at[acc.shape[0]]))
    for copy in copies:
        copy.start()
    for copy in copies:
        copy.wait()


def shards(state):
    count, npts, chords, spans, lanes = state.shape
    rows = chords * spans
    flat = state.reshape(count, npts, rows, lanes)
    f32 = jnp.float32
    sizes = (lax.axis_size("chord"), lax.axis_size("span"))

    def message(n, k):
        return (n, 25, spans if k < 2 else chords, lanes)

    def full(*shape):
        return jax.ShapeDtypeStruct(shape, f32)

    vmem = pl.BlockSpec(memory_space=pltpu.VMEM)
    nu, residual = pl.pallas_call(
        functools.partial(local_kernel, sizes, count, chords, spans),
        in_specs=[pl.BlockSpec(memory_space=pltpu.HBM)],
        out_specs=[vmem, vmem],
        out_shape=[full(npts, rows, lanes), full(count, npts, rows, lanes)],
        scratch_shapes=[
            pltpu.VMEM(shape, f32)
            for shape in [
                (count, npts, rows, lanes),
                (count, npts, rows, lanes),
                (3, 3, rows, lanes),
                (npts, rows, lanes),
                (rows, lanes),
                (count, 25, rows, lanes),
                (count, 25, rows, lanes),
                (2, npts, rows, lanes),
                (2, 50, rows, lanes),
                (2, 25, rows, lanes),
                (25, rows, lanes),
                (25, rows, lanes),
            ]
            + [message(count, k) for k in range(4)] * 4
        ]
        + [
            pltpu.SemaphoreType.DMA((count,)),
            pltpu.SemaphoreType.DMA((9,)),
            pltpu.SemaphoreType.DMA((9,)),
            pltpu.SemaphoreType.DMA((2, 4, count)),
            pltpu.SemaphoreType.DMA((2, 4, count)),
        ],
        compiler_params=pltpu.CompilerParams(
            collective_id=0, has_side_effects=True, vmem_limit_bytes=VMEM_BYTES
        ),
    )(flat)
    hbm = pl.BlockSpec(memory_space=pltpu.HBM)
    residual, nu = pl.pallas_call(
        finish_kernel,
        in_specs=[vmem, vmem],
        out_specs=[hbm, hbm],
        out_shape=[full(count, npts, rows, lanes), full(npts, rows, lanes)],
        scratch_shapes=[pltpu.SemaphoreType.DMA((count + 1,))],
        compiler_params=pltpu.CompilerParams(vmem_limit_bytes=FINISH_BYTES),
    )(residual, nu)
    return residual.reshape(state.shape), nu.reshape(npts, chords, spans, lanes)


def solution(mesh):
    in_specs = (P(None, None, "chord", "span", None),)
    out_specs = (P(None, None, "chord", "span", None), P(None, "chord", "span", None))
    return jax.shard_map(shards, mesh=mesh, in_specs=in_specs, out_specs=out_specs, check_vma=False)
```

```python
import functools
import math

import jax
import jax.numpy as jnp
import numpy as np
from jax import lax
from jax.experimental import pallas as pl
from jax.experimental.pallas import tpu as pltpu
from jax.sharding import PartitionSpec as P

VMEM_BYTES = 52_500_000
FINISH_BYTES = 8_000_000
EPS_SCALE = 0.01
SENSOR_CENTRE = -3.0
SENSOR_WIDTH = 1.5
RATIO_FLOOR = 1e-06
ENERGY_EPS = 1e-06
GAUSS_NODES = [-0.906179845938664, -0.5384693101056831, 0.0, 0.5384693101056831, 0.906179845938664]
GAUSS_WEIGHTS = [
    0.2369268850561891,
    0.4786286704993665,
    0.5688888888888889,
    0.4786286704993665,
    0.2369268850561891,
]


def legendre_values(points):
    values = [np.ones(points.shape), np.array(points)]
    for order in range(1, 5):
        values.append(
            ((2 * order + 1) * points * values[order] - order * values[order - 1]) / (order + 1)
        )
    return values


def line_tables():
    line_nodes = np.array(GAUSS_NODES)
    quadrature_weights = np.array(GAUSS_WEIGHTS)
    barycentric = np.array(
        [
            1.0 / np.prod([line_nodes[j] - line_nodes[k] for k in range(5) if k != j])
            for j in range(5)
        ]
    )
    derivative = np.zeros((5, 5))
    for i in range(5):
        for j in range(5):
            if i != j:
                derivative[i, j] = barycentric[j] / barycentric[i] / (line_nodes[i] - line_nodes[j])
        derivative[i, i] = -np.sum(derivative[i])
    left_values = np.ones(5)
    right_values = np.ones(5)
    for j in range(5):
        for k in range(5):
            if k != j:
                left_values[j] *= (-1.0 - line_nodes[k]) / (line_nodes[j] - line_nodes[k])
                right_values[j] *= (1.0 - line_nodes[k]) / (line_nodes[j] - line_nodes[k])
    legendre = legendre_values(line_nodes)
    fourth_slope = 7.0 * legendre[3] + 3.0 * legendre[1]
    fifth_slope = 9.0 * legendre[4] + 5.0 * legendre[2] + legendre[0]
    left_corr = 0.5 * (fourth_slope - fifth_slope)
    right_corr = 0.5 * (fourth_slope + fifth_slope)
    modal = np.zeros((5, 5))
    for k in range(5):
        modal[k, :] = quadrature_weights * math.sqrt((2 * k + 1) / 2.0) * legendre[k]
    return (line_nodes, derivative, left_values, right_values, left_corr, right_corr, modal)


NODES, DERIV, LEFT, RIGHT, LIFT_LEFT, LIFT_RIGHT, MODAL = line_tables()
HALF_LEFT = 0.5 * LIFT_LEFT
HALF_RIGHT = 0.5 * LIFT_RIGHT


def fold(u):
    return (u[0] + u[4], u[1] + u[3], u[2], u[0] - u[4], u[1] - u[3])


def traces(parts):
    s0, s1, mid, d0, d1 = parts
    r = [float(x) for x in RIGHT]
    even = 0.5 * (r[0] + r[4]) * s0 + 0.5 * (r[1] + r[3]) * s1 + r[2] * mid
    odd = 0.5 * (r[0] - r[4]) * d0 + 0.5 * (r[1] - r[3]) * d1
    return even - odd, even + odd


def slope(parts, before, after):
    s0, s1, mid, d0, d1 = parts
    h = [float(x) for x in HALF_LEFT]
    r = [float(x) for x in RIGHT]
    if before is not None:
        diff, both = before - after, before + after
    even, odd = [], []
    for i in range(3):
        lift = 0.5 * (h[i] + h[4 - i])
        value = (
            float(0.5 * (DERIV[i, 0] - DERIV[i, 4]) + lift * (r[0] - r[4])) * d0
            + float(0.5 * (DERIV[i, 1] - DERIV[i, 3]) + lift * (r[1] - r[3])) * d1
        )
        even.append(value if before is None else value + lift * diff)
    for i in range(2):
        lift = 0.5 * (h[i] - h[4 - i])
        value = (
            float(0.5 * (DERIV[i, 0] + DERIV[i, 4]) - lift * (r[0] + r[4])) * s0
            + float(0.5 * (DERIV[i, 1] + DERIV[i, 3]) - lift * (r[1] + r[3])) * s1
            + float(DERIV[i, 2] - 2.0 * lift * r[2]) * mid
        )
        odd.append(value if before is None else value + lift * both)
    return [even[0] + odd[0], even[1] + odd[1], even[2], even[1] - odd[1], even[0] - odd[0]]


def points(axis, q, j):
    if axis == 0:
        return [25 * i + 5 * q + j for i in range(5)]
    if axis == 1:
        return [25 * q + 5 * i + j for i in range(5)]
    return [25 * q + 5 * j + i for i in range(5)]


def modal_line(u):
    s0, s1, mid, d0, d1 = fold(u)
    out = []
    for k in range(5):
        m = [float(x) for x in MODAL[k]]
        out.append(m[0] * s0 + m[1] * s1 + m[2] * mid if k % 2 == 0 else m[0] * d0 + m[1] * d1)
    return out


def sensor(load, work):
    def first(q, carry):
        for j in range(5):
            pts = points(0, q, j)
            for i, value in zip(pts, modal_line([load(p) for p in pts])):
                work[i] = value
        return carry

    lax.fori_loop(0, 5, first, 0)

    def second(q, carry):
        total, high = carry
        plane = {}
        for c in range(5):
            for b, value in enumerate(modal_line([work[25 * q + 5 * b + c] for b in range(5)])):
                plane[b, c] = value
        low = jnp.zeros_like(total)
        edge = jnp.zeros_like(total)
        for b in range(5):
            line = modal_line([plane[b, c] for c in range(5)])
            squares = [x * x for x in line]
            if b < 4:
                low = low + ((squares[0] + squares[1]) + (squares[2] + squares[3]))
                edge = edge + squares[4]
            else:
                edge = edge + ((squares[0] + squares[1]) + (squares[2] + squares[3])) + squares[4]
        plane_total = low + edge
        return total + plane_total, high + jnp.where(q == 4, plane_total, edge)

    zero = jnp.zeros(work.shape[1:], jnp.float32)
    total, high = lax.fori_loop(0, 5, second, (zero, zero))
    level = jnp.log(jnp.maximum(high / (total + ENERGY_EPS), RATIO_FLOOR)) * (1.0 / math.log(10.0))
    ramp = jnp.clip((level - SENSOR_CENTRE) / SENSOR_WIDTH, -1.0, 1.0)
    return EPS_SCALE * 0.5 * (1.0 + jnp.sin(0.5 * math.pi * ramp))


def rolled(value, shift, axis):
    size = value.shape[axis]
    return pltpu.roll(value, shift % size, axis)


LOWER = [float((1.0 - x) / 2.0) for x in NODES]
UPPER = [float((1.0 + x) / 2.0) for x in NODES]


def along_lanes(line):
    lanes = line.shape[1]
    lane = lax.broadcasted_iota(jnp.int32, line.shape, 1)
    before = jnp.where(lane == 0, 0.0, rolled(line, 1, 1))
    after = jnp.where(lane == lanes - 1, 0.0, rolled(line, -1, 1))
    return jnp.maximum(line, before), jnp.maximum(line, after)


def interpolate(neighbours, nu):
    corner = {}
    for x in range(2):
        for y in range(2):
            line = jnp.maximum(
                jnp.maximum(neighbours[x][y], neighbours[x + 1][y]),
                jnp.maximum(neighbours[x][y + 1], neighbours[x + 1][y + 1]),
            )
            corner[x, y, 0], corner[x, y, 1] = along_lanes(line)
    lower, upper = LOWER, UPPER
    for a in range(5):
        face = {
            (y, z): lower[a] * corner[0, y, z] + upper[a] * corner[1, y, z]
            for y in range(2)
            for z in range(2)
        }
        for b in range(5):
            edge = [lower[b] * face[0, z] + upper[b] * face[1, z] for z in range(2)]
            for c in range(5):
                nu[25 * a + 5 * b + c] = lower[c] * edge[0] + upper[c] * edge[1]


def row_masks(axis, chords, spans, lanes):
    row = lax.broadcasted_iota(jnp.int32, (chords * spans, lanes), 0)
    if axis == 0:
        return row < spans, row >= (chords - 1) * spans
    place = row % spans
    return place == 0, place == spans - 1


def total_of(values):
    out = values[0]
    for value in values[1:]:
        out = out + value
    return out


def local_kernel(sizes, count, chords, spans, *refs):
    state_hbm = refs[0]
    nu, acc = refs[1:3]
    state, grad, around, work, eps_out = refs[3:8]
    faces = (refs[8:10], refs[10:12])
    ghosts = (refs[12:14], refs[14:16])
    load_sem, eps_send, eps_recv, send_sem, recv_sem = refs[16:]
    rows, lanes = nu.shape[1:]
    chord_size, span_size = sizes
    me_c, me_s = lax.axis_index("chord"), lax.axis_index("span")
    mesh_id = pl.DeviceIdType.MESH

    def whole(ref):
        return ref.reshape(count, 25, rows, lanes)

    def load(v):
        return pltpu.make_async_copy(state_hbm.at[v], state.at[v], load_sem.at[v])

    for v in range(count):
        load(v).start()

    def reachable(dx):
        if dx == 0:
            return None
        return me_c + 1 < chord_size if dx == 1 else me_c > 0

    def guarded(cond, run):
        if cond is None:
            run()
        else:
            pl.when(cond)(run)

    def partner(dx, dy):
        return (me_c + dx, lax.rem(me_s + dy + span_size, span_size))

    offsets = [(dx, dy) for dx in (0, -1, 1) for dy in (-1, 0, 1) if (dx, dy) != (0, 0)]
    barrier = pltpu.get_barrier_semaphore()
    for dx, dy in offsets:

        def greet(dx=dx, dy=dy):
            pl.semaphore_signal(barrier, inc=1, device_id=partner(dx, dy), device_id_type=mesh_id)

        guarded(reachable(dx), greet)

    def eps_copy(dx, dy):
        slot = 3 * (dx + 1) + dy + 1
        return pltpu.make_async_remote_copy(
            src_ref=eps_out, dst_ref=around.at[1 - dx, 1 - dy],
            send_sem=eps_send.at[slot], recv_sem=eps_recv.at[8 - slot],
            device_id=partner(dx, dy), device_id_type=mesh_id,
        )

    ways = ((1, 0), (-1, 0), (0, 1), (0, -1))

    def side(ref, axis, v, last):
        if axis == 0:
            return ref.at[v, :, chords - 1 if last else 0]
        return ref.at[v, :, :, spans - 1 if last else 0]

    def message(stage, k, v):
        dx, dy = ways[k]
        axis, up = k // 2, k % 2 == 0
        return pltpu.make_async_remote_copy(
            src_ref=side(faces[stage][axis], axis, v, up),
            dst_ref=side(ghosts[stage][axis], axis, v, not up),
            send_sem=send_sem.at[stage, k, v], recv_sem=recv_sem.at[stage, k, v],
            device_id=partner(dx, dy), device_id_type=mesh_id,
        )

    def launch(stage, axis, v):
        for k in (2 * axis, 2 * axis + 1):
            guarded(reachable(ways[k][0]), lambda k=k: message(stage, k, v).start())

    def arrived(stage, axis, v):
        for k in (2 * axis, 2 * axis + 1):
            guarded(reachable(-ways[k][0]), lambda k=k: message(stage, k, v).wait_recv())

    def sent(stage, axis, v):
        for k in (2 * axis, 2 * axis + 1):
            guarded(reachable(ways[k][0]), lambda k=k: message(stage, k, v).wait_send())

    masks = [row_masks(axis, chords, spans, lanes) for axis in range(2)]

    def send_traces(axis, v):
        low = masks[axis][0]
        ends = [jnp.where(low, float(LEFT[i]), float(RIGHT[i])) for i in range(5)]
        out = whole(faces[0][axis])
        for q in range(5):
            for j in range(5):
                pts = points(axis, q, j)
                out[v, 5 * q + j] = total_of([e * state[v, p] for e, p in zip(ends, pts)])
        launch(0, axis, v)

    load(0).wait()
    sides = jnp.where(me_c > 0, 1, 0) + jnp.where(me_c + 1 < chord_size, 1, 0)
    pl.semaphore_wait(barrier, 2 + 3 * sides)
    send_traces(1, 0)
    eps = sensor(lambda p: state[0, p], work)
    eps_out[...] = eps
    around[1, 1] = eps
    for dx, dy in offsets:
        guarded(reachable(dx), lambda dx=dx, dy=dy: eps_copy(dx, dy).start())

    send_traces(0, 0)

    def later_traces(v, carry):
        load(v).wait()
        for axis in (1, 0):
            send_traces(axis, v)
        return carry

    lax.fori_loop(1, count, later_traces, 0)

    lane = lax.broadcasted_iota(jnp.int32, (rows, lanes), 1)
    first, last = lane == 0, lane == lanes - 1

    def normal_gradient(v, carry):
        for q in range(5):
            for j in range(5):
                pts = points(2, q, j)
                parts = fold([state[v, p] for p in pts])
                left, right = traces(parts)
                before = jnp.where(first, left, rolled(right, 1, 1))
                after = jnp.where(last, right, rolled(left, -1, 1))
                for p, value in zip(pts, slope(parts, before, after)):
                    grad[v, p] = value
        return carry

    lax.fori_loop(0, count, normal_gradient, 0)

    row = lax.broadcasted_iota(jnp.int32, (rows, lanes), 0)
    for dx, dy in offsets:
        guarded(reachable(-dx), lambda dx=dx, dy=dy: eps_copy(dx, dy).wait_recv())

    have_low = jnp.where(me_c > 0, spans, 0)
    have_high = jnp.where(me_c + 1 < chord_size, rows, rows - spans)
    low_s, high_s = masks[1]
    low_c, high_c = masks[0]
    closed_low = row < spans - have_low
    closed_high = row >= have_high
    closed = closed_low | closed_high
    column = []
    for x in range(3):
        mine, left, right = around[x, 1], around[x, 0], around[x, 2]
        column.append([
            jnp.where(low_s, rolled(left, 1 - spans, 0), rolled(mine, 1, 0)),
            mine,
            jnp.where(high_s, rolled(right, spans - 1, 0), rolled(mine, -1, 0)),
        ])
    neighbours = [[], [], []]
    for y in range(3):
        inner = column[1][y]
        below = jnp.where(low_c, rolled(column[0][y], spans, 0), rolled(inner, spans, 0))
        above = jnp.where(high_c, rolled(column[2][y], -spans, 0), rolled(inner, -spans, 0))
        neighbours[0].append(jnp.where(closed_low, 0.0, below))
        neighbours[1].append(inner)
        neighbours[2].append(jnp.where(closed_high, 0.0, above))
    interpolate(neighbours, nu)

    for axis in (1, 0):
        low, high = masks[axis]
        step = spans if axis == 0 else 1
        shut = jnp.where(closed, -1.0, 0.0)
        mine, ghost = whole(faces[0][axis]), whole(ghosts[0][axis])
        out = whole(faces[1][axis])

        def variable(v, carry):
            arrived(0, axis, v)
            for q in range(5):
                for j in range(5):
                    f = 5 * q + j
                    pts = points(axis, q, j)
                    parts = fold([state[v, p] for p in pts])
                    left, right = traces(parts)
                    beyond = ghost[v, f]
                    if axis == 0:
                        beyond = jnp.where(closed, mine[v, f], beyond)
                    before = jnp.where(low, beyond, rolled(right, step, 0))
                    after = jnp.where(high, beyond, rolled(left, -step, 0))
                    gradient = slope(parts, before, after)
                    parts = fold([nu[p] * g for p, g in zip(pts, gradient)])
                    left, right = traces(parts)
                    ends = jnp.where(low, left, right)
                    out[v, f] = ends
                    beyond = shut * ends if axis == 0 else 0.0
                    before = jnp.where(low, beyond, rolled(right, step, 0))
                    after = jnp.where(high, beyond, rolled(left, -step, 0))
                    for p, value in zip(pts, slope(parts, before, after)):
                        if axis == 1:
                            acc[v, p] = value
                        else:
                            acc[v, p] += value
            launch(1, axis, v)
            return carry

        lax.fori_loop(0, count, variable, 0)

    def normal(v, carry):
        for q in range(5):
            for j in range(5):
                pts = points(2, q, j)
                parts = fold([nu[p] * grad[v, p] for p in pts])
                left, right = traces(parts)
                before = jnp.where(first, -left, rolled(right, 1, 1))
                after = jnp.where(last, -right, rolled(left, -1, 1))
                for p, value in zip(pts, slope(parts, before, after)):
                    acc[v, p] += value
        for axis in range(2):
            sent(0, axis, v)
        return carry

    lax.fori_loop(0, count, normal, 0)

    for dx, dy in offsets:
        guarded(reachable(dx), lambda dx=dx, dy=dy: eps_copy(dx, dy).wait_send())

    lifts = [
        [
            jnp.where(low, float(HALF_LEFT[i]), jnp.where(high, float(HALF_RIGHT[i]), 0.0))
            for i in range(5)
        ]
        for low, high in masks
    ]
    edges = [(low | high) for low, high in masks]
    edges[0] = edges[0] & jnp.logical_not(closed)

    def correct(v, carry):
        for axis in range(2):
            arrived(1, axis, v)
        for axis in range(2):
            sent(1, axis, v)
        flux_c, flux_s = whole(ghosts[1][0]), whole(ghosts[1][1])
        for c in range(5):
            along = [
                [jnp.where(edges[0], flux_c[v, 5 * b + c], 0.0) for b in range(5)],
                [jnp.where(edges[1], flux_s[v, 5 * a + c], 0.0) for a in range(5)],
            ]
            for a in range(5):
                for b in range(5):
                    acc[v, 25 * a + 5 * b + c] += (
                        lifts[0][a] * along[0][b] + lifts[1][b] * along[1][a]
                    )
        return carry

    lax.fori_loop(0, count, correct, 0)


def finish_kernel(acc, nu, residual_out, nu_out, sems):
    copies = [
        pltpu.make_async_copy(acc.at[v], residual_out.at[v], sems.at[v])
        for v in range(acc.shape[0])
    ]
    copies.append(pltpu.make_async_copy(nu, nu_out, sems.at[acc.shape[0]]))
    for copy in copies:
        copy.start()
    for copy in copies:
        copy.wait()


def shards(state):
    count, npts, chords, spans, lanes = state.shape
    rows = chords * spans
    flat = state.reshape(count, npts, rows, lanes)
    f32 = jnp.float32
    sizes = (lax.axis_size("chord"), lax.axis_size("span"))

    def full(*shape):
        return jax.ShapeDtypeStruct(shape, f32)

    vmem = pl.BlockSpec(memory_space=pltpu.VMEM)
    nu, residual = pl.pallas_call(
        functools.partial(local_kernel, sizes, count, chords, spans),
        in_specs=[pl.BlockSpec(memory_space=pltpu.HBM)],
        out_specs=[vmem, vmem],
        out_shape=[full(npts, rows, lanes), full(count, npts, rows, lanes)],
        scratch_shapes=[
            pltpu.VMEM(shape, f32)
            for shape in [
                (count, npts, rows, lanes),
                (count, npts, rows, lanes),
                (3, 3, rows, lanes),
                (npts, rows, lanes),
                (rows, lanes),
            ]
            + [(count, 25, chords, spans, lanes)] * 8
        ]
        + [
            pltpu.SemaphoreType.DMA((count,)),
            pltpu.SemaphoreType.DMA((9,)),
            pltpu.SemaphoreType.DMA((9,)),
            pltpu.SemaphoreType.DMA((2, 4, count)),
            pltpu.SemaphoreType.DMA((2, 4, count)),
        ],
        compiler_params=pltpu.CompilerParams(
            collective_id=0, has_side_effects=True, vmem_limit_bytes=VMEM_BYTES
        ),
    )(flat)
    hbm = pl.BlockSpec(memory_space=pltpu.HBM)
    residual, nu = pl.pallas_call(
        finish_kernel,
        in_specs=[vmem, vmem],
        out_specs=[hbm, hbm],
        out_shape=[full(count, npts, rows, lanes), full(npts, rows, lanes)],
        scratch_shapes=[pltpu.SemaphoreType.DMA((count + 1,))],
        compiler_params=pltpu.CompilerParams(vmem_limit_bytes=FINISH_BYTES),
    )(residual, nu)
    return residual.reshape(state.shape), nu.reshape(npts, chords, spans, lanes)


def solution(mesh):
    in_specs = (P(None, None, "chord", "span", None),)
    out_specs = (P(None, None, "chord", "span", None), P(None, "chord", "span", None))
    return jax.shard_map(shards, mesh=mesh, in_specs=in_specs, out_specs=out_specs, check_vma=False)
```

```python
import functools
import math

import jax
import jax.numpy as jnp
import numpy as np
from jax import lax
from jax.experimental import pallas as pl
from jax.experimental.pallas import tpu as pltpu
from jax.sharding import PartitionSpec as P

VMEM_BYTES = 52_500_000
FINISH_BYTES = 8_000_000
EPS_SCALE = 0.01
SENSOR_CENTRE = -3.0
SENSOR_WIDTH = 1.5
RATIO_FLOOR = 1e-06
ENERGY_EPS = 1e-06
GAUSS_NODES = [-0.906179845938664, -0.5384693101056831, 0.0, 0.5384693101056831, 0.906179845938664]
GAUSS_WEIGHTS = [
    0.2369268850561891,
    0.4786286704993665,
    0.5688888888888889,
    0.4786286704993665,
    0.2369268850561891,
]


def legendre_values(points):
    values = [np.ones(points.shape), np.array(points)]
    for order in range(1, 5):
        values.append(
            ((2 * order + 1) * points * values[order] - order * values[order - 1]) / (order + 1)
        )
    return values


def line_tables():
    line_nodes = np.array(GAUSS_NODES)
    quadrature_weights = np.array(GAUSS_WEIGHTS)
    barycentric = np.array(
        [
            1.0 / np.prod([line_nodes[j] - line_nodes[k] for k in range(5) if k != j])
            for j in range(5)
        ]
    )
    derivative = np.zeros((5, 5))
    for i in range(5):
        for j in range(5):
            if i != j:
                derivative[i, j] = barycentric[j] / barycentric[i] / (line_nodes[i] - line_nodes[j])
        derivative[i, i] = -np.sum(derivative[i])
    left_values = np.ones(5)
    right_values = np.ones(5)
    for j in range(5):
        for k in range(5):
            if k != j:
                left_values[j] *= (-1.0 - line_nodes[k]) / (line_nodes[j] - line_nodes[k])
                right_values[j] *= (1.0 - line_nodes[k]) / (line_nodes[j] - line_nodes[k])
    legendre = legendre_values(line_nodes)
    fourth_slope = 7.0 * legendre[3] + 3.0 * legendre[1]
    fifth_slope = 9.0 * legendre[4] + 5.0 * legendre[2] + legendre[0]
    left_corr = 0.5 * (fourth_slope - fifth_slope)
    right_corr = 0.5 * (fourth_slope + fifth_slope)
    modal = np.zeros((5, 5))
    for k in range(5):
        modal[k, :] = quadrature_weights * math.sqrt((2 * k + 1) / 2.0) * legendre[k]
    return (line_nodes, derivative, left_values, right_values, left_corr, right_corr, modal)


NODES, DERIV, LEFT, RIGHT, LIFT_LEFT, LIFT_RIGHT, MODAL = line_tables()
HALF_LEFT = 0.5 * LIFT_LEFT
HALF_RIGHT = 0.5 * LIFT_RIGHT


def fold(u):
    return (u[0] + u[4], u[1] + u[3], u[2], u[0] - u[4], u[1] - u[3])


def traces(parts):
    s0, s1, mid, d0, d1 = parts
    r = [float(x) for x in RIGHT]
    even = 0.5 * (r[0] + r[4]) * s0 + 0.5 * (r[1] + r[3]) * s1 + r[2] * mid
    odd = 0.5 * (r[0] - r[4]) * d0 + 0.5 * (r[1] - r[3]) * d1
    return even - odd, even + odd


def slope(parts, before, after):
    s0, s1, mid, d0, d1 = parts
    h = [float(x) for x in HALF_LEFT]
    r = [float(x) for x in RIGHT]
    if before is not None:
        diff, both = before - after, before + after
    even, odd = [], []
    for i in range(3):
        lift = 0.5 * (h[i] + h[4 - i])
        value = (
            float(0.5 * (DERIV[i, 0] - DERIV[i, 4]) + lift * (r[0] - r[4])) * d0
            + float(0.5 * (DERIV[i, 1] - DERIV[i, 3]) + lift * (r[1] - r[3])) * d1
        )
        even.append(value if before is None else value + lift * diff)
    for i in range(2):
        lift = 0.5 * (h[i] - h[4 - i])
        value = (
            float(0.5 * (DERIV[i, 0] + DERIV[i, 4]) - lift * (r[0] + r[4])) * s0
            + float(0.5 * (DERIV[i, 1] + DERIV[i, 3]) - lift * (r[1] + r[3])) * s1
            + float(DERIV[i, 2] - 2.0 * lift * r[2]) * mid
        )
        odd.append(value if before is None else value + lift * both)
    return [even[0] + odd[0], even[1] + odd[1], even[2], even[1] - odd[1], even[0] - odd[0]]


def points(axis, q, j):
    if axis == 0:
        return [25 * i + 5 * q + j for i in range(5)]
    if axis == 1:
        return [25 * q + 5 * i + j for i in range(5)]
    return [25 * q + 5 * j + i for i in range(5)]


def modal_line(u):
    s0, s1, mid, d0, d1 = fold(u)
    out = []
    for k in range(5):
        m = [float(x) for x in MODAL[k]]
        out.append(m[0] * s0 + m[1] * s1 + m[2] * mid if k % 2 == 0 else m[0] * d0 + m[1] * d1)
    return out


def sensor(load, work):
    def first(q, carry):
        for j in range(5):
            pts = points(0, q, j)
            for i, value in zip(pts, modal_line([load(p) for p in pts])):
                work[i] = value
        return carry

    lax.fori_loop(0, 5, first, 0)

    def second(q, carry):
        total, high = carry
        plane = {}
        for c in range(5):
            for b, value in enumerate(modal_line([work[25 * q + 5 * b + c] for b in range(5)])):
                plane[b, c] = value
        low = jnp.zeros_like(total)
        edge = jnp.zeros_like(total)
        for b in range(5):
            line = modal_line([plane[b, c] for c in range(5)])
            squares = [x * x for x in line]
            if b < 4:
                low = low + ((squares[0] + squares[1]) + (squares[2] + squares[3]))
                edge = edge + squares[4]
            else:
                edge = edge + ((squares[0] + squares[1]) + (squares[2] + squares[3])) + squares[4]
        plane_total = low + edge
        return total + plane_total, high + jnp.where(q == 4, plane_total, edge)

    zero = jnp.zeros(work.shape[1:], jnp.float32)
    total, high = lax.fori_loop(0, 5, second, (zero, zero))
    level = jnp.log(jnp.maximum(high / (total + ENERGY_EPS), RATIO_FLOOR)) * (1.0 / math.log(10.0))
    ramp = jnp.clip((level - SENSOR_CENTRE) / SENSOR_WIDTH, -1.0, 1.0)
    return EPS_SCALE * 0.5 * (1.0 + jnp.sin(0.5 * math.pi * ramp))


def rolled(value, shift, axis):
    size = value.shape[axis]
    return pltpu.roll(value, shift % size, axis)


LOWER = [float((1.0 - x) / 2.0) for x in NODES]
UPPER = [float((1.0 + x) / 2.0) for x in NODES]


def along_lanes(line):
    lanes = line.shape[1]
    lane = lax.broadcasted_iota(jnp.int32, line.shape, 1)
    before = jnp.where(lane == 0, 0.0, rolled(line, 1, 1))
    after = jnp.where(lane == lanes - 1, 0.0, rolled(line, -1, 1))
    return jnp.maximum(line, before), jnp.maximum(line, after)


def interpolate(neighbours, nu):
    corner = {}
    for x in range(2):
        for y in range(2):
            line = jnp.maximum(
                jnp.maximum(neighbours[x][y], neighbours[x + 1][y]),
                jnp.maximum(neighbours[x][y + 1], neighbours[x + 1][y + 1]),
            )
            corner[x, y, 0], corner[x, y, 1] = along_lanes(line)
    lower, upper = LOWER, UPPER
    for a in range(5):
        face = {
            (y, z): lower[a] * corner[0, y, z] + upper[a] * corner[1, y, z]
            for y in range(2)
            for z in range(2)
        }
        for b in range(5):
            edge = [lower[b] * face[0, z] + upper[b] * face[1, z] for z in range(2)]
            for c in range(5):
                nu[25 * a + 5 * b + c] = lower[c] * edge[0] + upper[c] * edge[1]


def row_masks(axis, chords, spans, lanes):
    row = lax.broadcasted_iota(jnp.int32, (chords * spans, lanes), 0)
    if axis == 0:
        return row < spans, row >= (chords - 1) * spans
    place = row % spans
    return place == 0, place == spans - 1


def total_of(values):
    out = values[0]
    for value in values[1:]:
        out = out + value
    return out


def local_kernel(sizes, count, chords, spans, *refs):
    state_hbm = refs[0]
    nu, acc = refs[1:3]
    state, grad, around, work, eps_out = refs[3:8]
    faces = (refs[8:10], refs[10:12])
    ghosts = (refs[12:14], refs[14:16])
    load_sem, eps_sem, send_sem, state_sem, flux_sem, chord_sem = refs[16:]
    rows, lanes = nu.shape[1:]
    chord_size, span_size = sizes
    me_c, me_s = lax.axis_index("chord"), lax.axis_index("span")
    mesh_id = pl.DeviceIdType.MESH

    def whole(ref):
        return ref.reshape(count, 25, rows, lanes)

    def load(first, size):
        part = pl.ds(first, size)
        return pltpu.make_async_copy(
            state_hbm.at[part], state.at[part], load_sem.at[min(first, 1)]
        )

    load(0, 1).start()
    load(1, count - 1).start()

    def reachable(dx):
        if dx == 0:
            return None
        return me_c + 1 < chord_size if dx == 1 else me_c > 0

    def guarded(cond, run):
        if cond is None:
            run()
        else:
            pl.when(cond)(run)

    def partner(dx, dy):
        return (me_c + dx, lax.rem(me_s + dy + span_size, span_size))

    offsets = [(dx, dy) for dx in (0, -1, 1) for dy in (-1, 0, 1) if (dx, dy) != (0, 0)]
    barrier = pltpu.get_barrier_semaphore()
    for dx, dy in offsets:

        def greet(dx=dx, dy=dy):
            pl.semaphore_signal(barrier, inc=1, device_id=partner(dx, dy), device_id_type=mesh_id)

        guarded(reachable(dx), greet)

    def eps_copy(dx, dy):
        return pltpu.make_async_remote_copy(
            src_ref=eps_out, dst_ref=around.at[1 - dx, 1 - dy],
            send_sem=eps_sem.at[0], recv_sem=eps_sem.at[1],
            device_id=partner(dx, dy), device_id_type=mesh_id,
        )

    ways = ((1, 0), (-1, 0), (0, 1), (0, -1))

    def side(ref, axis, v, last):
        if axis == 0:
            return ref.at[v, :, chords - 1 if last else 0]
        return ref.at[v, :, :, spans - 1 if last else 0]

    def recv_sem(stage, axis, v):
        if stage == 0:
            return state_sem.at[axis, v]
        return chord_sem if axis == 0 else flux_sem.at[v]

    def launch(stage, axis, v):
        for k in (2 * axis, 2 * axis + 1):
            dx, dy = ways[k]
            up = k % 2 == 0

            def start():
                pltpu.make_async_remote_copy(
                    src_ref=side(faces[stage][axis], axis, v, up),
                    dst_ref=side(ghosts[stage][axis], axis, v, not up),
                    send_sem=send_sem.at[stage, axis], recv_sem=recv_sem(stage, axis, v),
                    device_id=partner(dx, dy), device_id_type=mesh_id,
                ).start()

            guarded(reachable(dx), start)

    two_sided = (me_c > 0) & (me_c + 1 < chord_size)

    def await_bytes(ref, sem):
        pltpu.make_async_copy(ref, ref, sem).wait()

    def await_chord(ref, part, sem):
        pl.when(two_sided)(lambda: await_bytes(ref.at[part, :, pl.ds(0, 2)], sem))
        pl.when(jnp.logical_not(two_sided))(lambda: await_bytes(ref.at[part, :, pl.ds(0, 1)], sem))

    def await_eps(sem):
        pl.when(two_sided)(lambda: await_bytes(work.at[pl.ds(0, 8)], sem))
        pl.when(jnp.logical_not(two_sided))(lambda: await_bytes(work.at[pl.ds(0, 5)], sem))

    every = pl.ds(0, count)

    def all_sent(stage):
        await_chord(faces[stage][0], every, send_sem.at[stage, 0])
        await_bytes(faces[stage][1].at[:, :, :, pl.ds(0, 2)], send_sem.at[stage, 1])

    masks = [row_masks(axis, chords, spans, lanes) for axis in range(2)]

    def form_traces(axis, v):
        low = masks[axis][0]
        ends = [jnp.where(low, float(LEFT[i]), float(RIGHT[i])) for i in range(5)]
        out = whole(faces[0][axis])
        for q in range(5):
            for j in range(5):
                pts = points(axis, q, j)
                out[v, 5 * q + j] = total_of([e * state[v, p] for e, p in zip(ends, pts)])

    with jax.named_scope("load0"):
        load(0, 1).wait()
    with jax.named_scope("sensor"):
        form_traces(1, 0)
        eps = sensor(lambda p: state[0, p], work)
        eps_out[...] = eps
        around[1, 1] = eps
    with jax.named_scope("barrier"):
        pl.semaphore_wait(barrier, 2 + 3 * jnp.where(two_sided, 2, 1))
    for dx, dy in offsets:
        guarded(reachable(dx), lambda dx=dx, dy=dy: eps_copy(dx, dy).start())
    launch(0, 1, 0)
    with jax.named_scope("later"):
        load(1, count - 1).wait()

        def span_traces(v, carry):
            form_traces(1, v)
            launch(0, 1, v)
            return carry

        lax.fori_loop(1, count, span_traces, 0)

        def chord_traces(v, carry):
            form_traces(0, v)
            launch(0, 0, v)
            return carry

        lax.fori_loop(0, count, chord_traces, 0)

    lane = lax.broadcasted_iota(jnp.int32, (rows, lanes), 1)
    first, last = lane == 0, lane == lanes - 1

    def normal_gradient(v, carry):
        for q in range(5):
            for j in range(5):
                pts = points(2, q, j)
                parts = fold([state[v, p] for p in pts])
                left, right = traces(parts)
                before = jnp.where(first, left, rolled(right, 1, 1))
                after = jnp.where(last, right, rolled(left, -1, 1))
                for p, value in zip(pts, slope(parts, before, after)):
                    grad[v, p] = value
        return carry

    with jax.named_scope("ngrad"):
        lax.fori_loop(0, count, normal_gradient, 0)

    row = lax.broadcasted_iota(jnp.int32, (rows, lanes), 0)
    with jax.named_scope("epswait"):
        await_eps(eps_sem.at[1])

    have_low = jnp.where(me_c > 0, spans, 0)
    have_high = jnp.where(me_c + 1 < chord_size, rows, rows - spans)
    low_s, high_s = masks[1]
    low_c, high_c = masks[0]
    closed_low = row < spans - have_low
    closed_high = row >= have_high
    closed = closed_low | closed_high
    column = []
    for x in range(3):
        mine, left, right = around[x, 1], around[x, 0], around[x, 2]
        column.append([
            jnp.where(low_s, rolled(left, 1 - spans, 0), rolled(mine, 1, 0)),
            mine,
            jnp.where(high_s, rolled(right, spans - 1, 0), rolled(mine, -1, 0)),
        ])
    neighbours = [[], [], []]
    for y in range(3):
        inner = column[1][y]
        below = jnp.where(low_c, rolled(column[0][y], spans, 0), rolled(inner, spans, 0))
        above = jnp.where(high_c, rolled(column[2][y], -spans, 0), rolled(inner, -spans, 0))
        neighbours[0].append(jnp.where(closed_low, 0.0, below))
        neighbours[1].append(inner)
        neighbours[2].append(jnp.where(closed_high, 0.0, above))
    interpolate(neighbours, nu)

    shut = jnp.where(closed, -1.0, 0.0)

    def across(axis, v):
        low, high = masks[axis]
        step = spans if axis == 0 else 1
        mine, ghost = whole(faces[0][axis]), whole(ghosts[0][axis])
        out = whole(faces[1][axis])
        for q in range(5):
            for j in range(5):
                f = 5 * q + j
                pts = points(axis, q, j)
                parts = fold([state[v, p] for p in pts])
                left, right = traces(parts)
                beyond = ghost[v, f]
                if axis == 0:
                    beyond = jnp.where(closed, mine[v, f], beyond)
                before = jnp.where(low, beyond, rolled(right, step, 0))
                after = jnp.where(high, beyond, rolled(left, -step, 0))
                gradient = slope(parts, before, after)
                parts = fold([nu[p] * g for p, g in zip(pts, gradient)])
                left, right = traces(parts)
                ends = jnp.where(low, left, right)
                out[v, f] = ends
                beyond = shut * ends if axis == 0 else 0.0
                before = jnp.where(low, beyond, rolled(right, step, 0))
                after = jnp.where(high, beyond, rolled(left, -step, 0))
                for p, value in zip(pts, slope(parts, before, after)):
                    if axis == 1:
                        acc[v, p] = value
                    else:
                        acc[v, p] += value
        launch(1, axis, v)

    def normal(v):
        for q in range(5):
            for j in range(5):
                pts = points(2, q, j)
                parts = fold([nu[p] * grad[v, p] for p in pts])
                left, right = traces(parts)
                before = jnp.where(first, -left, rolled(right, 1, 1))
                after = jnp.where(last, -right, rolled(left, -1, 1))
                for p, value in zip(pts, slope(parts, before, after)):
                    acc[v, p] += value

    def variable(v, carry):
        with jax.named_scope("wait_u1"):
            await_bytes(ghosts[0][1].at[v, :, :, pl.ds(0, 2)], state_sem.at[1, v])
        with jax.named_scope("span"):
            across(1, v)
        with jax.named_scope("wait_u0"):
            await_chord(ghosts[0][0], v, state_sem.at[0, v])
        with jax.named_scope("chord"):
            across(0, v)
        with jax.named_scope("normal"):
            normal(v)
        return carry

    with jax.named_scope("fluxes"):
        lax.fori_loop(0, count, variable, 0)

    with jax.named_scope("sent0"):
        await_eps(eps_sem.at[0])
        all_sent(0)

    lifts = [
        [
            jnp.where(low, float(HALF_LEFT[i]), jnp.where(high, float(HALF_RIGHT[i]), 0.0))
            for i in range(5)
        ]
        for low, high in masks
    ]
    edges = [(low | high) for low, high in masks]
    edges[0] = edges[0] & jnp.logical_not(closed)

    def correct(v, carry):
        with jax.named_scope("wait_f1"):
            await_bytes(ghosts[1][1].at[v, :, :, pl.ds(0, 2)], flux_sem.at[v])
        flux_c, flux_s = whole(ghosts[1][0]), whole(ghosts[1][1])
        for c in range(5):
            along = [
                [jnp.where(edges[0], flux_c[v, 5 * b + c], 0.0) for b in range(5)],
                [jnp.where(edges[1], flux_s[v, 5 * a + c], 0.0) for a in range(5)],
            ]
            for a in range(5):
                for b in range(5):
                    acc[v, 25 * a + 5 * b + c] += (
                        lifts[0][a] * along[0][b] + lifts[1][b] * along[1][a]
                    )
        return carry

    with jax.named_scope("wait_f0"):
        await_chord(ghosts[1][0], every, chord_sem)
    with jax.named_scope("correct"):
        lax.fori_loop(0, count, correct, 0)
    with jax.named_scope("sent1"):
        all_sent(1)


def finish_kernel(acc, nu, residual_out, nu_out, sems):
    copies = [
        pltpu.make_async_copy(acc.at[v], residual_out.at[v], sems.at[v])
        for v in range(acc.shape[0])
    ]
    copies.append(pltpu.make_async_copy(nu, nu_out, sems.at[acc.shape[0]]))
    for copy in copies:
        copy.start()
    for copy in copies:
        copy.wait()


def shards(state):
    count, npts, chords, spans, lanes = state.shape
    rows = chords * spans
    flat = state.reshape(count, npts, rows, lanes)
    f32 = jnp.float32
    sizes = (lax.axis_size("chord"), lax.axis_size("span"))

    def full(*shape):
        return jax.ShapeDtypeStruct(shape, f32)

    vmem = pl.BlockSpec(memory_space=pltpu.VMEM)
    nu, residual = pl.pallas_call(
        functools.partial(local_kernel, sizes, count, chords, spans),
        in_specs=[pl.BlockSpec(memory_space=pltpu.HBM)],
        out_specs=[vmem, vmem],
        out_shape=[full(npts, rows, lanes), full(count, npts, rows, lanes)],
        scratch_shapes=[
            pltpu.VMEM(shape, f32)
            for shape in [
                (count, npts, rows, lanes),
                (count, npts, rows, lanes),
                (3, 3, rows, lanes),
                (npts, rows, lanes),
                (rows, lanes),
            ]
            + [(count, 25, chords, spans, lanes)] * 8
        ]
        + [
            pltpu.SemaphoreType.DMA((2,)),
            pltpu.SemaphoreType.DMA((2,)),
            pltpu.SemaphoreType.DMA((2, 2)),
            pltpu.SemaphoreType.DMA((2, count)),
            pltpu.SemaphoreType.DMA((count,)),
            pltpu.SemaphoreType.DMA,
        ],
        compiler_params=pltpu.CompilerParams(
            collective_id=0, has_side_effects=True, vmem_limit_bytes=VMEM_BYTES
        ),
    )(flat)
    hbm = pl.BlockSpec(memory_space=pltpu.HBM)
    residual, nu = pl.pallas_call(
        finish_kernel,
        in_specs=[vmem, vmem],
        out_specs=[hbm, hbm],
        out_shape=[full(count, npts, rows, lanes), full(npts, rows, lanes)],
        scratch_shapes=[pltpu.SemaphoreType.DMA((count + 1,))],
        compiler_params=pltpu.CompilerParams(vmem_limit_bytes=FINISH_BYTES),
    )(residual, nu)
    return residual.reshape(state.shape), nu.reshape(npts, chords, spans, lanes)


def solution(mesh):
    in_specs = (P(None, None, "chord", "span", None),)
    out_specs = (P(None, None, "chord", "span", None), P(None, "chord", "span", None))
    return jax.shard_map(shards, mesh=mesh, in_specs=in_specs, out_specs=out_specs, check_vma=False)
```

```python
import functools
import math

import jax
import jax.numpy as jnp
import numpy as np
from jax import lax
from jax.experimental import pallas as pl
from jax.experimental.pallas import tpu as pltpu
from jax.sharding import PartitionSpec as P

VMEM_BYTES = 52_500_000
FINISH_BYTES = 8_000_000
EPS_SCALE = 0.01
SENSOR_CENTRE = -3.0
SENSOR_WIDTH = 1.5
RATIO_FLOOR = 1e-06
ENERGY_EPS = 1e-06
GAUSS_NODES = [-0.906179845938664, -0.5384693101056831, 0.0, 0.5384693101056831, 0.906179845938664]
GAUSS_WEIGHTS = [
    0.2369268850561891,
    0.4786286704993665,
    0.5688888888888889,
    0.4786286704993665,
    0.2369268850561891,
]


def legendre_values(points):
    values = [np.ones(points.shape), np.array(points)]
    for order in range(1, 5):
        values.append(
            ((2 * order + 1) * points * values[order] - order * values[order - 1]) / (order + 1)
        )
    return values


def line_tables():
    line_nodes = np.array(GAUSS_NODES)
    quadrature_weights = np.array(GAUSS_WEIGHTS)
    barycentric = np.array(
        [
            1.0 / np.prod([line_nodes[j] - line_nodes[k] for k in range(5) if k != j])
            for j in range(5)
        ]
    )
    derivative = np.zeros((5, 5))
    for i in range(5):
        for j in range(5):
            if i != j:
                derivative[i, j] = barycentric[j] / barycentric[i] / (line_nodes[i] - line_nodes[j])
        derivative[i, i] = -np.sum(derivative[i])
    left_values = np.ones(5)
    right_values = np.ones(5)
    for j in range(5):
        for k in range(5):
            if k != j:
                left_values[j] *= (-1.0 - line_nodes[k]) / (line_nodes[j] - line_nodes[k])
                right_values[j] *= (1.0 - line_nodes[k]) / (line_nodes[j] - line_nodes[k])
    legendre = legendre_values(line_nodes)
    fourth_slope = 7.0 * legendre[3] + 3.0 * legendre[1]
    fifth_slope = 9.0 * legendre[4] + 5.0 * legendre[2] + legendre[0]
    left_corr = 0.5 * (fourth_slope - fifth_slope)
    right_corr = 0.5 * (fourth_slope + fifth_slope)
    modal = np.zeros((5, 5))
    for k in range(5):
        modal[k, :] = quadrature_weights * math.sqrt((2 * k + 1) / 2.0) * legendre[k]
    return (line_nodes, derivative, left_values, right_values, left_corr, right_corr, modal)


NODES, DERIV, LEFT, RIGHT, LIFT_LEFT, LIFT_RIGHT, MODAL = line_tables()
HALF_LEFT = 0.5 * LIFT_LEFT
HALF_RIGHT = 0.5 * LIFT_RIGHT


def fold(u):
    return (u[0] + u[4], u[1] + u[3], u[2], u[0] - u[4], u[1] - u[3])


def traces(parts):
    s0, s1, mid, d0, d1 = parts
    r = [float(x) for x in RIGHT]
    even = 0.5 * (r[0] + r[4]) * s0 + 0.5 * (r[1] + r[3]) * s1 + r[2] * mid
    odd = 0.5 * (r[0] - r[4]) * d0 + 0.5 * (r[1] - r[3]) * d1
    return even - odd, even + odd


def slope(parts, before, after):
    s0, s1, mid, d0, d1 = parts
    h = [float(x) for x in HALF_LEFT]
    r = [float(x) for x in RIGHT]
    if before is not None:
        diff, both = before - after, before + after
    even, odd = [], []
    for i in range(3):
        lift = 0.5 * (h[i] + h[4 - i])
        value = (
            float(0.5 * (DERIV[i, 0] - DERIV[i, 4]) + lift * (r[0] - r[4])) * d0
            + float(0.5 * (DERIV[i, 1] - DERIV[i, 3]) + lift * (r[1] - r[3])) * d1
        )
        even.append(value if before is None else value + lift * diff)
    for i in range(2):
        lift = 0.5 * (h[i] - h[4 - i])
        value = (
            float(0.5 * (DERIV[i, 0] + DERIV[i, 4]) - lift * (r[0] + r[4])) * s0
            + float(0.5 * (DERIV[i, 1] + DERIV[i, 3]) - lift * (r[1] + r[3])) * s1
            + float(DERIV[i, 2] - 2.0 * lift * r[2]) * mid
        )
        odd.append(value if before is None else value + lift * both)
    return [even[0] + odd[0], even[1] + odd[1], even[2], even[1] - odd[1], even[0] - odd[0]]


def points(axis, q, j):
    if axis == 0:
        return [25 * i + 5 * q + j for i in range(5)]
    if axis == 1:
        return [25 * q + 5 * i + j for i in range(5)]
    return [25 * q + 5 * j + i for i in range(5)]


def modal_line(u):
    s0, s1, mid, d0, d1 = fold(u)
    out = []
    for k in range(5):
        m = [float(x) for x in MODAL[k]]
        out.append(m[0] * s0 + m[1] * s1 + m[2] * mid if k % 2 == 0 else m[0] * d0 + m[1] * d1)
    return out


def sensor(load, work):
    def first(q, carry):
        for j in range(5):
            pts = points(0, q, j)
            for i, value in zip(pts, modal_line([load(p) for p in pts])):
                work[i] = value
        return carry

    lax.fori_loop(0, 5, first, 0)

    def second(q, carry):
        total, high = carry
        plane = {}
        for c in range(5):
            for b, value in enumerate(modal_line([work[25 * q + 5 * b + c] for b in range(5)])):
                plane[b, c] = value
        low = jnp.zeros_like(total)
        edge = jnp.zeros_like(total)
        for b in range(5):
            line = modal_line([plane[b, c] for c in range(5)])
            squares = [x * x for x in line]
            if b < 4:
                low = low + ((squares[0] + squares[1]) + (squares[2] + squares[3]))
                edge = edge + squares[4]
            else:
                edge = edge + ((squares[0] + squares[1]) + (squares[2] + squares[3])) + squares[4]
        plane_total = low + edge
        return total + plane_total, high + jnp.where(q == 4, plane_total, edge)

    zero = jnp.zeros(work.shape[1:], jnp.float32)
    total, high = lax.fori_loop(0, 5, second, (zero, zero))
    level = jnp.log(jnp.maximum(high / (total + ENERGY_EPS), RATIO_FLOOR)) * (1.0 / math.log(10.0))
    ramp = jnp.clip((level - SENSOR_CENTRE) / SENSOR_WIDTH, -1.0, 1.0)
    return EPS_SCALE * 0.5 * (1.0 + jnp.sin(0.5 * math.pi * ramp))


def rolled(value, shift, axis):
    size = value.shape[axis]
    return pltpu.roll(value, shift % size, axis)


LOWER = [float((1.0 - x) / 2.0) for x in NODES]
UPPER = [float((1.0 + x) / 2.0) for x in NODES]


def along_lanes(line):
    lanes = line.shape[1]
    lane = lax.broadcasted_iota(jnp.int32, line.shape, 1)
    before = jnp.where(lane == 0, 0.0, rolled(line, 1, 1))
    after = jnp.where(lane == lanes - 1, 0.0, rolled(line, -1, 1))
    return jnp.maximum(line, before), jnp.maximum(line, after)


def interpolate(neighbours, nu):
    corner = {}
    for x in range(2):
        for y in range(2):
            line = jnp.maximum(
                jnp.maximum(neighbours[x][y], neighbours[x + 1][y]),
                jnp.maximum(neighbours[x][y + 1], neighbours[x + 1][y + 1]),
            )
            corner[x, y, 0], corner[x, y, 1] = along_lanes(line)
    lower, upper = LOWER, UPPER
    for a in range(5):
        face = {
            (y, z): lower[a] * corner[0, y, z] + upper[a] * corner[1, y, z]
            for y in range(2)
            for z in range(2)
        }
        for b in range(5):
            edge = [lower[b] * face[0, z] + upper[b] * face[1, z] for z in range(2)]
            for c in range(5):
                nu[25 * a + 5 * b + c] = lower[c] * edge[0] + upper[c] * edge[1]


def row_masks(axis, chords, spans, lanes):
    row = lax.broadcasted_iota(jnp.int32, (chords * spans, lanes), 0)
    if axis == 0:
        return row < spans, row >= (chords - 1) * spans
    place = row % spans
    return place == 0, place == spans - 1


def total_of(values):
    out = values[0]
    for value in values[1:]:
        out = out + value
    return out


def local_kernel(sizes, count, chords, spans, *refs):
    state_hbm = refs[0]
    nu, acc = refs[1:3]
    state, grad, around, work, eps_out = refs[3:8]
    faces = (refs[8:10], refs[10:12])
    ghosts = (refs[12:14], refs[14:16])
    load_sem, eps_sem, send_sem, state_sem, flux_sem, chord_sem, answer = refs[16:]
    rows, lanes = nu.shape[1:]
    chord_size, span_size = sizes
    me_c, me_s = lax.axis_index("chord"), lax.axis_index("span")
    mesh_id = pl.DeviceIdType.MESH

    def whole(ref):
        return ref.reshape(count, 25, rows, lanes)

    def load(first, size):
        part = pl.ds(first, size)
        return pltpu.make_async_copy(
            state_hbm.at[part], state.at[part], load_sem.at[min(first, 1)]
        )

    load(0, 1).start()
    load(1, count - 1).start()

    def reachable(dx):
        if dx == 0:
            return None
        return me_c + 1 < chord_size if dx == 1 else me_c > 0

    def guarded(cond, run):
        if cond is None:
            run()
        else:
            pl.when(cond)(run)

    def partner(dx, dy):
        return (me_c + dx, lax.rem(me_s + dy + span_size, span_size))

    level = ((0, -1), (0, 1))
    lower, upper = (tuple((dx, dy) for dy in (0, -1, 1)) for dx in (-1, 1))

    def greet(sem, offsets):
        for dx, dy in offsets:
            pl.semaphore_signal(sem, inc=1, device_id=partner(dx, dy), device_id_type=mesh_id)

    barrier = pltpu.get_barrier_semaphore()
    greet(barrier, level)
    guarded(reachable(1), lambda: greet(barrier, upper))

    def eps_copy(dx, dy):
        return pltpu.make_async_remote_copy(
            src_ref=eps_out, dst_ref=around.at[1 - dx, 1 - dy],
            send_sem=eps_sem.at[0], recv_sem=eps_sem.at[1 if dx == 0 else 2],
            device_id=partner(dx, dy), device_id_type=mesh_id,
        )

    def column_copy():
        return pltpu.make_async_remote_copy(
            src_ref=around.at[1], dst_ref=around.at[0],
            send_sem=eps_sem.at[0], recv_sem=eps_sem.at[2],
            device_id=partner(1, 0), device_id_type=mesh_id,
        )

    ways = ((1, 0), (-1, 0), (0, 1), (0, -1))

    def side(ref, axis, v, last, part):
        if axis == 0:
            return ref.at[v, part, chords - 1 if last else 0]
        return ref.at[v, part, :, spans - 1 if last else 0]

    def recv_sem(stage, axis, v):
        if stage == 0:
            return state_sem.at[axis, v]
        return chord_sem if axis == 0 else flux_sem.at[v]

    def send_eps(offsets):
        for dx, dy in offsets:
            eps_copy(dx, dy).start()

    def launch(stage, axis, v, sides=(0, 1), part=pl.ds(0, 25)):
        for k in (2 * axis + i for i in sides):
            dx, dy = ways[k]
            up = k % 2 == 0

            def start():
                pltpu.make_async_remote_copy(
                    src_ref=side(faces[stage][axis], axis, v, up, part),
                    dst_ref=side(ghosts[stage][axis], axis, v, not up, part),
                    send_sem=send_sem.at[stage, axis], recv_sem=recv_sem(stage, axis, v),
                    device_id=partner(dx, dy), device_id_type=mesh_id,
                ).start()

            guarded(reachable(dx), start)

    two_sided = (me_c > 0) & (me_c + 1 < chord_size)

    def await_bytes(ref, sem):
        pltpu.make_async_copy(ref, ref, sem).wait()

    def await_chord(ref, part, sem):
        pl.when(two_sided)(lambda: await_bytes(ref.at[part, :, pl.ds(0, 2)], sem))
        pl.when(jnp.logical_not(two_sided))(lambda: await_bytes(ref.at[part, :, pl.ds(0, 1)], sem))

    def await_eps(sem, base):
        pl.when(two_sided)(lambda: await_bytes(work.at[pl.ds(0, base + 6)], sem))
        pl.when(jnp.logical_not(two_sided))(
            lambda: await_bytes(work.at[pl.ds(0, base + 3)], sem)
        )

    every = pl.ds(0, count)

    def all_sent(stage):
        await_chord(faces[stage][0], every, send_sem.at[stage, 0])
        await_bytes(faces[stage][1].at[:, :, :, pl.ds(0, 2)], send_sem.at[stage, 1])

    masks = [row_masks(axis, chords, spans, lanes) for axis in range(2)]

    def form_traces(axis, v, lines=range(5)):
        low = masks[axis][0]
        ends = [jnp.where(low, float(LEFT[i]), float(RIGHT[i])) for i in range(5)]
        out = whole(faces[0][axis])
        for q in lines:
            for j in range(5):
                pts = points(axis, q, j)
                out[v, 5 * q + j] = total_of([e * state[v, p] for e, p in zip(ends, pts)])

    with jax.named_scope("load0"):
        load(0, 1).wait()
    form_traces(1, 0, range(2))
    with jax.named_scope("barrier"):
        pl.semaphore_wait(barrier, 2 + jnp.where(me_c > 0, 3, 0))
    launch(0, 1, 0, part=pl.ds(0, 10))
    guarded(reachable(-1), lambda: greet(answer, ((-1, 0),)))
    with jax.named_scope("sensor"):
        eps = sensor(lambda p: state[0, p], work)
        eps_out[...] = eps
        around[1, 1] = eps
    send_eps(level)
    guarded(reachable(-1), lambda: send_eps(lower))
    form_traces(1, 0, range(2, 5))
    launch(0, 1, 0, part=pl.ds(10, 15))
    with jax.named_scope("later"):
        load(1, count - 1).wait()

        def span_traces(v, carry):
            form_traces(1, v)
            launch(0, 1, v)
            return carry

        lax.fori_loop(1, count, span_traces, 0)

        def chord_traces(v, carry):
            form_traces(0, v)
            launch(0, 0, v, (1,))
            return carry

        lax.fori_loop(0, count, chord_traces, 0)

    lane = lax.broadcasted_iota(jnp.int32, (rows, lanes), 1)
    first, last = lane == 0, lane == lanes - 1

    def normal_gradient(v, carry):
        for q in range(5):
            for j in range(5):
                pts = points(2, q, j)
                parts = fold([state[v, p] for p in pts])
                left, right = traces(parts)
                before = jnp.where(first, left, rolled(right, 1, 1))
                after = jnp.where(last, right, rolled(left, -1, 1))
                for p, value in zip(pts, slope(parts, before, after)):
                    grad[v, p] = value
        return carry

    with jax.named_scope("ngrad"):
        lax.fori_loop(0, count, normal_gradient, 0)

    with jax.named_scope("level"):
        await_bytes(work.at[pl.ds(0, 2)], eps_sem.at[1])
    with jax.named_scope("answer"):

        @pl.when(reachable(1))
        def _():
            pl.semaphore_wait(answer, 1)
            column_copy().start()

        def chord_up(v, carry):
            launch(0, 0, v, (0,))
            return carry

        lax.fori_loop(0, count, chord_up, 0)

    row = lax.broadcasted_iota(jnp.int32, (rows, lanes), 0)
    with jax.named_scope("epswait"):
        await_eps(eps_sem.at[2], 0)

    have_low = jnp.where(me_c > 0, spans, 0)
    have_high = jnp.where(me_c + 1 < chord_size, rows, rows - spans)
    low_s, high_s = masks[1]
    low_c, high_c = masks[0]
    closed_low = row < spans - have_low
    closed_high = row >= have_high
    closed = closed_low | closed_high
    column = []
    for x in range(3):
        mine, left, right = around[x, 1], around[x, 0], around[x, 2]
        column.append([
            jnp.where(low_s, rolled(left, 1 - spans, 0), rolled(mine, 1, 0)),
            mine,
            jnp.where(high_s, rolled(right, spans - 1, 0), rolled(mine, -1, 0)),
        ])
    neighbours = [[], [], []]
    for y in range(3):
        inner = column[1][y]
        below = jnp.where(low_c, rolled(column[0][y], spans, 0), rolled(inner, spans, 0))
        above = jnp.where(high_c, rolled(column[2][y], -spans, 0), rolled(inner, -spans, 0))
        neighbours[0].append(jnp.where(closed_low, 0.0, below))
        neighbours[1].append(inner)
        neighbours[2].append(jnp.where(closed_high, 0.0, above))
    interpolate(neighbours, nu)

    shut = jnp.where(closed, -1.0, 0.0)

    def across(axis, v):
        low, high = masks[axis]
        step = spans if axis == 0 else 1
        mine, ghost = whole(faces[0][axis]), whole(ghosts[0][axis])
        out = whole(faces[1][axis])
        for q in range(5):
            for j in range(5):
                f = 5 * q + j
                pts = points(axis, q, j)
                parts = fold([state[v, p] for p in pts])
                left, right = traces(parts)
                beyond = ghost[v, f]
                if axis == 0:
                    beyond = jnp.where(closed, mine[v, f], beyond)
                before = jnp.where(low, beyond, rolled(right, step, 0))
                after = jnp.where(high, beyond, rolled(left, -step, 0))
                gradient = slope(parts, before, after)
                parts = fold([nu[p] * g for p, g in zip(pts, gradient)])
                left, right = traces(parts)
                ends = jnp.where(low, left, right)
                out[v, f] = ends
                beyond = shut * ends if axis == 0 else 0.0
                before = jnp.where(low, beyond, rolled(right, step, 0))
                after = jnp.where(high, beyond, rolled(left, -step, 0))
                for p, value in zip(pts, slope(parts, before, after)):
                    if axis == 1:
                        acc[v, p] = value
                    else:
                        acc[v, p] += value
        launch(1, axis, v)

    def normal(v):
        for q in range(5):
            for j in range(5):
                pts = points(2, q, j)
                parts = fold([nu[p] * grad[v, p] for p in pts])
                left, right = traces(parts)
                before = jnp.where(first, -left, rolled(right, 1, 1))
                after = jnp.where(last, -right, rolled(left, -1, 1))
                for p, value in zip(pts, slope(parts, before, after)):
                    acc[v, p] += value

    def variable(v, carry):
        with jax.named_scope("wait_u1"):
            await_bytes(ghosts[0][1].at[v, :, :, pl.ds(0, 2)], state_sem.at[1, v])
        with jax.named_scope("span"):
            across(1, v)
        with jax.named_scope("wait_u0"):
            await_chord(ghosts[0][0], v, state_sem.at[0, v])
        with jax.named_scope("chord"):
            across(0, v)
        return carry

    with jax.named_scope("fluxes"):
        lax.fori_loop(0, count, variable, 0)

    def rest(v, carry):
        normal(v)
        return carry

    with jax.named_scope("normal"):
        lax.fori_loop(0, count, rest, 0)

    with jax.named_scope("sent0"):
        await_eps(eps_sem.at[0], 2)
        all_sent(0)

    lifts = [
        [
            jnp.where(low, float(HALF_LEFT[i]), jnp.where(high, float(HALF_RIGHT[i]), 0.0))
            for i in range(5)
        ]
        for low, high in masks
    ]
    edges = [(low | high) for low, high in masks]
    edges[0] = edges[0] & jnp.logical_not(closed)

    def correct(v, carry):
        with jax.named_scope("wait_f1"):
            await_bytes(ghosts[1][1].at[v, :, :, pl.ds(0, 2)], flux_sem.at[v])
        flux_c, flux_s = whole(ghosts[1][0]), whole(ghosts[1][1])
        for c in range(5):
            along = [
                [jnp.where(edges[0], flux_c[v, 5 * b + c], 0.0) for b in range(5)],
                [jnp.where(edges[1], flux_s[v, 5 * a + c], 0.0) for a in range(5)],
            ]
            for a in range(5):
                for b in range(5):
                    acc[v, 25 * a + 5 * b + c] += (
                        lifts[0][a] * along[0][b] + lifts[1][b] * along[1][a]
                    )
        return carry

    with jax.named_scope("wait_f0"):
        await_chord(ghosts[1][0], every, chord_sem)
    with jax.named_scope("correct"):
        lax.fori_loop(0, count, correct, 0)
    with jax.named_scope("sent1"):
        all_sent(1)


def finish_kernel(acc, nu, residual_out, nu_out, sems):
    copies = [
        pltpu.make_async_copy(acc.at[v], residual_out.at[v], sems.at[v])
        for v in range(acc.shape[0])
    ]
    copies.append(pltpu.make_async_copy(nu, nu_out, sems.at[acc.shape[0]]))
    for copy in copies:
        copy.start()
    for copy in copies:
        copy.wait()


def shards(state):
    count, npts, chords, spans, lanes = state.shape
    rows = chords * spans
    flat = state.reshape(count, npts, rows, lanes)
    f32 = jnp.float32
    sizes = (lax.axis_size("chord"), lax.axis_size("span"))

    def full(*shape):
        return jax.ShapeDtypeStruct(shape, f32)

    vmem = pl.BlockSpec(memory_space=pltpu.VMEM)
    nu, residual = pl.pallas_call(
        functools.partial(local_kernel, sizes, count, chords, spans),
        in_specs=[pl.BlockSpec(memory_space=pltpu.HBM)],
        out_specs=[vmem, vmem],
        out_shape=[full(npts, rows, lanes), full(count, npts, rows, lanes)],
        scratch_shapes=[
            pltpu.VMEM(shape, f32)
            for shape in [
                (count, npts, rows, lanes),
                (count, npts, rows, lanes),
                (3, 3, rows, lanes),
                (npts, rows, lanes),
                (rows, lanes),
            ]
            + [(count, 25, chords, spans, lanes)] * 8
        ]
        + [
            pltpu.SemaphoreType.DMA((2,)),
            pltpu.SemaphoreType.DMA((3,)),
            pltpu.SemaphoreType.DMA((2, 2)),
            pltpu.SemaphoreType.DMA((2, count)),
            pltpu.SemaphoreType.DMA((count,)),
            pltpu.SemaphoreType.DMA,
            pltpu.SemaphoreType.REGULAR,
        ],
        compiler_params=pltpu.CompilerParams(
            collective_id=0, has_side_effects=True, vmem_limit_bytes=VMEM_BYTES
        ),
    )(flat)
    hbm = pl.BlockSpec(memory_space=pltpu.HBM)
    residual, nu = pl.pallas_call(
        finish_kernel,
        in_specs=[vmem, vmem],
        out_specs=[hbm, hbm],
        out_shape=[full(count, npts, rows, lanes), full(npts, rows, lanes)],
        scratch_shapes=[pltpu.SemaphoreType.DMA((count + 1,))],
        compiler_params=pltpu.CompilerParams(vmem_limit_bytes=FINISH_BYTES),
    )(residual, nu)
    return residual.reshape(state.shape), nu.reshape(npts, chords, spans, lanes)


def solution(mesh):
    in_specs = (P(None, None, "chord", "span", None),)
    out_specs = (P(None, None, "chord", "span", None), P(None, "chord", "span", None))
    return jax.shard_map(shards, mesh=mesh, in_specs=in_specs, out_specs=out_specs, check_vma=False)
```

```python
import functools
import math

import jax
import jax.numpy as jnp
import numpy as np
from jax import lax
from jax.experimental import pallas as pl
from jax.experimental.pallas import tpu as pltpu
from jax.sharding import PartitionSpec as P

VMEM_BYTES = 52_500_000
FINISH_BYTES = 8_000_000
LAG = 3
EPS_SCALE = 0.01
SENSOR_CENTRE = -3.0
SENSOR_WIDTH = 1.5
RATIO_FLOOR = 1e-06
ENERGY_EPS = 1e-06
GAUSS_NODES = [-0.906179845938664, -0.5384693101056831, 0.0, 0.5384693101056831, 0.906179845938664]
GAUSS_WEIGHTS = [
    0.2369268850561891,
    0.4786286704993665,
    0.5688888888888889,
    0.4786286704993665,
    0.2369268850561891,
]


def legendre_values(points):
    values = [np.ones(points.shape), np.array(points)]
    for order in range(1, 5):
        values.append(
            ((2 * order + 1) * points * values[order] - order * values[order - 1]) / (order + 1)
        )
    return values


def line_tables():
    line_nodes = np.array(GAUSS_NODES)
    quadrature_weights = np.array(GAUSS_WEIGHTS)
    barycentric = np.array(
        [
            1.0 / np.prod([line_nodes[j] - line_nodes[k] for k in range(5) if k != j])
            for j in range(5)
        ]
    )
    derivative = np.zeros((5, 5))
    for i in range(5):
        for j in range(5):
            if i != j:
                derivative[i, j] = barycentric[j] / barycentric[i] / (line_nodes[i] - line_nodes[j])
        derivative[i, i] = -np.sum(derivative[i])
    left_values = np.ones(5)
    right_values = np.ones(5)
    for j in range(5):
        for k in range(5):
            if k != j:
                left_values[j] *= (-1.0 - line_nodes[k]) / (line_nodes[j] - line_nodes[k])
                right_values[j] *= (1.0 - line_nodes[k]) / (line_nodes[j] - line_nodes[k])
    legendre = legendre_values(line_nodes)
    fourth_slope = 7.0 * legendre[3] + 3.0 * legendre[1]
    fifth_slope = 9.0 * legendre[4] + 5.0 * legendre[2] + legendre[0]
    left_corr = 0.5 * (fourth_slope - fifth_slope)
    right_corr = 0.5 * (fourth_slope + fifth_slope)
    modal = np.zeros((5, 5))
    for k in range(5):
        modal[k, :] = quadrature_weights * math.sqrt((2 * k + 1) / 2.0) * legendre[k]
    return (line_nodes, derivative, left_values, right_values, left_corr, right_corr, modal)


NODES, DERIV, LEFT, RIGHT, LIFT_LEFT, LIFT_RIGHT, MODAL = line_tables()
HALF_LEFT = 0.5 * LIFT_LEFT
HALF_RIGHT = 0.5 * LIFT_RIGHT


def fold(u):
    return (u[0] + u[4], u[1] + u[3], u[2], u[0] - u[4], u[1] - u[3])


def traces(parts):
    s0, s1, mid, d0, d1 = parts
    r = [float(x) for x in RIGHT]
    even = 0.5 * (r[0] + r[4]) * s0 + 0.5 * (r[1] + r[3]) * s1 + r[2] * mid
    odd = 0.5 * (r[0] - r[4]) * d0 + 0.5 * (r[1] - r[3]) * d1
    return even - odd, even + odd


def slope(parts, before, after):
    s0, s1, mid, d0, d1 = parts
    h = [float(x) for x in HALF_LEFT]
    r = [float(x) for x in RIGHT]
    if before is not None:
        diff, both = before - after, before + after
    even, odd = [], []
    for i in range(3):
        lift = 0.5 * (h[i] + h[4 - i])
        value = (
            float(0.5 * (DERIV[i, 0] - DERIV[i, 4]) + lift * (r[0] - r[4])) * d0
            + float(0.5 * (DERIV[i, 1] - DERIV[i, 3]) + lift * (r[1] - r[3])) * d1
        )
        even.append(value if before is None else value + lift * diff)
    for i in range(2):
        lift = 0.5 * (h[i] - h[4 - i])
        value = (
            float(0.5 * (DERIV[i, 0] + DERIV[i, 4]) - lift * (r[0] + r[4])) * s0
            + float(0.5 * (DERIV[i, 1] + DERIV[i, 3]) - lift * (r[1] + r[3])) * s1
            + float(DERIV[i, 2] - 2.0 * lift * r[2]) * mid
        )
        odd.append(value if before is None else value + lift * both)
    return [even[0] + odd[0], even[1] + odd[1], even[2], even[1] - odd[1], even[0] - odd[0]]


def points(axis, q, j):
    if axis == 0:
        return [25 * i + 5 * q + j for i in range(5)]
    if axis == 1:
        return [25 * q + 5 * i + j for i in range(5)]
    return [25 * q + 5 * j + i for i in range(5)]


def modal_line(u):
    s0, s1, mid, d0, d1 = fold(u)
    out = []
    for k in range(5):
        m = [float(x) for x in MODAL[k]]
        out.append(m[0] * s0 + m[1] * s1 + m[2] * mid if k % 2 == 0 else m[0] * d0 + m[1] * d1)
    return out


def sensor(load, work):
    def first(q, carry):
        for j in range(5):
            pts = points(0, q, j)
            for i, value in zip(pts, modal_line([load(p) for p in pts])):
                work[i] = value
        return carry

    lax.fori_loop(0, 5, first, 0)

    def second(q, carry):
        total, high = carry
        plane = {}
        for c in range(5):
            for b, value in enumerate(modal_line([work[25 * q + 5 * b + c] for b in range(5)])):
                plane[b, c] = value
        low = jnp.zeros_like(total)
        edge = jnp.zeros_like(total)
        for b in range(5):
            line = modal_line([plane[b, c] for c in range(5)])
            squares = [x * x for x in line]
            if b < 4:
                low = low + ((squares[0] + squares[1]) + (squares[2] + squares[3]))
                edge = edge + squares[4]
            else:
                edge = edge + ((squares[0] + squares[1]) + (squares[2] + squares[3])) + squares[4]
        plane_total = low + edge
        return total + plane_total, high + jnp.where(q == 4, plane_total, edge)

    zero = jnp.zeros(work.shape[1:], jnp.float32)
    total, high = lax.fori_loop(0, 5, second, (zero, zero))
    level = jnp.log(jnp.maximum(high / (total + ENERGY_EPS), RATIO_FLOOR)) * (1.0 / math.log(10.0))
    ramp = jnp.clip((level - SENSOR_CENTRE) / SENSOR_WIDTH, -1.0, 1.0)
    return EPS_SCALE * 0.5 * (1.0 + jnp.sin(0.5 * math.pi * ramp))


def rolled(value, shift, axis):
    size = value.shape[axis]
    return pltpu.roll(value, shift % size, axis)


LOWER = [float((1.0 - x) / 2.0) for x in NODES]
UPPER = [float((1.0 + x) / 2.0) for x in NODES]


def along_lanes(line):
    lanes = line.shape[1]
    lane = lax.broadcasted_iota(jnp.int32, line.shape, 1)
    before = jnp.where(lane == 0, 0.0, rolled(line, 1, 1))
    after = jnp.where(lane == lanes - 1, 0.0, rolled(line, -1, 1))
    return jnp.maximum(line, before), jnp.maximum(line, after)


def interpolate(neighbours, nu):
    corner = {}
    for x in range(2):
        for y in range(2):
            line = jnp.maximum(
                jnp.maximum(neighbours[x][y], neighbours[x + 1][y]),
                jnp.maximum(neighbours[x][y + 1], neighbours[x + 1][y + 1]),
            )
            corner[x, y, 0], corner[x, y, 1] = along_lanes(line)
    lower, upper = LOWER, UPPER
    for a in range(5):
        face = {
            (y, z): lower[a] * corner[0, y, z] + upper[a] * corner[1, y, z]
            for y in range(2)
            for z in range(2)
        }
        for b in range(5):
            edge = [lower[b] * face[0, z] + upper[b] * face[1, z] for z in range(2)]
            for c in range(5):
                nu[25 * a + 5 * b + c] = lower[c] * edge[0] + upper[c] * edge[1]


def row_masks(axis, chords, spans, lanes):
    row = lax.broadcasted_iota(jnp.int32, (chords * spans, lanes), 0)
    if axis == 0:
        return row < spans, row >= (chords - 1) * spans
    place = row % spans
    return place == 0, place == spans - 1


def total_of(values):
    out = values[0]
    for value in values[1:]:
        out = out + value
    return out


def local_kernel(sizes, count, chords, spans, *refs):
    state_hbm = refs[0]
    nu, acc = refs[1:3]
    state, around, work, eps_out = refs[3:7]
    grads = refs[7:10]
    faces = (refs[10:12], refs[12:14])
    ghosts = (refs[14:16], refs[16:18])
    load_sem, eps_sem, send_sem, state_sem, flux_sem, chord_sem, answer = refs[18:]
    rows, lanes = nu.shape[1:]
    chord_size, span_size = sizes
    me_c, me_s = lax.axis_index("chord"), lax.axis_index("span")
    mesh_id = pl.DeviceIdType.MESH

    def whole(ref):
        return ref.reshape(count, 25, rows, lanes)

    def load(v, k, first, size):
        part = pl.ds(first, size)
        return pltpu.make_async_copy(
            state_hbm.at[v, part], state.at[v, part], load_sem.at[k]
        )

    start, remainder = load(0, 0, 0, 50), load(0, 1, 50, 75)
    others = pltpu.make_async_copy(
        state_hbm.at[pl.ds(1, count - 1)], state.at[pl.ds(1, count - 1)], load_sem.at[2]
    )
    for copy in (start, remainder, others):
        copy.start()

    def reachable(dx):
        if dx == 0:
            return None
        return me_c + 1 < chord_size if dx == 1 else me_c > 0

    def guarded(cond, run):
        if cond is None:
            run()
        else:
            pl.when(cond)(run)

    def partner(dx, dy):
        return (me_c + dx, lax.rem(me_s + dy + span_size, span_size))

    level = ((0, -1), (0, 1))
    lower, upper = (tuple((dx, dy) for dy in (0, -1, 1)) for dx in (-1, 1))

    def greet(sem, offsets):
        for dx, dy in offsets:
            pl.semaphore_signal(sem, inc=1, device_id=partner(dx, dy), device_id_type=mesh_id)

    barrier = pltpu.get_barrier_semaphore()
    greet(barrier, level)
    guarded(reachable(1), lambda: greet(barrier, upper))

    def eps_copy(dx, dy):
        return pltpu.make_async_remote_copy(
            src_ref=eps_out, dst_ref=around.at[1 - dx, 1 - dy],
            send_sem=eps_sem.at[0], recv_sem=eps_sem.at[1 if dx == 0 else 2],
            device_id=partner(dx, dy), device_id_type=mesh_id,
        )

    def column_copy():
        return pltpu.make_async_remote_copy(
            src_ref=around.at[1], dst_ref=around.at[0],
            send_sem=eps_sem.at[0], recv_sem=eps_sem.at[2],
            device_id=partner(1, 0), device_id_type=mesh_id,
        )

    ways = ((1, 0), (-1, 0), (0, 1), (0, -1))

    def side(ref, axis, v, last, part):
        if axis == 0:
            return ref.at[v, part, chords - 1 if last else 0]
        return ref.at[v, part, :, spans - 1 if last else 0]

    def recv_sem(stage, axis, v):
        if stage == 0:
            return state_sem.at[axis, v]
        return chord_sem if axis == 0 else flux_sem.at[v]

    def send_eps(offsets):
        for dx, dy in offsets:
            eps_copy(dx, dy).start()

    def launch(stage, axis, v, sides=(0, 1), part=pl.ds(0, 25), only=None):
        for k in (2 * axis + i for i in sides):
            dx, dy = ways[k]
            up = k % 2 == 0

            def start():
                pltpu.make_async_remote_copy(
                    src_ref=side(faces[stage][axis], axis, v, up, part),
                    dst_ref=side(ghosts[stage][axis], axis, v, not up, part),
                    send_sem=send_sem.at[stage, axis], recv_sem=recv_sem(stage, axis, v),
                    device_id=partner(dx, dy), device_id_type=mesh_id,
                ).start()

            allowed = reachable(dx) if only is None else only(partner(dx, dy)[1])
            guarded(allowed, start)

    def first_half(s):
        return s < span_size // 2

    def second_half(s):
        return s >= span_size // 2

    two_sided = (me_c > 0) & (me_c + 1 < chord_size)

    def await_bytes(ref, sem):
        pltpu.make_async_copy(ref, ref, sem).wait()

    def await_chord(ref, part, sem):
        pl.when(two_sided)(lambda: await_bytes(ref.at[part, :, pl.ds(0, 2)], sem))
        pl.when(jnp.logical_not(two_sided))(lambda: await_bytes(ref.at[part, :, pl.ds(0, 1)], sem))

    def await_eps(sem, base):
        pl.when(two_sided)(lambda: await_bytes(work.at[pl.ds(0, base + 6)], sem))
        pl.when(jnp.logical_not(two_sided))(
            lambda: await_bytes(work.at[pl.ds(0, base + 3)], sem)
        )

    every = pl.ds(0, count)

    def all_sent(stage):
        await_chord(faces[stage][0], every, send_sem.at[stage, 0])
        await_bytes(faces[stage][1].at[:, :, :, pl.ds(0, 2)], send_sem.at[stage, 1])

    masks = [row_masks(axis, chords, spans, lanes) for axis in range(2)]

    def form_traces(axis, v, lines=range(5)):
        low = masks[axis][0]
        ends = [jnp.where(low, float(LEFT[i]), float(RIGHT[i])) for i in range(5)]
        out = whole(faces[0][axis])
        for q in lines:
            for j in range(5):
                pts = points(axis, q, j)
                out[v, 5 * q + j] = total_of([e * state[v, p] for e, p in zip(ends, pts)])

    with jax.named_scope("load0"):
        start.wait()
    form_traces(1, 0, range(2))
    with jax.named_scope("barrier"):
        pl.semaphore_wait(barrier, 2 + jnp.where(me_c > 0, 3, 0))
    launch(0, 1, 0, part=pl.ds(0, 10))
    guarded(reachable(-1), lambda: greet(answer, ((-1, 0),)))
    with jax.named_scope("sensor"):
        remainder.wait()
        eps = sensor(lambda p: state[0, p], work)
        eps_out[...] = eps
        around[1, 1] = eps
    send_eps(level)
    guarded(reachable(-1), lambda: send_eps(lower))
    form_traces(1, 0, range(2, 5))
    launch(0, 1, 0, part=pl.ds(10, 15))
    with jax.named_scope("later"):
        others.wait()

        def span_traces(v, carry):
            form_traces(1, v)
            launch(0, 1, v)
            return carry

        lax.fori_loop(1, count, span_traces, 0)

        def chord_traces(v, carry):
            form_traces(0, v)
            launch(0, 0, v, (1,))
            return carry

        lax.fori_loop(0, count, chord_traces, 0)

    lane = lax.broadcasted_iota(jnp.int32, (rows, lanes), 1)
    first, last = lane == 0, lane == lanes - 1
    row = lax.broadcasted_iota(jnp.int32, (rows, lanes), 0)
    have_low = jnp.where(me_c > 0, spans, 0)
    have_high = jnp.where(me_c + 1 < chord_size, rows, rows - spans)
    low_s, high_s = masks[1]
    low_c, high_c = masks[0]
    closed_low = row < spans - have_low
    closed_high = row >= have_high
    closed = closed_low | closed_high
    shut = jnp.where(closed, 1.0, 0.0)

    def normal_gradient(v, carry):
        grad = grads[2]
        for q in range(5):
            for j in range(5):
                pts = points(2, q, j)
                parts = fold([state[v, p] for p in pts])
                left, right = traces(parts)
                before = jnp.where(first, left, rolled(right, 1, 1))
                after = jnp.where(last, right, rolled(left, -1, 1))
                for p, value in zip(pts, slope(parts, before, after)):
                    grad[v, p] = value
        return carry

    def across_gradient(axis):
        low, high = masks[axis]
        step = spans if axis == 0 else 1
        mine, grad = whole(faces[0][axis]), grads[axis]

        def body(v, carry):
            for q in range(5):
                for j in range(5):
                    pts = points(axis, q, j)
                    parts = fold([state[v, p] for p in pts])
                    left, right = traces(parts)
                    beyond = shut * mine[v, 5 * q + j] if axis == 0 else 0.0
                    before = jnp.where(low, beyond, rolled(right, step, 0))
                    after = jnp.where(high, beyond, rolled(left, -step, 0))
                    for p, value in zip(pts, slope(parts, before, after)):
                        grad[v, p] = value
            return carry

        return body

    with jax.named_scope("ngrad"):
        lax.fori_loop(0, count, normal_gradient, 0)
    with jax.named_scope("sgrad"):
        lax.fori_loop(0, count, across_gradient(1), 0)

    with jax.named_scope("level"):
        await_bytes(work.at[pl.ds(0, 2)], eps_sem.at[1])
    with jax.named_scope("answer"):

        @pl.when(reachable(1))
        def _():
            pl.semaphore_wait(answer, 1)
            column_copy().start()

        def chord_up(v, carry):
            launch(0, 0, v, (0,))
            return carry

        lax.fori_loop(0, count, chord_up, 0)

    with jax.named_scope("cgrad"):
        lax.fori_loop(0, count, across_gradient(0), 0)

    with jax.named_scope("epswait"):
        await_eps(eps_sem.at[2], 0)

    column = []
    for x in range(3):
        mine, left, right = around[x, 1], around[x, 0], around[x, 2]
        column.append([
            jnp.where(low_s, rolled(left, 1 - spans, 0), rolled(mine, 1, 0)),
            mine,
            jnp.where(high_s, rolled(right, spans - 1, 0), rolled(mine, -1, 0)),
        ])
    neighbours = [[], [], []]
    for y in range(3):
        inner = column[1][y]
        below = jnp.where(low_c, rolled(column[0][y], spans, 0), rolled(inner, spans, 0))
        above = jnp.where(high_c, rolled(column[2][y], -spans, 0), rolled(inner, -spans, 0))
        neighbours[0].append(jnp.where(closed_low, 0.0, below))
        neighbours[1].append(inner)
        neighbours[2].append(jnp.where(closed_high, 0.0, above))
    interpolate(neighbours, nu)

    lifts = [
        [
            jnp.where(low, float(HALF_LEFT[i]), jnp.where(high, float(HALF_RIGHT[i]), 0.0))
            for i in range(5)
        ]
        for low, high in masks
    ]
    edges = [(low | high) for low, high in masks]
    edges[0] = edges[0] & jnp.logical_not(closed)
    full_edge = (chords == 1, spans <= 2)

    def outside(ref, axis, v, f):
        value = ref[v, f]
        return value if full_edge[axis] else jnp.where(edges[axis], value, 0.0)

    def across(axis, v):
        low, high = masks[axis]
        step = spans if axis == 0 else 1
        grad, ghost, out = grads[axis], whole(ghosts[0][axis]), whole(faces[1][axis])
        for q in range(5):
            for j in range(5):
                f = 5 * q + j
                pts = points(axis, q, j)
                beyond = outside(ghost, axis, v, f)
                gradient = [grad[v, p] + lift * beyond for p, lift in zip(pts, lifts[axis])]
                parts = fold([nu[p] * g for p, g in zip(pts, gradient)])
                left, right = traces(parts)
                ends = jnp.where(low, left, right)
                out[v, f] = ends
                beyond = -shut * ends if axis == 0 else 0.0
                before = jnp.where(low, beyond, rolled(right, step, 0))
                after = jnp.where(high, beyond, rolled(left, -step, 0))
                for p, value in zip(pts, slope(parts, before, after)):
                    if axis == 1:
                        acc[v, p] = value
                    else:
                        acc[v, p] += value

    def normal(v):
        for q in range(5):
            for j in range(5):
                pts = points(2, q, j)
                parts = fold([nu[p] * grads[2][v, p] for p in pts])
                left, right = traces(parts)
                before = jnp.where(first, -left, rolled(right, 1, 1))
                after = jnp.where(last, -right, rolled(left, -1, 1))
                for p, value in zip(pts, slope(parts, before, after)):
                    acc[v, p] += value

    lag = min(LAG, count)

    def variable(v, carry):
        with jax.named_scope("wait_u1"):
            await_bytes(ghosts[0][1].at[v, :, :, pl.ds(0, 2)], state_sem.at[1, v])
        with jax.named_scope("span"):
            across(1, v)
            launch(1, 1, v, only=first_half)
        with jax.named_scope("wait_u0"):
            await_chord(ghosts[0][0], v, state_sem.at[0, v])
        with jax.named_scope("chord"):
            across(0, v)
            launch(1, 0, v)
            due = v >= lag
            launch(1, 1, jnp.maximum(v - lag, 0), only=lambda s: second_half(s) & due)
        return carry

    with jax.named_scope("fluxes"):
        lax.fori_loop(0, count, variable, 0)

    def launch_rest(v, carry):
        launch(1, 1, v, only=second_half)
        return carry

    lax.fori_loop(count - lag, count, launch_rest, 0)

    def rest(v, carry):
        normal(v)
        return carry

    with jax.named_scope("normal"):
        lax.fori_loop(0, count, rest, 0)

    with jax.named_scope("sent0"):
        await_eps(eps_sem.at[0], 2)
        all_sent(0)

    def correct(v, carry):
        with jax.named_scope("wait_f1"):
            await_bytes(ghosts[1][1].at[v, :, :, pl.ds(0, 2)], flux_sem.at[v])
        flux_c, flux_s = whole(ghosts[1][0]), whole(ghosts[1][1])
        for c in range(5):
            along = [
                [outside(flux_c, 0, v, 5 * b + c) for b in range(5)],
                [outside(flux_s, 1, v, 5 * a + c) for a in range(5)],
            ]
            for a in range(5):
                for b in range(5):
                    acc[v, 25 * a + 5 * b + c] += (
                        lifts[0][a] * along[0][b] + lifts[1][b] * along[1][a]
                    )
        return carry

    with jax.named_scope("wait_f0"):
        await_chord(ghosts[1][0], every, chord_sem)
    with jax.named_scope("correct"):
        lax.fori_loop(0, count, correct, 0)
    with jax.named_scope("sent1"):
        all_sent(1)


def finish_kernel(acc, nu, residual_out, nu_out, sems):
    copies = [
        pltpu.make_async_copy(acc.at[v], residual_out.at[v], sems.at[v])
        for v in range(acc.shape[0])
    ]
    copies.append(pltpu.make_async_copy(nu, nu_out, sems.at[acc.shape[0]]))
    for copy in copies:
        copy.start()
    for copy in copies:
        copy.wait()


def shards(state):
    count, npts, chords, spans, lanes = state.shape
    rows = chords * spans
    flat = state.reshape(count, npts, rows, lanes)
    f32 = jnp.float32
    sizes = (lax.axis_size("chord"), lax.axis_size("span"))

    def full(*shape):
        return jax.ShapeDtypeStruct(shape, f32)

    vmem = pl.BlockSpec(memory_space=pltpu.VMEM)
    nu, residual = pl.pallas_call(
        functools.partial(local_kernel, sizes, count, chords, spans),
        in_specs=[pl.BlockSpec(memory_space=pltpu.HBM)],
        out_specs=[vmem, vmem],
        out_shape=[full(npts, rows, lanes), full(count, npts, rows, lanes)],
        scratch_shapes=[
            pltpu.VMEM(shape, f32)
            for shape in [
                (count, npts, rows, lanes),
                (3, 3, rows, lanes),
                (npts, rows, lanes),
                (rows, lanes),
                (count, npts, rows, lanes),
                (count, npts, rows, lanes),
                (count, npts, rows, lanes),
            ]
            + [(count, 25, chords, spans, lanes)] * 8
        ]
        + [
            pltpu.SemaphoreType.DMA((3,)),
            pltpu.SemaphoreType.DMA((3,)),
            pltpu.SemaphoreType.DMA((2, 2)),
            pltpu.SemaphoreType.DMA((2, count)),
            pltpu.SemaphoreType.DMA((count,)),
            pltpu.SemaphoreType.DMA,
            pltpu.SemaphoreType.REGULAR,
        ],
        compiler_params=pltpu.CompilerParams(
            collective_id=0, has_side_effects=True, vmem_limit_bytes=VMEM_BYTES
        ),
    )(flat)
    hbm = pl.BlockSpec(memory_space=pltpu.HBM)
    residual, nu = pl.pallas_call(
        finish_kernel,
        in_specs=[vmem, vmem],
        out_specs=[hbm, hbm],
        out_shape=[full(count, npts, rows, lanes), full(npts, rows, lanes)],
        scratch_shapes=[pltpu.SemaphoreType.DMA((count + 1,))],
        compiler_params=pltpu.CompilerParams(vmem_limit_bytes=FINISH_BYTES),
    )(residual, nu)
    return residual.reshape(state.shape), nu.reshape(npts, chords, spans, lanes)


def solution(mesh):
    in_specs = (P(None, None, "chord", "span", None),)
    out_specs = (P(None, None, "chord", "span", None), P(None, "chord", "span", None))
    return jax.shard_map(shards, mesh=mesh, in_specs=in_specs, out_specs=out_specs, check_vma=False)
```

```python
import functools
import math

import jax
import jax.numpy as jnp
import numpy as np
from jax import lax
from jax.experimental import pallas as pl
from jax.experimental.pallas import tpu as pltpu
from jax.sharding import PartitionSpec as P

VMEM_BYTES = 52_500_000
FINISH_BYTES = 8_000_000
LAG = 3
EPS_SCALE = 0.01
SENSOR_CENTRE = -3.0
SENSOR_WIDTH = 1.5
RATIO_FLOOR = 1e-06
ENERGY_EPS = 1e-06
GAUSS_NODES = [-0.906179845938664, -0.5384693101056831, 0.0, 0.5384693101056831, 0.906179845938664]
GAUSS_WEIGHTS = [
    0.2369268850561891,
    0.4786286704993665,
    0.5688888888888889,
    0.4786286704993665,
    0.2369268850561891,
]


def legendre_values(points):
    values = [np.ones(points.shape), np.array(points)]
    for order in range(1, 5):
        values.append(
            ((2 * order + 1) * points * values[order] - order * values[order - 1]) / (order + 1)
        )
    return values


def line_tables():
    line_nodes = np.array(GAUSS_NODES)
    quadrature_weights = np.array(GAUSS_WEIGHTS)
    barycentric = np.array(
        [
            1.0 / np.prod([line_nodes[j] - line_nodes[k] for k in range(5) if k != j])
            for j in range(5)
        ]
    )
    derivative = np.zeros((5, 5))
    for i in range(5):
        for j in range(5):
            if i != j:
                derivative[i, j] = barycentric[j] / barycentric[i] / (line_nodes[i] - line_nodes[j])
        derivative[i, i] = -np.sum(derivative[i])
    left_values = np.ones(5)
    right_values = np.ones(5)
    for j in range(5):
        for k in range(5):
            if k != j:
                left_values[j] *= (-1.0 - line_nodes[k]) / (line_nodes[j] - line_nodes[k])
                right_values[j] *= (1.0 - line_nodes[k]) / (line_nodes[j] - line_nodes[k])
    legendre = legendre_values(line_nodes)
    fourth_slope = 7.0 * legendre[3] + 3.0 * legendre[1]
    fifth_slope = 9.0 * legendre[4] + 5.0 * legendre[2] + legendre[0]
    left_corr = 0.5 * (fourth_slope - fifth_slope)
    right_corr = 0.5 * (fourth_slope + fifth_slope)
    modal = np.zeros((5, 5))
    for k in range(5):
        modal[k, :] = quadrature_weights * math.sqrt((2 * k + 1) / 2.0) * legendre[k]
    return (line_nodes, derivative, left_values, right_values, left_corr, right_corr, modal)


NODES, DERIV, LEFT, RIGHT, LIFT_LEFT, LIFT_RIGHT, MODAL = line_tables()
HALF_LEFT = 0.5 * LIFT_LEFT
HALF_RIGHT = 0.5 * LIFT_RIGHT


def fold(u):
    return (u[0] + u[4], u[1] + u[3], u[2], u[0] - u[4], u[1] - u[3])


def traces(parts):
    s0, s1, mid, d0, d1 = parts
    r = [float(x) for x in RIGHT]
    even = 0.5 * (r[0] + r[4]) * s0 + 0.5 * (r[1] + r[3]) * s1 + r[2] * mid
    odd = 0.5 * (r[0] - r[4]) * d0 + 0.5 * (r[1] - r[3]) * d1
    return even - odd, even + odd


def slope(parts, before, after):
    s0, s1, mid, d0, d1 = parts
    h = [float(x) for x in HALF_LEFT]
    r = [float(x) for x in RIGHT]
    if before is not None:
        diff, both = before - after, before + after
    even, odd = [], []
    for i in range(3):
        lift = 0.5 * (h[i] + h[4 - i])
        value = (
            float(0.5 * (DERIV[i, 0] - DERIV[i, 4]) + lift * (r[0] - r[4])) * d0
            + float(0.5 * (DERIV[i, 1] - DERIV[i, 3]) + lift * (r[1] - r[3])) * d1
        )
        even.append(value if before is None else value + lift * diff)
    for i in range(2):
        lift = 0.5 * (h[i] - h[4 - i])
        value = (
            float(0.5 * (DERIV[i, 0] + DERIV[i, 4]) - lift * (r[0] + r[4])) * s0
            + float(0.5 * (DERIV[i, 1] + DERIV[i, 3]) - lift * (r[1] + r[3])) * s1
            + float(DERIV[i, 2] - 2.0 * lift * r[2]) * mid
        )
        odd.append(value if before is None else value + lift * both)
    return [even[0] + odd[0], even[1] + odd[1], even[2], even[1] - odd[1], even[0] - odd[0]]


def points(axis, q, j):
    if axis == 0:
        return [25 * i + 5 * q + j for i in range(5)]
    if axis == 1:
        return [25 * q + 5 * i + j for i in range(5)]
    return [25 * q + 5 * j + i for i in range(5)]


TOP = [float(x) for x in MODAL[4]]
WEIGHTS = [float(x) for x in GAUSS_WEIGHTS]


def total_of(values):
    out = values[0]
    for value in values[1:]:
        out = out + value
    return out


def symmetric(coefficients, u):
    c = coefficients
    return c[0] * (u[0] + u[4]) + c[1] * (u[1] + u[3]) + c[2] * u[2]


def energy(values):
    return symmetric(WEIGHTS, [x * x for x in values])


def sensor(load):
    planes = {"y": [], "z": [], "yz": [], "total": [], "ez": [], "ey": [], "eyz": []}
    top_x = {}
    for a in range(5):
        u = [[load(25 * a + 5 * b + c) for c in range(5)] for b in range(5)]
        for b in range(5):
            for c in range(5):
                term = TOP[a] * u[b][c]
                top_x[b, c] = term if a == 0 else top_x[b, c] + term
        z = [symmetric(TOP, u[b]) for b in range(5)]
        y = [symmetric(TOP, [u[b][c] for b in range(5)]) for c in range(5)]
        yz = symmetric(TOP, z)
        planes["total"].append(symmetric(WEIGHTS, [energy(u[b]) for b in range(5)]))
        planes["ez"].append(energy(z))
        planes["ey"].append(energy(y))
        planes["eyz"].append(yz * yz)
        planes["z"].append(z)
        planes["y"].append(y)
        planes["yz"].append(yz)
    total, e_z, e_y, e_yz = (symmetric(WEIGHTS, planes[k]) for k in ("total", "ez", "ey", "eyz"))
    x_z = [symmetric(TOP, [planes["z"][a][b] for a in range(5)]) for b in range(5)]
    x_y = [symmetric(TOP, [planes["y"][a][c] for a in range(5)]) for c in range(5)]
    x_yz = symmetric(TOP, planes["yz"])
    e_x = symmetric(WEIGHTS, [energy([top_x[b, c] for c in range(5)]) for b in range(5)])
    high = e_x + (e_y - energy(x_y)) + ((e_z - energy(x_z)) - (e_yz - x_yz * x_yz))
    level = jnp.log(jnp.maximum(high / (total + ENERGY_EPS), RATIO_FLOOR)) * (1.0 / math.log(10.0))
    ramp = jnp.clip((level - SENSOR_CENTRE) / SENSOR_WIDTH, -1.0, 1.0)
    return EPS_SCALE * 0.5 * (1.0 + jnp.sin(0.5 * math.pi * ramp))


def rolled(value, shift, axis):
    size = value.shape[axis]
    return pltpu.roll(value, shift % size, axis)


LOWER = [float((1.0 - x) / 2.0) for x in NODES]
UPPER = [float((1.0 + x) / 2.0) for x in NODES]


def along_lanes(line):
    lanes = line.shape[1]
    lane = lax.broadcasted_iota(jnp.int32, line.shape, 1)
    before = jnp.where(lane == 0, 0.0, rolled(line, 1, 1))
    after = jnp.where(lane == lanes - 1, 0.0, rolled(line, -1, 1))
    return jnp.maximum(line, before), jnp.maximum(line, after)


def interpolate(neighbours, nu):
    corner = {}
    for x in range(2):
        for y in range(2):
            line = jnp.maximum(
                jnp.maximum(neighbours[x][y], neighbours[x + 1][y]),
                jnp.maximum(neighbours[x][y + 1], neighbours[x + 1][y + 1]),
            )
            corner[x, y, 0], corner[x, y, 1] = along_lanes(line)
    lower, upper = LOWER, UPPER
    for a in range(5):
        face = {
            (y, z): lower[a] * corner[0, y, z] + upper[a] * corner[1, y, z]
            for y in range(2)
            for z in range(2)
        }
        for b in range(5):
            edge = [lower[b] * face[0, z] + upper[b] * face[1, z] for z in range(2)]
            for c in range(5):
                nu[25 * a + 5 * b + c] = lower[c] * edge[0] + upper[c] * edge[1]


def row_masks(axis, chords, spans, lanes):
    row = lax.broadcasted_iota(jnp.int32, (chords * spans, lanes), 0)
    if axis == 0:
        return row < spans, row >= (chords - 1) * spans
    place = row % spans
    return place == 0, place == spans - 1


def local_kernel(sizes, count, chords, spans, *refs):
    state_hbm = refs[0]
    nu, acc = refs[1:3]
    state, around, work, eps_out = refs[3:7]
    grads = refs[7:10]
    faces = (refs[10:12], refs[12:14])
    ghosts = (refs[14:16], refs[16:18])
    load_sem, eps_sem, send_sem, state_sem, flux_sem, chord_sem, answer = refs[18:]
    rows, lanes = nu.shape[1:]
    chord_size, span_size = sizes
    me_c, me_s = lax.axis_index("chord"), lax.axis_index("span")
    mesh_id = pl.DeviceIdType.MESH

    def whole(ref):
        return ref.reshape(count, 25, rows, lanes)

    def reachable(dx):
        if dx == 0:
            return None
        return me_c + 1 < chord_size if dx == 1 else me_c > 0

    def guarded(cond, run):
        if cond is None:
            run()
        else:
            pl.when(cond)(run)

    def partner(dx, dy):
        return (me_c + dx, lax.rem(me_s + dy + span_size, span_size))

    level = ((0, -1), (0, 1))
    lower, upper = (tuple((dx, dy) for dy in (0, -1, 1)) for dx in (-1, 1))

    def greet(sem, offsets):
        for dx, dy in offsets:
            pl.semaphore_signal(sem, inc=1, device_id=partner(dx, dy), device_id_type=mesh_id)

    barrier = pltpu.get_barrier_semaphore()
    greet(barrier, level)

    def load(k, *part):
        return pltpu.make_async_copy(state_hbm.at[part], state.at[part], load_sem.at[k])

    start, remainder = load(0, 0, pl.ds(0, 50)), load(1, 0, pl.ds(50, 75))
    second, others = load(2, pl.ds(1, 1)), load(3, pl.ds(2, count - 2))
    for copy in (start, remainder, second, others):
        copy.start()

    guarded(reachable(1), lambda: greet(barrier, upper))

    def eps_copy(dx, dy):
        return pltpu.make_async_remote_copy(
            src_ref=eps_out, dst_ref=around.at[1 - dx, 1 - dy],
            send_sem=eps_sem.at[0], recv_sem=eps_sem.at[1 if dx == 0 else 2],
            device_id=partner(dx, dy), device_id_type=mesh_id,
        )

    def column_copy():
        return pltpu.make_async_remote_copy(
            src_ref=around.at[1], dst_ref=around.at[0],
            send_sem=eps_sem.at[0], recv_sem=eps_sem.at[2],
            device_id=partner(1, 0), device_id_type=mesh_id,
        )

    ways = ((1, 0), (-1, 0), (0, 1), (0, -1))

    def side(ref, axis, v, last, part):
        if axis == 0:
            return ref.at[v, part, chords - 1 if last else 0]
        return ref.at[v, part, :, spans - 1 if last else 0]

    def recv_sem(stage, axis, v):
        if stage == 0:
            return state_sem.at[axis, v]
        return chord_sem if axis == 0 else flux_sem.at[v]

    def send_eps(offsets):
        for dx, dy in offsets:
            eps_copy(dx, dy).start()

    def launch(stage, axis, v, sides=(0, 1), part=pl.ds(0, 25), only=None):
        for k in (2 * axis + i for i in sides):
            dx, dy = ways[k]
            up = k % 2 == 0

            def start():
                pltpu.make_async_remote_copy(
                    src_ref=side(faces[stage][axis], axis, v, up, part),
                    dst_ref=side(ghosts[stage][axis], axis, v, not up, part),
                    send_sem=send_sem.at[stage, axis], recv_sem=recv_sem(stage, axis, v),
                    device_id=partner(dx, dy), device_id_type=mesh_id,
                ).start()

            allowed = reachable(dx) if only is None else only(partner(dx, dy)[1])
            guarded(allowed, start)

    def first_half(s):
        return s < span_size // 2

    def second_half(s):
        return s >= span_size // 2

    two_sided = (me_c > 0) & (me_c + 1 < chord_size)

    def await_bytes(ref, sem):
        pltpu.make_async_copy(ref, ref, sem).wait()

    def await_chord(ref, part, sem):
        pl.when(two_sided)(lambda: await_bytes(ref.at[part, :, pl.ds(0, 2)], sem))
        pl.when(jnp.logical_not(two_sided))(lambda: await_bytes(ref.at[part, :, pl.ds(0, 1)], sem))

    def await_eps(sem, base):
        pl.when(two_sided)(lambda: await_bytes(work.at[pl.ds(0, base + 6)], sem))
        pl.when(jnp.logical_not(two_sided))(
            lambda: await_bytes(work.at[pl.ds(0, base + 3)], sem)
        )

    every = pl.ds(0, count)

    def all_sent(stage):
        await_chord(faces[stage][0], every, send_sem.at[stage, 0])
        await_bytes(faces[stage][1].at[:, :, :, pl.ds(0, 2)], send_sem.at[stage, 1])

    masks = [row_masks(axis, chords, spans, lanes) for axis in range(2)]

    def form_traces(axis, v, lines=range(5)):
        low = masks[axis][0]
        ends = [jnp.where(low, float(LEFT[i]), float(RIGHT[i])) for i in range(5)]
        out = whole(faces[0][axis])
        for q in lines:
            for j in range(5):
                pts = points(axis, q, j)
                out[v, 5 * q + j] = total_of([e * state[v, p] for e, p in zip(ends, pts)])

    with jax.named_scope("load0"):
        start.wait()
    form_traces(1, 0, range(2))
    with jax.named_scope("barrier"):
        pl.semaphore_wait(barrier, 2 + jnp.where(me_c > 0, 3, 0))
    launch(0, 1, 0, part=pl.ds(0, 10))
    guarded(reachable(-1), lambda: greet(answer, ((-1, 0),)))
    with jax.named_scope("sensor"):
        remainder.wait()
        eps = sensor(lambda p: state[0, p])
        eps_out[...] = eps
        around[1, 1] = eps
    send_eps(level)
    guarded(reachable(-1), lambda: send_eps(lower))
    form_traces(1, 0, range(2, 5))
    launch(0, 1, 0, part=pl.ds(10, 15))
    with jax.named_scope("later"):
        def span_traces(v, carry):
            form_traces(1, v)
            launch(0, 1, v)
            return carry

        second.wait()
        span_traces(1, 0)
        others.wait()
        lax.fori_loop(2, count, span_traces, 0)

        def chord_traces(v, carry):
            form_traces(0, v)
            launch(0, 0, v, (1,))
            return carry

        lax.fori_loop(0, count, chord_traces, 0)

    lane = lax.broadcasted_iota(jnp.int32, (rows, lanes), 1)
    first, last = lane == 0, lane == lanes - 1
    row = lax.broadcasted_iota(jnp.int32, (rows, lanes), 0)
    have_low = jnp.where(me_c > 0, spans, 0)
    have_high = jnp.where(me_c + 1 < chord_size, rows, rows - spans)
    low_s, high_s = masks[1]
    low_c, high_c = masks[0]
    closed_low = row < spans - have_low
    closed_high = row >= have_high
    closed = closed_low | closed_high
    shut = jnp.where(closed, 1.0, 0.0)

    def normal_gradient(v, carry):
        grad = grads[2]
        for q in range(5):
            for j in range(5):
                pts = points(2, q, j)
                parts = fold([state[v, p] for p in pts])
                left, right = traces(parts)
                before = jnp.where(first, left, rolled(right, 1, 1))
                after = jnp.where(last, right, rolled(left, -1, 1))
                for p, value in zip(pts, slope(parts, before, after)):
                    grad[v, p] = value
        return carry

    def across_gradient(axis):
        low, high = masks[axis]
        step = spans if axis == 0 else 1
        mine, grad = whole(faces[0][axis]), grads[axis]

        def body(v, carry):
            for q in range(5):
                for j in range(5):
                    pts = points(axis, q, j)
                    parts = fold([state[v, p] for p in pts])
                    left, right = traces(parts)
                    beyond = shut * mine[v, 5 * q + j] if axis == 0 else 0.0
                    before = jnp.where(low, beyond, rolled(right, step, 0))
                    after = jnp.where(high, beyond, rolled(left, -step, 0))
                    for p, value in zip(pts, slope(parts, before, after)):
                        grad[v, p] = value
            return carry

        return body

    with jax.named_scope("ngrad"):
        lax.fori_loop(0, count, normal_gradient, 0)
    with jax.named_scope("sgrad"):
        lax.fori_loop(0, count, across_gradient(1), 0)

    with jax.named_scope("level"):
        await_bytes(work.at[pl.ds(0, 2)], eps_sem.at[1])
    with jax.named_scope("answer"):

        @pl.when(reachable(1))
        def _():
            pl.semaphore_wait(answer, 1)
            column_copy().start()

        def chord_up(v, carry):
            launch(0, 0, v, (0,))
            return carry

        lax.fori_loop(0, count, chord_up, 0)

    with jax.named_scope("cgrad"):
        lax.fori_loop(0, count, across_gradient(0), 0)

    with jax.named_scope("epswait"):
        await_eps(eps_sem.at[2], 0)

    column = []
    for x in range(3):
        mine, left, right = around[x, 1], around[x, 0], around[x, 2]
        column.append([
            jnp.where(low_s, rolled(left, 1 - spans, 0), rolled(mine, 1, 0)),
            mine,
            jnp.where(high_s, rolled(right, spans - 1, 0), rolled(mine, -1, 0)),
        ])
    neighbours = [[], [], []]
    for y in range(3):
        inner = column[1][y]
        below = jnp.where(low_c, rolled(column[0][y], spans, 0), rolled(inner, spans, 0))
        above = jnp.where(high_c, rolled(column[2][y], -spans, 0), rolled(inner, -spans, 0))
        neighbours[0].append(jnp.where(closed_low, 0.0, below))
        neighbours[1].append(inner)
        neighbours[2].append(jnp.where(closed_high, 0.0, above))
    interpolate(neighbours, nu)

    lifts = [
        [
            jnp.where(low, float(HALF_LEFT[i]), jnp.where(high, float(HALF_RIGHT[i]), 0.0))
            for i in range(5)
        ]
        for low, high in masks
    ]
    edges = [(low | high) for low, high in masks]
    edges[0] = edges[0] & jnp.logical_not(closed)
    full_edge = (chords == 1, spans <= 2)

    def outside(ref, axis, v, f):
        value = ref[v, f]
        return value if full_edge[axis] else jnp.where(edges[axis], value, 0.0)

    def across(axis, v):
        low, high = masks[axis]
        step = spans if axis == 0 else 1
        grad, ghost, out = grads[axis], whole(ghosts[0][axis]), whole(faces[1][axis])
        for q in range(5):
            for j in range(5):
                f = 5 * q + j
                pts = points(axis, q, j)
                beyond = outside(ghost, axis, v, f)
                gradient = [grad[v, p] + lift * beyond for p, lift in zip(pts, lifts[axis])]
                parts = fold([nu[p] * g for p, g in zip(pts, gradient)])
                left, right = traces(parts)
                ends = jnp.where(low, left, right)
                out[v, f] = ends
                beyond = -shut * ends if axis == 0 else 0.0
                before = jnp.where(low, beyond, rolled(right, step, 0))
                after = jnp.where(high, beyond, rolled(left, -step, 0))
                for p, value in zip(pts, slope(parts, before, after)):
                    if axis == 1:
                        acc[v, p] = value
                    else:
                        acc[v, p] += value

    def normal(v):
        for q in range(5):
            for j in range(5):
                pts = points(2, q, j)
                parts = fold([nu[p] * grads[2][v, p] for p in pts])
                left, right = traces(parts)
                before = jnp.where(first, -left, rolled(right, 1, 1))
                after = jnp.where(last, -right, rolled(left, -1, 1))
                for p, value in zip(pts, slope(parts, before, after)):
                    acc[v, p] += value

    lag = min(LAG, count)

    def variable(v, carry):
        with jax.named_scope("wait_u1"):
            await_bytes(ghosts[0][1].at[v, :, :, pl.ds(0, 2)], state_sem.at[1, v])
        with jax.named_scope("span"):
            across(1, v)
            launch(1, 1, v, only=first_half)
        with jax.named_scope("wait_u0"):
            await_chord(ghosts[0][0], v, state_sem.at[0, v])
        with jax.named_scope("chord"):
            across(0, v)
            launch(1, 0, v)
            due = v >= lag
            launch(1, 1, jnp.maximum(v - lag, 0), only=lambda s: second_half(s) & due)
        return carry

    with jax.named_scope("fluxes"):
        lax.fori_loop(0, count, variable, 0)

    def launch_rest(v, carry):
        launch(1, 1, v, only=second_half)
        return carry

    lax.fori_loop(count - lag, count, launch_rest, 0)

    def rest(v, carry):
        normal(v)
        return carry

    with jax.named_scope("normal"):
        lax.fori_loop(0, count, rest, 0)

    with jax.named_scope("sent0"):
        await_eps(eps_sem.at[0], 2)
        all_sent(0)

    def correct(v, carry):
        with jax.named_scope("wait_f1"):
            await_bytes(ghosts[1][1].at[v, :, :, pl.ds(0, 2)], flux_sem.at[v])
        flux_c, flux_s = whole(ghosts[1][0]), whole(ghosts[1][1])
        for c in range(5):
            along = [
                [outside(flux_c, 0, v, 5 * b + c) for b in range(5)],
                [outside(flux_s, 1, v, 5 * a + c) for a in range(5)],
            ]
            for a in range(5):
                for b in range(5):
                    acc[v, 25 * a + 5 * b + c] += (
                        lifts[0][a] * along[0][b] + lifts[1][b] * along[1][a]
                    )
        return carry

    with jax.named_scope("wait_f0"):
        await_chord(ghosts[1][0], every, chord_sem)
    with jax.named_scope("correct"):
        lax.fori_loop(0, count, correct, 0)
    with jax.named_scope("sent1"):
        all_sent(1)


def finish_kernel(acc, nu, residual_out, nu_out, sems):
    copies = (
        pltpu.make_async_copy(acc, residual_out, sems.at[0]),
        pltpu.make_async_copy(nu, nu_out, sems.at[1]),
    )
    for copy in copies:
        copy.start()
    for copy in copies:
        copy.wait()


def shards(state):
    count, npts, chords, spans, lanes = state.shape
    rows = chords * spans
    flat = state.reshape(count, npts, rows, lanes)
    f32 = jnp.float32
    sizes = (lax.axis_size("chord"), lax.axis_size("span"))

    def full(*shape):
        return jax.ShapeDtypeStruct(shape, f32)

    vmem = pl.BlockSpec(memory_space=pltpu.VMEM)
    nu, residual = pl.pallas_call(
        functools.partial(local_kernel, sizes, count, chords, spans),
        in_specs=[pl.BlockSpec(memory_space=pltpu.HBM)],
        out_specs=[vmem, vmem],
        out_shape=[full(npts, rows, lanes), full(count, npts, rows, lanes)],
        scratch_shapes=[
            pltpu.VMEM(shape, f32)
            for shape in [
                (count, npts, rows, lanes),
                (3, 3, rows, lanes),
                (8, rows, lanes),
                (rows, lanes),
                (count, npts, rows, lanes),
                (count, npts, rows, lanes),
                (count, npts, rows, lanes),
            ]
            + [(count, 25, chords, spans, lanes)] * 8
        ]
        + [
            pltpu.SemaphoreType.DMA((4,)),
            pltpu.SemaphoreType.DMA((3,)),
            pltpu.SemaphoreType.DMA((2, 2)),
            pltpu.SemaphoreType.DMA((2, count)),
            pltpu.SemaphoreType.DMA((count,)),
            pltpu.SemaphoreType.DMA,
            pltpu.SemaphoreType.REGULAR,
        ],
        compiler_params=pltpu.CompilerParams(
            collective_id=0, has_side_effects=True, vmem_limit_bytes=VMEM_BYTES
        ),
    )(flat)
    hbm = pl.BlockSpec(memory_space=pltpu.HBM)
    residual, nu = pl.pallas_call(
        finish_kernel,
        in_specs=[vmem, vmem],
        out_specs=[hbm, hbm],
        out_shape=[full(count, npts, rows, lanes), full(npts, rows, lanes)],
        scratch_shapes=[pltpu.SemaphoreType.DMA((2,))],
        compiler_params=pltpu.CompilerParams(vmem_limit_bytes=FINISH_BYTES),
    )(residual, nu)
    return residual.reshape(state.shape), nu.reshape(npts, chords, spans, lanes)


def solution(mesh):
    in_specs = (P(None, None, "chord", "span", None),)
    out_specs = (P(None, None, "chord", "span", None), P(None, "chord", "span", None))
    return jax.shard_map(shards, mesh=mesh, in_specs=in_specs, out_specs=out_specs, check_vma=False)
```

```python
import functools
import math

import jax
import jax.numpy as jnp
import numpy as np
from jax import lax
from jax.experimental import pallas as pl
from jax.experimental.pallas import tpu as pltpu
from jax.sharding import PartitionSpec as P

VMEM_BYTES = 52_500_000
FINISH_BYTES = 8_000_000
LAG = 3
EPS_SCALE = 0.01
SENSOR_CENTRE = -3.0
SENSOR_WIDTH = 1.5
RATIO_FLOOR = 1e-06
ENERGY_EPS = 1e-06
GAUSS_NODES = [-0.906179845938664, -0.5384693101056831, 0.0, 0.5384693101056831, 0.906179845938664]
GAUSS_WEIGHTS = [
    0.2369268850561891,
    0.4786286704993665,
    0.5688888888888889,
    0.4786286704993665,
    0.2369268850561891,
]


def legendre_values(points):
    values = [np.ones(points.shape), np.array(points)]
    for order in range(1, 5):
        values.append(
            ((2 * order + 1) * points * values[order] - order * values[order - 1]) / (order + 1)
        )
    return values


def line_tables():
    line_nodes = np.array(GAUSS_NODES)
    quadrature_weights = np.array(GAUSS_WEIGHTS)
    barycentric = np.array(
        [
            1.0 / np.prod([line_nodes[j] - line_nodes[k] for k in range(5) if k != j])
            for j in range(5)
        ]
    )
    derivative = np.zeros((5, 5))
    for i in range(5):
        for j in range(5):
            if i != j:
                derivative[i, j] = barycentric[j] / barycentric[i] / (line_nodes[i] - line_nodes[j])
        derivative[i, i] = -np.sum(derivative[i])
    left_values = np.ones(5)
    right_values = np.ones(5)
    for j in range(5):
        for k in range(5):
            if k != j:
                left_values[j] *= (-1.0 - line_nodes[k]) / (line_nodes[j] - line_nodes[k])
                right_values[j] *= (1.0 - line_nodes[k]) / (line_nodes[j] - line_nodes[k])
    legendre = legendre_values(line_nodes)
    fourth_slope = 7.0 * legendre[3] + 3.0 * legendre[1]
    fifth_slope = 9.0 * legendre[4] + 5.0 * legendre[2] + legendre[0]
    left_corr = 0.5 * (fourth_slope - fifth_slope)
    right_corr = 0.5 * (fourth_slope + fifth_slope)
    modal = np.zeros((5, 5))
    for k in range(5):
        modal[k, :] = quadrature_weights * math.sqrt((2 * k + 1) / 2.0) * legendre[k]
    return (line_nodes, derivative, left_values, right_values, left_corr, right_corr, modal)


NODES, DERIV, LEFT, RIGHT, LIFT_LEFT, LIFT_RIGHT, MODAL = line_tables()
HALF_LEFT = 0.5 * LIFT_LEFT
HALF_RIGHT = 0.5 * LIFT_RIGHT


def fold(u):
    return (u[0] + u[4], u[1] + u[3], u[2], u[0] - u[4], u[1] - u[3])


def traces(parts):
    s0, s1, mid, d0, d1 = parts
    r = [float(x) for x in RIGHT]
    even = 0.5 * (r[0] + r[4]) * s0 + 0.5 * (r[1] + r[3]) * s1 + r[2] * mid
    odd = 0.5 * (r[0] - r[4]) * d0 + 0.5 * (r[1] - r[3]) * d1
    return even - odd, even + odd


def slope(parts, before, after):
    s0, s1, mid, d0, d1 = parts
    h = [float(x) for x in HALF_LEFT]
    r = [float(x) for x in RIGHT]
    if before is not None:
        diff, both = before - after, before + after
    even, odd = [], []
    for i in range(3):
        lift = 0.5 * (h[i] + h[4 - i])
        value = (
            float(0.5 * (DERIV[i, 0] - DERIV[i, 4]) + lift * (r[0] - r[4])) * d0
            + float(0.5 * (DERIV[i, 1] - DERIV[i, 3]) + lift * (r[1] - r[3])) * d1
        )
        even.append(value if before is None else value + lift * diff)
    for i in range(2):
        lift = 0.5 * (h[i] - h[4 - i])
        value = (
            float(0.5 * (DERIV[i, 0] + DERIV[i, 4]) - lift * (r[0] + r[4])) * s0
            + float(0.5 * (DERIV[i, 1] + DERIV[i, 3]) - lift * (r[1] + r[3])) * s1
            + float(DERIV[i, 2] - 2.0 * lift * r[2]) * mid
        )
        odd.append(value if before is None else value + lift * both)
    return [even[0] + odd[0], even[1] + odd[1], even[2], even[1] - odd[1], even[0] - odd[0]]


def points(axis, q, j):
    if axis == 0:
        return [25 * i + 5 * q + j for i in range(5)]
    if axis == 1:
        return [25 * q + 5 * i + j for i in range(5)]
    return [25 * q + 5 * j + i for i in range(5)]


TOP = [float(x) for x in MODAL[4]]
WEIGHTS = [float(x) for x in GAUSS_WEIGHTS]


def total_of(values):
    out = values[0]
    for value in values[1:]:
        out = out + value
    return out


def symmetric(coefficients, u):
    c = coefficients
    return c[0] * (u[0] + u[4]) + c[1] * (u[1] + u[3]) + c[2] * u[2]


def energy(values):
    return symmetric(WEIGHTS, [x * x for x in values])


def sensor(load):
    planes = {"y": [], "z": [], "yz": [], "total": [], "ez": [], "ey": [], "eyz": []}
    top_x = {}
    for a in range(5):
        u = [[load(25 * a + 5 * b + c) for c in range(5)] for b in range(5)]
        for b in range(5):
            for c in range(5):
                term = TOP[a] * u[b][c]
                top_x[b, c] = term if a == 0 else top_x[b, c] + term
        z = [symmetric(TOP, u[b]) for b in range(5)]
        y = [symmetric(TOP, [u[b][c] for b in range(5)]) for c in range(5)]
        yz = symmetric(TOP, z)
        planes["total"].append(symmetric(WEIGHTS, [energy(u[b]) for b in range(5)]))
        planes["ez"].append(energy(z))
        planes["ey"].append(energy(y))
        planes["eyz"].append(yz * yz)
        planes["z"].append(z)
        planes["y"].append(y)
        planes["yz"].append(yz)
    total, e_z, e_y, e_yz = (symmetric(WEIGHTS, planes[k]) for k in ("total", "ez", "ey", "eyz"))
    x_z = [symmetric(TOP, [planes["z"][a][b] for a in range(5)]) for b in range(5)]
    x_y = [symmetric(TOP, [planes["y"][a][c] for a in range(5)]) for c in range(5)]
    x_yz = symmetric(TOP, planes["yz"])
    e_x = symmetric(WEIGHTS, [energy([top_x[b, c] for c in range(5)]) for b in range(5)])
    high = e_x + (e_y - energy(x_y)) + ((e_z - energy(x_z)) - (e_yz - x_yz * x_yz))
    level = jnp.log(jnp.maximum(high / (total + ENERGY_EPS), RATIO_FLOOR)) * (1.0 / math.log(10.0))
    ramp = jnp.clip((level - SENSOR_CENTRE) / SENSOR_WIDTH, -1.0, 1.0)
    return EPS_SCALE * 0.5 * (1.0 + jnp.sin(0.5 * math.pi * ramp))


def rolled(value, shift, axis):
    size = value.shape[axis]
    return pltpu.roll(value, shift % size, axis)


LOWER = [float((1.0 - x) / 2.0) for x in NODES]
UPPER = [float((1.0 + x) / 2.0) for x in NODES]


def along_lanes(line):
    lanes = line.shape[1]
    lane = lax.broadcasted_iota(jnp.int32, line.shape, 1)
    before = jnp.where(lane == 0, 0.0, rolled(line, 1, 1))
    after = jnp.where(lane == lanes - 1, 0.0, rolled(line, -1, 1))
    return jnp.maximum(line, before), jnp.maximum(line, after)


def interpolate(neighbours, nu):
    corner = {}
    for x in range(2):
        for y in range(2):
            line = jnp.maximum(
                jnp.maximum(neighbours[x][y], neighbours[x + 1][y]),
                jnp.maximum(neighbours[x][y + 1], neighbours[x + 1][y + 1]),
            )
            corner[x, y, 0], corner[x, y, 1] = along_lanes(line)
    lower, upper = LOWER, UPPER
    for a in range(5):
        face = {
            (y, z): lower[a] * corner[0, y, z] + upper[a] * corner[1, y, z]
            for y in range(2)
            for z in range(2)
        }
        for b in range(5):
            edge = [lower[b] * face[0, z] + upper[b] * face[1, z] for z in range(2)]
            for c in range(5):
                nu[25 * a + 5 * b + c] = lower[c] * edge[0] + upper[c] * edge[1]


def row_masks(axis, chords, spans, lanes):
    row = lax.broadcasted_iota(jnp.int32, (chords * spans, lanes), 0)
    if axis == 0:
        return row < spans, row >= (chords - 1) * spans
    place = row % spans
    return place == 0, place == spans - 1


def local_kernel(sizes, count, chords, spans, *refs):
    state_hbm = refs[0]
    nu, acc = refs[1:3]
    state, around, tally = refs[3:6]
    grads = refs[6:9]
    faces = (refs[9:11], refs[11:13])
    ghosts = (refs[13:15], refs[15:17])
    load_sem, eps_sem, send_sem, state_sem, flux_sem, chord_sem, answer = refs[17:]
    rows, lanes = nu.shape[1:]
    chord_size, span_size = sizes
    me_c, me_s = lax.axis_index("chord"), lax.axis_index("span")
    mesh_id = pl.DeviceIdType.MESH

    def whole(ref):
        return ref.reshape(count, 25, rows, lanes)

    all_eps = around.reshape(3, 3, rows, lanes)

    def reachable(dx):
        if dx == 0:
            return None
        return me_c + 1 < chord_size if dx == 1 else me_c > 0

    def guarded(cond, run):
        if cond is None:
            run()
        else:
            pl.when(cond)(run)

    def partner(dx, dy):
        return (me_c + dx, lax.rem(me_s + dy + span_size, span_size))

    level = ((0, -1), (0, 1))
    lower, upper = (tuple((dx, dy) for dy in (0, -1, 1)) for dx in (-1, 1))

    def greet(sem, offsets):
        for dx, dy in offsets:
            pl.semaphore_signal(sem, inc=1, device_id=partner(dx, dy), device_id_type=mesh_id)

    barrier = pltpu.get_barrier_semaphore()
    greet(barrier, level)

    def load(k, *part):
        return pltpu.make_async_copy(state_hbm.at[part], state.at[part], load_sem.at[k])

    start, remainder = load(0, 0, pl.ds(0, 75)), load(1, 0, pl.ds(75, 50))
    second, others = load(2, pl.ds(1, 1)), load(3, pl.ds(2, count - 2))
    for copy in (start, remainder, second, others):
        copy.start()

    guarded(reachable(1), lambda: greet(barrier, upper))

    def edge_of(step, size):
        return pl.ds(0, size) if step == 0 else (size - 1 if step == 1 else 0)

    def eps_copy(dx, dy):
        part = (edge_of(dx, chords), edge_of(dy, spans))
        return pltpu.make_async_remote_copy(
            src_ref=around.at[(1, 1) + part], dst_ref=around.at[(1 - dx, 1 - dy) + part],
            send_sem=eps_sem.at[0], recv_sem=eps_sem.at[1 if dx == 0 else 2],
            device_id=partner(dx, dy), device_id_type=mesh_id,
        )

    def column_copy():
        return pltpu.make_async_remote_copy(
            src_ref=around.at[1, :, chords - 1], dst_ref=around.at[0, :, chords - 1],
            send_sem=eps_sem.at[0], recv_sem=eps_sem.at[2],
            device_id=partner(1, 0), device_id_type=mesh_id,
        )

    ways = ((1, 0), (-1, 0), (0, 1), (0, -1))

    def side(ref, axis, v, last, part):
        if axis == 0:
            return ref.at[v, part, chords - 1 if last else 0]
        return ref.at[v, part, :, spans - 1 if last else 0]

    def recv_sem(stage, axis, v):
        if stage == 0:
            return state_sem.at[axis, v]
        return chord_sem if axis == 0 else flux_sem.at[v]

    def send_eps(offsets):
        for dx, dy in offsets:
            eps_copy(dx, dy).start()

    def launch(stage, axis, v, sides=(0, 1), part=pl.ds(0, 25), only=None):
        for k in (2 * axis + i for i in sides):
            dx, dy = ways[k]
            up = k % 2 == 0

            def start():
                pltpu.make_async_remote_copy(
                    src_ref=side(faces[stage][axis], axis, v, up, part),
                    dst_ref=side(ghosts[stage][axis], axis, v, not up, part),
                    send_sem=send_sem.at[stage, axis], recv_sem=recv_sem(stage, axis, v),
                    device_id=partner(dx, dy), device_id_type=mesh_id,
                ).start()

            allowed = reachable(dx) if only is None else only(partner(dx, dy)[1])
            guarded(allowed, start)

    def first_half(s):
        return s < span_size // 2

    def second_half(s):
        return s >= span_size // 2

    two_sided = (me_c > 0) & (me_c + 1 < chord_size)

    def await_bytes(ref, sem):
        pltpu.make_async_copy(ref, ref, sem).wait()

    def await_chord(ref, part, sem):
        pl.when(two_sided)(lambda: await_bytes(ref.at[part, :, pl.ds(0, 2)], sem))
        pl.when(jnp.logical_not(two_sided))(lambda: await_bytes(ref.at[part, :, pl.ds(0, 1)], sem))

    def await_eps(sem, base, below, above):
        has_below, has_above = me_c > 0, me_c + 1 < chord_size
        for use_below in (False, True):
            for use_above in (False, True):
                size = base + use_below * below + use_above * above
                if size:
                    case = (has_below == use_below) & (has_above == use_above)
                    pl.when(case)(lambda size=size: await_bytes(tally.at[pl.ds(0, size)], sem))

    every = pl.ds(0, count)

    def all_sent(stage):
        await_chord(faces[stage][0], every, send_sem.at[stage, 0])
        await_bytes(faces[stage][1].at[:, :, :, pl.ds(0, 2)], send_sem.at[stage, 1])

    masks = [row_masks(axis, chords, spans, lanes) for axis in range(2)]

    def form_traces(axis, v, lines=range(5)):
        low = masks[axis][0]
        ends = [jnp.where(low, float(LEFT[i]), float(RIGHT[i])) for i in range(5)]
        out = whole(faces[0][axis])
        for q in lines:
            for j in range(5):
                pts = points(axis, q, j)
                out[v, 5 * q + j] = total_of([e * state[v, p] for e, p in zip(ends, pts)])

    with jax.named_scope("load0"):
        start.wait()
    form_traces(1, 0, range(3))
    with jax.named_scope("barrier"):
        pl.semaphore_wait(barrier, 2 + jnp.where(me_c > 0, 3, 0))
    launch(0, 1, 0, part=pl.ds(0, 15))
    guarded(reachable(-1), lambda: greet(answer, ((-1, 0),)))
    with jax.named_scope("sensor"):
        remainder.wait()
        eps = sensor(lambda p: state[0, p])
        all_eps[1, 1] = eps
    send_eps(level)
    guarded(reachable(-1), lambda: send_eps(lower))
    form_traces(1, 0, range(3, 5))
    launch(0, 1, 0, part=pl.ds(15, 10))
    with jax.named_scope("later"):
        def span_traces(v, carry):
            form_traces(1, v)
            launch(0, 1, v)
            return carry

        second.wait()
        span_traces(1, 0)
        others.wait()
        lax.fori_loop(2, count, span_traces, 0)

        def chord_traces(v, carry):
            form_traces(0, v)
            launch(0, 0, v, (1,))
            return carry

        lax.fori_loop(0, count, chord_traces, 0)

    lane = lax.broadcasted_iota(jnp.int32, (rows, lanes), 1)
    first, last = lane == 0, lane == lanes - 1
    row = lax.broadcasted_iota(jnp.int32, (rows, lanes), 0)
    have_low = jnp.where(me_c > 0, spans, 0)
    have_high = jnp.where(me_c + 1 < chord_size, rows, rows - spans)
    low_s, high_s = masks[1]
    low_c, high_c = masks[0]
    closed_low = row < spans - have_low
    closed_high = row >= have_high
    closed = closed_low | closed_high
    shut = jnp.where(closed, 1.0, 0.0)

    def normal_gradient(v, carry):
        grad = grads[2]
        for q in range(5):
            for j in range(5):
                pts = points(2, q, j)
                parts = fold([state[v, p] for p in pts])
                left, right = traces(parts)
                before = jnp.where(first, left, rolled(right, 1, 1))
                after = jnp.where(last, right, rolled(left, -1, 1))
                for p, value in zip(pts, slope(parts, before, after)):
                    grad[v, p] = value
        return carry

    def across_gradient(axis):
        low, high = masks[axis]
        step = spans if axis == 0 else 1
        mine, grad = whole(faces[0][axis]), grads[axis]

        def body(v, carry):
            for q in range(5):
                for j in range(5):
                    pts = points(axis, q, j)
                    parts = fold([state[v, p] for p in pts])
                    left, right = traces(parts)
                    beyond = shut * mine[v, 5 * q + j] if axis == 0 else 0.0
                    before = jnp.where(low, beyond, rolled(right, step, 0))
                    after = jnp.where(high, beyond, rolled(left, -step, 0))
                    for p, value in zip(pts, slope(parts, before, after)):
                        grad[v, p] = value
            return carry

        return body

    with jax.named_scope("ngrad"):
        lax.fori_loop(0, count, normal_gradient, 0)
    with jax.named_scope("sgrad"):
        lax.fori_loop(0, count, across_gradient(1), 0)

    with jax.named_scope("level"):
        await_bytes(tally.at[pl.ds(0, 2 * chords)], eps_sem.at[1])
    with jax.named_scope("answer"):

        @pl.when(reachable(1))
        def _():
            pl.semaphore_wait(answer, 1)
            column_copy().start()

        def chord_up(v, carry):
            launch(0, 0, v, (0,))
            return carry

        lax.fori_loop(0, count, chord_up, 0)

    with jax.named_scope("cgrad"):
        lax.fori_loop(0, count, across_gradient(0), 0)

    with jax.named_scope("epswait"):
        await_eps(eps_sem.at[2], 0, 3 * spans, spans + 2)

    column = []
    for x in range(3):
        mine, left, right = all_eps[x, 1], all_eps[x, 0], all_eps[x, 2]
        column.append([
            jnp.where(low_s, rolled(left, 1 - spans, 0), rolled(mine, 1, 0)),
            mine,
            jnp.where(high_s, rolled(right, spans - 1, 0), rolled(mine, -1, 0)),
        ])
    neighbours = [[], [], []]
    for y in range(3):
        inner = column[1][y]
        below = jnp.where(low_c, rolled(column[0][y], spans, 0), rolled(inner, spans, 0))
        above = jnp.where(high_c, rolled(column[2][y], -spans, 0), rolled(inner, -spans, 0))
        neighbours[0].append(jnp.where(closed_low, 0.0, below))
        neighbours[1].append(inner)
        neighbours[2].append(jnp.where(closed_high, 0.0, above))
    interpolate(neighbours, nu)

    lifts = [
        [
            jnp.where(low, float(HALF_LEFT[i]), jnp.where(high, float(HALF_RIGHT[i]), 0.0))
            for i in range(5)
        ]
        for low, high in masks
    ]
    edges = [(low | high) for low, high in masks]
    edges[0] = edges[0] & jnp.logical_not(closed)
    full_edge = (chords == 1, spans <= 2)

    def outside(ref, axis, v, f):
        value = ref[v, f]
        return value if full_edge[axis] else jnp.where(edges[axis], value, 0.0)

    def across(axis, v):
        low, high = masks[axis]
        step = spans if axis == 0 else 1
        grad, ghost, out = grads[axis], whole(ghosts[0][axis]), whole(faces[1][axis])
        for q in range(5):
            for j in range(5):
                f = 5 * q + j
                pts = points(axis, q, j)
                beyond = outside(ghost, axis, v, f)
                gradient = [grad[v, p] + lift * beyond for p, lift in zip(pts, lifts[axis])]
                parts = fold([nu[p] * g for p, g in zip(pts, gradient)])
                left, right = traces(parts)
                ends = jnp.where(low, left, right)
                out[v, f] = ends
                beyond = -shut * ends if axis == 0 else 0.0
                before = jnp.where(low, beyond, rolled(right, step, 0))
                after = jnp.where(high, beyond, rolled(left, -step, 0))
                for p, value in zip(pts, slope(parts, before, after)):
                    if axis == 1:
                        acc[v, p] = value
                    else:
                        acc[v, p] += value

    def normal(v):
        for q in range(5):
            for j in range(5):
                pts = points(2, q, j)
                parts = fold([nu[p] * grads[2][v, p] for p in pts])
                left, right = traces(parts)
                before = jnp.where(first, -left, rolled(right, 1, 1))
                after = jnp.where(last, -right, rolled(left, -1, 1))
                for p, value in zip(pts, slope(parts, before, after)):
                    acc[v, p] += value

    lag = min(LAG, count)

    def variable(v, carry):
        with jax.named_scope("wait_u1"):
            await_bytes(ghosts[0][1].at[v, :, :, pl.ds(0, 2)], state_sem.at[1, v])
        with jax.named_scope("span"):
            across(1, v)
            launch(1, 1, v, only=first_half)
        with jax.named_scope("wait_u0"):
            await_chord(ghosts[0][0], v, state_sem.at[0, v])
        with jax.named_scope("chord"):
            across(0, v)
            launch(1, 0, v)
            due = v >= lag
            launch(1, 1, jnp.maximum(v - lag, 0), only=lambda s: second_half(s) & due)
        return carry

    with jax.named_scope("fluxes"):
        lax.fori_loop(0, count, variable, 0)

    def launch_rest(v, carry):
        launch(1, 1, v, only=second_half)
        return carry

    lax.fori_loop(count - lag, count, launch_rest, 0)

    def rest(v, carry):
        normal(v)
        return carry

    with jax.named_scope("normal"):
        lax.fori_loop(0, count, rest, 0)

    with jax.named_scope("sent0"):
        await_eps(eps_sem.at[0], 2 * chords, spans + 2, 3 * spans)
        all_sent(0)

    def correct(v, carry):
        with jax.named_scope("wait_f1"):
            await_bytes(ghosts[1][1].at[v, :, :, pl.ds(0, 2)], flux_sem.at[v])
        flux_c, flux_s = whole(ghosts[1][0]), whole(ghosts[1][1])
        for c in range(5):
            along = [
                [outside(flux_c, 0, v, 5 * b + c) for b in range(5)],
                [outside(flux_s, 1, v, 5 * a + c) for a in range(5)],
            ]
            for a in range(5):
                for b in range(5):
                    acc[v, 25 * a + 5 * b + c] += (
                        lifts[0][a] * along[0][b] + lifts[1][b] * along[1][a]
                    )
        return carry

    with jax.named_scope("wait_f0"):
        await_chord(ghosts[1][0], every, chord_sem)
    with jax.named_scope("correct"):
        lax.fori_loop(0, count, correct, 0)
    with jax.named_scope("sent1"):
        all_sent(1)


def finish_kernel(acc, nu, residual_out, nu_out, sems):
    copies = (
        pltpu.make_async_copy(acc, residual_out, sems.at[0]),
        pltpu.make_async_copy(nu, nu_out, sems.at[1]),
    )
    for copy in copies:
        copy.start()
    for copy in copies:
        copy.wait()


def shards(state):
    count, npts, chords, spans, lanes = state.shape
    rows = chords * spans
    flat = state.reshape(count, npts, rows, lanes)
    f32 = jnp.float32
    sizes = (lax.axis_size("chord"), lax.axis_size("span"))

    def full(*shape):
        return jax.ShapeDtypeStruct(shape, f32)

    vmem = pl.BlockSpec(memory_space=pltpu.VMEM)
    nu, residual = pl.pallas_call(
        functools.partial(local_kernel, sizes, count, chords, spans),
        in_specs=[pl.BlockSpec(memory_space=pltpu.HBM)],
        out_specs=[vmem, vmem],
        out_shape=[full(npts, rows, lanes), full(count, npts, rows, lanes)],
        scratch_shapes=[
            pltpu.VMEM(shape, f32)
            for shape in [
                (count, npts, rows, lanes),
                (3, 3, chords, spans, lanes),
                (2 * chords + 4 * spans + 2, 1, lanes),
                (count, npts, rows, lanes),
                (count, npts, rows, lanes),
                (count, npts, rows, lanes),
            ]
            + [(count, 25, chords, spans, lanes)] * 8
        ]
        + [
            pltpu.SemaphoreType.DMA((4,)),
            pltpu.SemaphoreType.DMA((3,)),
            pltpu.SemaphoreType.DMA((2, 2)),
            pltpu.SemaphoreType.DMA((2, count)),
            pltpu.SemaphoreType.DMA((count,)),
            pltpu.SemaphoreType.DMA,
            pltpu.SemaphoreType.REGULAR,
        ],
        compiler_params=pltpu.CompilerParams(
            collective_id=0, has_side_effects=True, vmem_limit_bytes=VMEM_BYTES
        ),
    )(flat)
    hbm = pl.BlockSpec(memory_space=pltpu.HBM)
    residual, nu = pl.pallas_call(
        finish_kernel,
        in_specs=[vmem, vmem],
        out_specs=[hbm, hbm],
        out_shape=[full(count, npts, rows, lanes), full(npts, rows, lanes)],
        scratch_shapes=[pltpu.SemaphoreType.DMA((2,))],
        compiler_params=pltpu.CompilerParams(vmem_limit_bytes=FINISH_BYTES),
    )(residual, nu)
    return residual.reshape(state.shape), nu.reshape(npts, chords, spans, lanes)


def solution(mesh):
    in_specs = (P(None, None, "chord", "span", None),)
    out_specs = (P(None, None, "chord", "span", None), P(None, "chord", "span", None))
    return jax.shard_map(shards, mesh=mesh, in_specs=in_specs, out_specs=out_specs, check_vma=False)
```

```python
import functools
import math

import jax
import jax.numpy as jnp
import numpy as np
from jax import lax
from jax.experimental import pallas as pl
from jax.experimental.pallas import tpu as pltpu
from jax.sharding import PartitionSpec as P

VMEM_BYTES = 50_750_000
FINISH_BYTES = 8_000_000
HELD = 2
LAG = 3
EPS_SCALE = 0.01
SENSOR_CENTRE = -3.0
SENSOR_WIDTH = 1.5
RATIO_FLOOR = 1e-06
ENERGY_EPS = 1e-06
GAUSS_NODES = [-0.906179845938664, -0.5384693101056831, 0.0, 0.5384693101056831, 0.906179845938664]
GAUSS_WEIGHTS = [
    0.2369268850561891,
    0.4786286704993665,
    0.5688888888888889,
    0.4786286704993665,
    0.2369268850561891,
]


def legendre_values(points):
    values = [np.ones(points.shape), np.array(points)]
    for order in range(1, 5):
        values.append(
            ((2 * order + 1) * points * values[order] - order * values[order - 1]) / (order + 1)
        )
    return values


def line_tables():
    line_nodes = np.array(GAUSS_NODES)
    quadrature_weights = np.array(GAUSS_WEIGHTS)
    barycentric = np.array(
        [
            1.0 / np.prod([line_nodes[j] - line_nodes[k] for k in range(5) if k != j])
            for j in range(5)
        ]
    )
    derivative = np.zeros((5, 5))
    for i in range(5):
        for j in range(5):
            if i != j:
                derivative[i, j] = barycentric[j] / barycentric[i] / (line_nodes[i] - line_nodes[j])
        derivative[i, i] = -np.sum(derivative[i])
    left_values = np.ones(5)
    right_values = np.ones(5)
    for j in range(5):
        for k in range(5):
            if k != j:
                left_values[j] *= (-1.0 - line_nodes[k]) / (line_nodes[j] - line_nodes[k])
                right_values[j] *= (1.0 - line_nodes[k]) / (line_nodes[j] - line_nodes[k])
    legendre = legendre_values(line_nodes)
    fourth_slope = 7.0 * legendre[3] + 3.0 * legendre[1]
    fifth_slope = 9.0 * legendre[4] + 5.0 * legendre[2] + legendre[0]
    left_corr = 0.5 * (fourth_slope - fifth_slope)
    right_corr = 0.5 * (fourth_slope + fifth_slope)
    modal = np.zeros((5, 5))
    for k in range(5):
        modal[k, :] = quadrature_weights * math.sqrt((2 * k + 1) / 2.0) * legendre[k]
    return (line_nodes, derivative, left_values, right_values, left_corr, right_corr, modal)


NODES, DERIV, LEFT, RIGHT, LIFT_LEFT, LIFT_RIGHT, MODAL = line_tables()
HALF_LEFT = 0.5 * LIFT_LEFT
HALF_RIGHT = 0.5 * LIFT_RIGHT


def fold(u):
    return (u[0] + u[4], u[1] + u[3], u[2], u[0] - u[4], u[1] - u[3])


def traces(parts):
    s0, s1, mid, d0, d1 = parts
    r = [float(x) for x in RIGHT]
    even = 0.5 * (r[0] + r[4]) * s0 + 0.5 * (r[1] + r[3]) * s1 + r[2] * mid
    odd = 0.5 * (r[0] - r[4]) * d0 + 0.5 * (r[1] - r[3]) * d1
    return even - odd, even + odd


def slope(parts, before, after):
    s0, s1, mid, d0, d1 = parts
    h = [float(x) for x in HALF_LEFT]
    r = [float(x) for x in RIGHT]
    if before is not None:
        diff, both = before - after, before + after
    even, odd = [], []
    for i in range(3):
        lift = 0.5 * (h[i] + h[4 - i])
        value = (
            float(0.5 * (DERIV[i, 0] - DERIV[i, 4]) + lift * (r[0] - r[4])) * d0
            + float(0.5 * (DERIV[i, 1] - DERIV[i, 3]) + lift * (r[1] - r[3])) * d1
        )
        even.append(value if before is None else value + lift * diff)
    for i in range(2):
        lift = 0.5 * (h[i] - h[4 - i])
        value = (
            float(0.5 * (DERIV[i, 0] + DERIV[i, 4]) - lift * (r[0] + r[4])) * s0
            + float(0.5 * (DERIV[i, 1] + DERIV[i, 3]) - lift * (r[1] + r[3])) * s1
            + float(DERIV[i, 2] - 2.0 * lift * r[2]) * mid
        )
        odd.append(value if before is None else value + lift * both)
    return [even[0] + odd[0], even[1] + odd[1], even[2], even[1] - odd[1], even[0] - odd[0]]


def points(axis, q, j):
    if axis == 0:
        return [25 * i + 5 * q + j for i in range(5)]
    if axis == 1:
        return [25 * q + 5 * i + j for i in range(5)]
    return [25 * q + 5 * j + i for i in range(5)]


TOP = [float(x) for x in MODAL[4]]
WEIGHTS = [float(x) for x in GAUSS_WEIGHTS]


def total_of(values):
    out = values[0]
    for value in values[1:]:
        out = out + value
    return out


def symmetric(coefficients, u):
    c = coefficients
    return c[0] * (u[0] + u[4]) + c[1] * (u[1] + u[3]) + c[2] * u[2]


def energy(values):
    return symmetric(WEIGHTS, [x * x for x in values])


def sensor(load):
    planes = {"y": [], "z": [], "yz": [], "total": [], "ez": [], "ey": [], "eyz": []}
    top_x = {}
    for a in range(5):
        u = [[load(25 * a + 5 * b + c) for c in range(5)] for b in range(5)]
        for b in range(5):
            for c in range(5):
                term = TOP[a] * u[b][c]
                top_x[b, c] = term if a == 0 else top_x[b, c] + term
        z = [symmetric(TOP, u[b]) for b in range(5)]
        y = [symmetric(TOP, [u[b][c] for b in range(5)]) for c in range(5)]
        yz = symmetric(TOP, z)
        planes["total"].append(symmetric(WEIGHTS, [energy(u[b]) for b in range(5)]))
        planes["ez"].append(energy(z))
        planes["ey"].append(energy(y))
        planes["eyz"].append(yz * yz)
        planes["z"].append(z)
        planes["y"].append(y)
        planes["yz"].append(yz)
    total, e_z, e_y, e_yz = (symmetric(WEIGHTS, planes[k]) for k in ("total", "ez", "ey", "eyz"))
    x_z = [symmetric(TOP, [planes["z"][a][b] for a in range(5)]) for b in range(5)]
    x_y = [symmetric(TOP, [planes["y"][a][c] for a in range(5)]) for c in range(5)]
    x_yz = symmetric(TOP, planes["yz"])
    e_x = symmetric(WEIGHTS, [energy([top_x[b, c] for c in range(5)]) for b in range(5)])
    high = e_x + (e_y - energy(x_y)) + ((e_z - energy(x_z)) - (e_yz - x_yz * x_yz))
    level = jnp.log(jnp.maximum(high / (total + ENERGY_EPS), RATIO_FLOOR)) * (1.0 / math.log(10.0))
    ramp = jnp.clip((level - SENSOR_CENTRE) / SENSOR_WIDTH, -1.0, 1.0)
    return EPS_SCALE * 0.5 * (1.0 + jnp.sin(0.5 * math.pi * ramp))


def rolled(value, shift, axis):
    size = value.shape[axis]
    return pltpu.roll(value, shift % size, axis)


LOWER = [float((1.0 - x) / 2.0) for x in NODES]
UPPER = [float((1.0 + x) / 2.0) for x in NODES]


def along_lanes(line):
    lanes = line.shape[1]
    lane = lax.broadcasted_iota(jnp.int32, line.shape, 1)
    before = jnp.where(lane == 0, 0.0, rolled(line, 1, 1))
    after = jnp.where(lane == lanes - 1, 0.0, rolled(line, -1, 1))
    return jnp.maximum(line, before), jnp.maximum(line, after)


def interpolate(neighbours, nu):
    corner = {}
    for x in range(2):
        for y in range(2):
            line = jnp.maximum(
                jnp.maximum(neighbours[x][y], neighbours[x + 1][y]),
                jnp.maximum(neighbours[x][y + 1], neighbours[x + 1][y + 1]),
            )
            corner[x, y, 0], corner[x, y, 1] = along_lanes(line)
    lower, upper = LOWER, UPPER
    for a in range(5):
        face = {
            (y, z): lower[a] * corner[0, y, z] + upper[a] * corner[1, y, z]
            for y in range(2)
            for z in range(2)
        }
        for b in range(5):
            edge = [lower[b] * face[0, z] + upper[b] * face[1, z] for z in range(2)]
            for c in range(5):
                nu[25 * a + 5 * b + c] = lower[c] * edge[0] + upper[c] * edge[1]


def row_masks(axis, chords, spans, lanes):
    row = lax.broadcasted_iota(jnp.int32, (chords * spans, lanes), 0)
    if axis == 0:
        return row < spans, row >= (chords - 1) * spans
    place = row % spans
    return place == 0, place == spans - 1


def closed_rows(chord_size, chords, spans, lanes):
    rows = chords * spans
    me_c = lax.axis_index("chord")
    row = lax.broadcasted_iota(jnp.int32, (rows, lanes), 0)
    have_low = jnp.where(me_c > 0, spans, 0)
    have_high = jnp.where(me_c + 1 < chord_size, rows, rows - spans)
    return row < spans - have_low, row >= have_high


def boundary_lifts(masks, closed):
    lifts = [
        [
            jnp.where(low, float(HALF_LEFT[i]), jnp.where(high, float(HALF_RIGHT[i]), 0.0))
            for i in range(5)
        ]
        for low, high in masks
    ]
    edges = [(low | high) for low, high in masks]
    edges[0] = edges[0] & jnp.logical_not(closed)
    return lifts, edges


def masked_edge(value, axis, edges, spans):
    return value if axis == 1 and spans <= 2 else jnp.where(edges[axis], value, 0.0)


def add_fluxes(flux, lifts, store):
    for c in range(5):
        along = [[flux(axis, 5 * m + c) for m in range(5)] for axis in range(2)]
        for a in range(5):
            for b in range(5):
                store(25 * a + 5 * b + c, lifts[0][a] * along[0][b] + lifts[1][b] * along[1][a])


def local_kernel(sizes, count, chords, spans, *refs):
    state_hbm = refs[0]
    nu, acc = refs[1:3]
    state, around, tally = refs[5:8]
    grads = refs[8:11]
    faces = (refs[11:13], refs[13:15])
    ghosts = (refs[15:17], refs[3:5])
    load_sem, eps_sem, send_sem, state_sem, flux_sem, chord_sem, answer = refs[17:]
    rows, lanes = nu.shape[1:]
    chord_size, span_size = sizes
    me_c, me_s = lax.axis_index("chord"), lax.axis_index("span")
    mesh_id = pl.DeviceIdType.MESH

    def whole(ref):
        return ref.reshape(count, 25, rows, lanes)

    all_eps = around.reshape(3, 3, rows, lanes)

    def reachable(dx):
        if dx == 0:
            return None
        return me_c + 1 < chord_size if dx == 1 else me_c > 0

    def guarded(cond, run):
        if cond is None:
            run()
        else:
            pl.when(cond)(run)

    def partner(dx, dy):
        return (me_c + dx, lax.rem(me_s + dy + span_size, span_size))

    level = ((0, -1), (0, 1))
    lower, upper = (tuple((dx, dy) for dy in (0, -1, 1)) for dx in (-1, 1))

    def greet(sem, offsets):
        for dx, dy in offsets:
            pl.semaphore_signal(sem, inc=1, device_id=partner(dx, dy), device_id_type=mesh_id)

    barrier = pltpu.get_barrier_semaphore()
    greet(barrier, level)

    def load(k, *part):
        return pltpu.make_async_copy(state_hbm.at[part], state.at[part], load_sem.at[k])

    start, remainder = load(0, 0, pl.ds(0, 75)), load(1, 0, pl.ds(75, 50))
    second, others = load(2, pl.ds(1, 1)), load(3, pl.ds(2, count - 2))
    for copy in (start, remainder, second, others):
        copy.start()

    guarded(reachable(1), lambda: greet(barrier, upper))

    def edge_of(step, size):
        return pl.ds(0, size) if step == 0 else (size - 1 if step == 1 else 0)

    def eps_copy(dx, dy):
        part = (edge_of(dx, chords), edge_of(dy, spans))
        return pltpu.make_async_remote_copy(
            src_ref=around.at[(1, 1) + part], dst_ref=around.at[(1 - dx, 1 - dy) + part],
            send_sem=eps_sem.at[0], recv_sem=eps_sem.at[1 if dx == 0 else 2],
            device_id=partner(dx, dy), device_id_type=mesh_id,
        )

    def column_copy():
        return pltpu.make_async_remote_copy(
            src_ref=around.at[1, :, chords - 1], dst_ref=around.at[0, :, chords - 1],
            send_sem=eps_sem.at[0], recv_sem=eps_sem.at[2],
            device_id=partner(1, 0), device_id_type=mesh_id,
        )

    ways = ((1, 0), (-1, 0), (0, 1), (0, -1))

    def side(ref, axis, v, last, part):
        if axis == 0:
            return ref.at[v, part, chords - 1 if last else 0]
        return ref.at[v, part, :, spans - 1 if last else 0]

    def recv_sem(stage, axis, v):
        if stage == 0:
            return state_sem.at[axis, v]
        return chord_sem if axis == 0 else flux_sem.at[v]

    def send_eps(offsets):
        for dx, dy in offsets:
            eps_copy(dx, dy).start()

    def launch(stage, axis, v, sides=(0, 1), part=pl.ds(0, 25), only=None):
        for k in (2 * axis + i for i in sides):
            dx, dy = ways[k]
            up = k % 2 == 0

            def start():
                pltpu.make_async_remote_copy(
                    src_ref=side(faces[stage][axis], axis, v, up, part),
                    dst_ref=side(ghosts[stage][axis], axis, v, not up, part),
                    send_sem=send_sem.at[stage, axis], recv_sem=recv_sem(stage, axis, v),
                    device_id=partner(dx, dy), device_id_type=mesh_id,
                ).start()

            allowed = reachable(dx) if only is None else only(partner(dx, dy)[1])
            guarded(allowed, start)

    def first_half(s):
        return s < span_size // 2

    def second_half(s):
        return s >= span_size // 2

    def by_one_link(s):
        return (s % 4 == 1) | (s % 4 == 2)

    two_sided = (me_c > 0) & (me_c + 1 < chord_size)

    def await_bytes(ref, sem):
        pltpu.make_async_copy(ref, ref, sem).wait()

    def await_chord(ref, part, sem):
        pl.when(two_sided)(lambda: await_bytes(ref.at[part, :, pl.ds(0, 2)], sem))
        pl.when(jnp.logical_not(two_sided))(lambda: await_bytes(ref.at[part, :, pl.ds(0, 1)], sem))

    def await_eps(sem, base, below, above):
        has_below, has_above = me_c > 0, me_c + 1 < chord_size
        for use_below in (False, True):
            for use_above in (False, True):
                size = base + use_below * below + use_above * above
                if size:
                    case = (has_below == use_below) & (has_above == use_above)
                    pl.when(case)(lambda size=size: await_bytes(tally.at[pl.ds(0, size)], sem))

    every = pl.ds(0, count)

    def all_sent(stage):
        await_chord(faces[stage][0], every, send_sem.at[stage, 0])
        await_bytes(faces[stage][1].at[:, :, :, pl.ds(0, 2)], send_sem.at[stage, 1])

    masks = [row_masks(axis, chords, spans, lanes) for axis in range(2)]

    def form_traces(axis, v, lines=range(5)):
        low = masks[axis][0]
        ends = [jnp.where(low, float(LEFT[i]), float(RIGHT[i])) for i in range(5)]
        out = whole(faces[0][axis])
        for q in lines:
            for j in range(5):
                pts = points(axis, q, j)
                out[v, 5 * q + j] = total_of([e * state[v, p] for e, p in zip(ends, pts)])

    with jax.named_scope("load0"):
        start.wait()
    form_traces(1, 0, range(3))
    with jax.named_scope("barrier"):
        pl.semaphore_wait(barrier, 2 + jnp.where(me_c > 0, 3, 0))
    launch(0, 1, 0, part=pl.ds(0, 15))
    guarded(reachable(-1), lambda: greet(answer, ((-1, 0),)))
    with jax.named_scope("sensor"):
        remainder.wait()
        eps = sensor(lambda p: state[0, p])
        all_eps[1, 1] = eps
    send_eps(level)
    guarded(reachable(-1), lambda: send_eps(lower))
    form_traces(1, 0, range(3, 5))
    launch(0, 1, 0, part=pl.ds(15, 10))
    with jax.named_scope("later"):
        def span_traces(v, carry):
            form_traces(1, v)
            early = v < count - held
            launch(0, 1, v, only=lambda s: jnp.logical_not(by_one_link(s)) | early)
            return carry

        held = min(HELD, count - 1)
        second.wait()
        span_traces(1, 0)
        others.wait()
        lax.fori_loop(2, count, span_traces, 0)

        def chord_traces(v, carry):
            form_traces(0, v)
            launch(0, 0, v, (1,))
            return carry

        lax.fori_loop(0, count, chord_traces, 0)

    lane = lax.broadcasted_iota(jnp.int32, (rows, lanes), 1)
    first, last = lane == 0, lane == lanes - 1
    low_s, high_s = masks[1]
    low_c, high_c = masks[0]
    closed_low, closed_high = closed_rows(sizes[0], chords, spans, lanes)
    closed = closed_low | closed_high
    shut = jnp.where(closed, 1.0, 0.0)

    def normal_gradient(v, carry):
        grad = grads[2]
        for q in range(5):
            for j in range(5):
                pts = points(2, q, j)
                parts = fold([state[v, p] for p in pts])
                left, right = traces(parts)
                before = jnp.where(first, left, rolled(right, 1, 1))
                after = jnp.where(last, right, rolled(left, -1, 1))
                for p, value in zip(pts, slope(parts, before, after)):
                    grad[v, p] = value
        return carry

    def across_gradient(axis):
        low, high = masks[axis]
        step = spans if axis == 0 else 1
        mine, grad = whole(faces[0][axis]), grads[axis]

        def body(v, carry):
            for q in range(5):
                for j in range(5):
                    pts = points(axis, q, j)
                    parts = fold([state[v, p] for p in pts])
                    left, right = traces(parts)
                    beyond = shut * mine[v, 5 * q + j] if axis == 0 else 0.0
                    before = jnp.where(low, beyond, rolled(right, step, 0))
                    after = jnp.where(high, beyond, rolled(left, -step, 0))
                    for p, value in zip(pts, slope(parts, before, after)):
                        grad[v, p] = value
            return carry

        return body

    with jax.named_scope("ngrad"):
        lax.fori_loop(0, count, normal_gradient, 0)
    with jax.named_scope("sgrad"):
        lax.fori_loop(0, count, across_gradient(1), 0)

    with jax.named_scope("level"):
        await_bytes(tally.at[pl.ds(0, 2 * chords)], eps_sem.at[1])
    with jax.named_scope("answer"):

        @pl.when(reachable(1))
        def _():
            pl.semaphore_wait(answer, 1)
            column_copy().start()

        def chord_up(v, carry):
            launch(0, 0, v, (0,))
            return carry

        lax.fori_loop(0, count, chord_up, 0)

    def launch_held(v, carry):
        launch(0, 1, v, only=by_one_link)
        return carry

    lax.fori_loop(count - held, count, launch_held, 0)

    with jax.named_scope("cgrad"):
        lax.fori_loop(0, count, across_gradient(0), 0)

    with jax.named_scope("epswait"):
        await_eps(eps_sem.at[2], 0, 3 * spans, spans + 2)

    column = []
    for x in range(3):
        mine, left, right = all_eps[x, 1], all_eps[x, 0], all_eps[x, 2]
        column.append([
            jnp.where(low_s, rolled(left, 1 - spans, 0), rolled(mine, 1, 0)),
            mine,
            jnp.where(high_s, rolled(right, spans - 1, 0), rolled(mine, -1, 0)),
        ])
    neighbours = [[], [], []]
    for y in range(3):
        inner = column[1][y]
        below = jnp.where(low_c, rolled(column[0][y], spans, 0), rolled(inner, spans, 0))
        above = jnp.where(high_c, rolled(column[2][y], -spans, 0), rolled(inner, -spans, 0))
        neighbours[0].append(jnp.where(closed_low, 0.0, below))
        neighbours[1].append(inner)
        neighbours[2].append(jnp.where(closed_high, 0.0, above))
    interpolate(neighbours, nu)

    lifts, edges = boundary_lifts(masks, closed)

    def outside(ref, axis, v, f):
        return masked_edge(ref[v, f], axis, edges, spans)

    def across(axis, v):
        low, high = masks[axis]
        step = spans if axis == 0 else 1
        grad, ghost, out = grads[axis], whole(ghosts[0][axis]), whole(faces[1][axis])
        for q in range(5):
            for j in range(5):
                f = 5 * q + j
                pts = points(axis, q, j)
                beyond = outside(ghost, axis, v, f)
                gradient = [grad[v, p] + lift * beyond for p, lift in zip(pts, lifts[axis])]
                parts = fold([nu[p] * g for p, g in zip(pts, gradient)])
                left, right = traces(parts)
                ends = jnp.where(low, left, right)
                out[v, f] = ends
                beyond = -shut * ends if axis == 0 else 0.0
                before = jnp.where(low, beyond, rolled(right, step, 0))
                after = jnp.where(high, beyond, rolled(left, -step, 0))
                for p, value in zip(pts, slope(parts, before, after)):
                    if axis == 1:
                        acc[v, p] = value
                    else:
                        acc[v, p] += value

    def normal(v):
        for q in range(5):
            for j in range(5):
                pts = points(2, q, j)
                parts = fold([nu[p] * grads[2][v, p] for p in pts])
                left, right = traces(parts)
                before = jnp.where(first, -left, rolled(right, 1, 1))
                after = jnp.where(last, -right, rolled(left, -1, 1))
                for p, value in zip(pts, slope(parts, before, after)):
                    acc[v, p] += value

    lag = min(LAG, count)

    def variable(v, carry):
        with jax.named_scope("wait_u1"):
            await_bytes(ghosts[0][1].at[v, :, :, pl.ds(0, 2)], state_sem.at[1, v])
        with jax.named_scope("span"):
            across(1, v)
            launch(1, 1, v, only=first_half)
        with jax.named_scope("wait_u0"):
            await_chord(ghosts[0][0], v, state_sem.at[0, v])
        with jax.named_scope("chord"):
            across(0, v)
            launch(1, 0, v)
            due = v >= lag
            launch(1, 1, jnp.maximum(v - lag, 0), only=lambda s: second_half(s) & due)
        return carry

    with jax.named_scope("fluxes"):
        lax.fori_loop(0, count, variable, 0)

    def launch_rest(v, carry):
        launch(1, 1, v, only=second_half)
        return carry

    lax.fori_loop(count - lag, count, launch_rest, 0)

    def rest(v, carry):
        normal(v)
        return carry

    with jax.named_scope("normal"):
        lax.fori_loop(0, count, rest, 0)

    with jax.named_scope("sent0"):
        await_eps(eps_sem.at[0], 2 * chords, spans + 2, 3 * spans)
        all_sent(0)

    def correct(v, carry):
        with jax.named_scope("wait_f1"):
            await_bytes(ghosts[1][1].at[v, :, :, pl.ds(0, 2)], flux_sem.at[v])
        add_fluxes(
            lambda axis, f: outside(whole(ghosts[1][axis]), axis, v, f), lifts,
            lambda p, value: acc.__setitem__((v, p), acc[v, p] + value),
        )
        return carry

    with jax.named_scope("wait_f0"):
        await_chord(ghosts[1][0], every, chord_sem)
    with jax.named_scope("correct"):
        lax.fori_loop(0, count - 1, correct, 0)
        await_bytes(ghosts[1][1].at[count - 1, :, :, pl.ds(0, 2)], flux_sem.at[count - 1])
    with jax.named_scope("sent1"):
        all_sent(1)


def finish_kernel(chord_size, acc, nu, flux_c, flux_s, residual_out, nu_out, last, sems):
    count, chords, spans, lanes = flux_c.shape[0], *flux_c.shape[2:]
    v = count - 1
    copies = (
        pltpu.make_async_copy(acc.at[pl.ds(0, v)], residual_out.at[pl.ds(0, v)], sems.at[0]),
        pltpu.make_async_copy(nu, nu_out, sems.at[1]),
        pltpu.make_async_copy(last, residual_out.at[v], sems.at[2]),
    )
    copies[0].start()
    copies[1].start()
    masks = [row_masks(axis, chords, spans, lanes) for axis in range(2)]
    closed_low, closed_high = closed_rows(chord_size, chords, spans, lanes)
    lifts, edges = boundary_lifts(masks, closed_low | closed_high)
    whole = [ref.reshape(count, 25, chords * spans, lanes) for ref in (flux_c, flux_s)]

    def store(p, value):
        last[p] = acc[v, p] + value

    add_fluxes(
        lambda axis, f: masked_edge(whole[axis][v, f], axis, edges, spans), lifts, store
    )
    copies[2].start()
    for copy in copies:
        copy.wait()


def shards(state):
    count, npts, chords, spans, lanes = state.shape
    rows = chords * spans
    flat = state.reshape(count, npts, rows, lanes)
    f32 = jnp.float32
    sizes = (lax.axis_size("chord"), lax.axis_size("span"))

    def full(*shape):
        return jax.ShapeDtypeStruct(shape, f32)

    vmem = pl.BlockSpec(memory_space=pltpu.VMEM)
    faces = (count, 25, chords, spans, lanes)
    nu, residual, flux_c, flux_s = pl.pallas_call(
        functools.partial(local_kernel, sizes, count, chords, spans),
        in_specs=[pl.BlockSpec(memory_space=pltpu.HBM)],
        out_specs=[vmem] * 4,
        out_shape=[
            full(npts, rows, lanes), full(count, npts, rows, lanes), full(*faces), full(*faces)
        ],
        scratch_shapes=[
            pltpu.VMEM(shape, f32)
            for shape in [
                (count, npts, rows, lanes),
                (3, 3, chords, spans, lanes),
                (2 * chords + 4 * spans + 2, 1, lanes),
                (count, npts, rows, lanes),
                (count, npts, rows, lanes),
                (count, npts, rows, lanes),
            ]
            + [faces] * 6
        ]
        + [
            pltpu.SemaphoreType.DMA((4,)),
            pltpu.SemaphoreType.DMA((3,)),
            pltpu.SemaphoreType.DMA((2, 2)),
            pltpu.SemaphoreType.DMA((2, count)),
            pltpu.SemaphoreType.DMA((count,)),
            pltpu.SemaphoreType.DMA,
            pltpu.SemaphoreType.REGULAR,
        ],
        compiler_params=pltpu.CompilerParams(
            collective_id=0, has_side_effects=True, vmem_limit_bytes=VMEM_BYTES
        ),
    )(flat)
    hbm = pl.BlockSpec(memory_space=pltpu.HBM)
    residual, nu = pl.pallas_call(
        functools.partial(finish_kernel, sizes[0]),
        in_specs=[vmem] * 4,
        out_specs=[hbm, hbm],
        out_shape=[full(count, npts, rows, lanes), full(npts, rows, lanes)],
        scratch_shapes=[pltpu.VMEM((npts, rows, lanes), f32), pltpu.SemaphoreType.DMA((3,))],
        compiler_params=pltpu.CompilerParams(vmem_limit_bytes=FINISH_BYTES),
    )(residual, nu, flux_c, flux_s)
    return residual.reshape(state.shape), nu.reshape(npts, chords, spans, lanes)


def solution(mesh):
    in_specs = (P(None, None, "chord", "span", None),)
    out_specs = (P(None, None, "chord", "span", None), P(None, "chord", "span", None))
    return jax.shard_map(shards, mesh=mesh, in_specs=in_specs, out_specs=out_specs, check_vma=False)
```

```python
import functools
import math

import jax
import jax.numpy as jnp
import numpy as np
from jax import lax
from jax.experimental import pallas as pl
from jax.experimental.pallas import tpu as pltpu
from jax.sharding import PartitionSpec as P

VMEM_BYTES = 50_750_000
FINISH_BYTES = 8_000_000
HELD = 2
LAG = 3
EPS_SCALE = 0.01
SENSOR_CENTRE = -3.0
SENSOR_WIDTH = 1.5
RATIO_FLOOR = 1e-06
ENERGY_EPS = 1e-06
GAUSS_NODES = [-0.906179845938664, -0.5384693101056831, 0.0, 0.5384693101056831, 0.906179845938664]
GAUSS_WEIGHTS = [
    0.2369268850561891,
    0.4786286704993665,
    0.5688888888888889,
    0.4786286704993665,
    0.2369268850561891,
]


def legendre_values(points):
    values = [np.ones(points.shape), np.array(points)]
    for order in range(1, 5):
        values.append(
            ((2 * order + 1) * points * values[order] - order * values[order - 1]) / (order + 1)
        )
    return values


def line_tables():
    line_nodes = np.array(GAUSS_NODES)
    quadrature_weights = np.array(GAUSS_WEIGHTS)
    barycentric = np.array(
        [
            1.0 / np.prod([line_nodes[j] - line_nodes[k] for k in range(5) if k != j])
            for j in range(5)
        ]
    )
    derivative = np.zeros((5, 5))
    for i in range(5):
        for j in range(5):
            if i != j:
                derivative[i, j] = barycentric[j] / barycentric[i] / (line_nodes[i] - line_nodes[j])
        derivative[i, i] = -np.sum(derivative[i])
    left_values = np.ones(5)
    right_values = np.ones(5)
    for j in range(5):
        for k in range(5):
            if k != j:
                left_values[j] *= (-1.0 - line_nodes[k]) / (line_nodes[j] - line_nodes[k])
                right_values[j] *= (1.0 - line_nodes[k]) / (line_nodes[j] - line_nodes[k])
    legendre = legendre_values(line_nodes)
    fourth_slope = 7.0 * legendre[3] + 3.0 * legendre[1]
    fifth_slope = 9.0 * legendre[4] + 5.0 * legendre[2] + legendre[0]
    left_corr = 0.5 * (fourth_slope - fifth_slope)
    right_corr = 0.5 * (fourth_slope + fifth_slope)
    modal = np.zeros((5, 5))
    for k in range(5):
        modal[k, :] = quadrature_weights * math.sqrt((2 * k + 1) / 2.0) * legendre[k]
    return (line_nodes, derivative, left_values, right_values, left_corr, right_corr, modal)


NODES, DERIV, LEFT, RIGHT, LIFT_LEFT, LIFT_RIGHT, MODAL = line_tables()
HALF_LEFT = 0.5 * LIFT_LEFT
HALF_RIGHT = 0.5 * LIFT_RIGHT


def fold(u):
    return (u[0] + u[4], u[1] + u[3], u[2], u[0] - u[4], u[1] - u[3])


def traces(parts):
    s0, s1, mid, d0, d1 = parts
    r = [float(x) for x in RIGHT]
    even = 0.5 * (r[0] + r[4]) * s0 + 0.5 * (r[1] + r[3]) * s1 + r[2] * mid
    odd = 0.5 * (r[0] - r[4]) * d0 + 0.5 * (r[1] - r[3]) * d1
    return even - odd, even + odd


def slope(parts, before, after):
    s0, s1, mid, d0, d1 = parts
    h = [float(x) for x in HALF_LEFT]
    r = [float(x) for x in RIGHT]
    if before is not None:
        diff, both = before - after, before + after
    even, odd = [], []
    for i in range(3):
        lift = 0.5 * (h[i] + h[4 - i])
        value = (
            float(0.5 * (DERIV[i, 0] - DERIV[i, 4]) + lift * (r[0] - r[4])) * d0
            + float(0.5 * (DERIV[i, 1] - DERIV[i, 3]) + lift * (r[1] - r[3])) * d1
        )
        even.append(value if before is None else value + lift * diff)
    for i in range(2):
        lift = 0.5 * (h[i] - h[4 - i])
        value = (
            float(0.5 * (DERIV[i, 0] + DERIV[i, 4]) - lift * (r[0] + r[4])) * s0
            + float(0.5 * (DERIV[i, 1] + DERIV[i, 3]) - lift * (r[1] + r[3])) * s1
            + float(DERIV[i, 2] - 2.0 * lift * r[2]) * mid
        )
        odd.append(value if before is None else value + lift * both)
    return [even[0] + odd[0], even[1] + odd[1], even[2], even[1] - odd[1], even[0] - odd[0]]


def points(axis, q, j):
    if axis == 0:
        return [25 * i + 5 * q + j for i in range(5)]
    if axis == 1:
        return [25 * q + 5 * i + j for i in range(5)]
    return [25 * q + 5 * j + i for i in range(5)]


TOP = [float(x) for x in MODAL[4]]
WEIGHTS = [float(x) for x in GAUSS_WEIGHTS]


def total_of(values):
    out = values[0]
    for value in values[1:]:
        out = out + value
    return out


def symmetric(coefficients, u):
    c = coefficients
    return c[0] * (u[0] + u[4]) + c[1] * (u[1] + u[3]) + c[2] * u[2]


def energy(values):
    return symmetric(WEIGHTS, [x * x for x in values])


def sensor(load):
    planes = {"y": [], "z": [], "yz": [], "total": [], "ez": [], "ey": [], "eyz": []}
    top_x = {}
    for a in range(5):
        u = [[load(25 * a + 5 * b + c) for c in range(5)] for b in range(5)]
        for b in range(5):
            for c in range(5):
                term = TOP[a] * u[b][c]
                top_x[b, c] = term if a == 0 else top_x[b, c] + term
        z = [symmetric(TOP, u[b]) for b in range(5)]
        y = [symmetric(TOP, [u[b][c] for b in range(5)]) for c in range(5)]
        yz = symmetric(TOP, z)
        planes["total"].append(symmetric(WEIGHTS, [energy(u[b]) for b in range(5)]))
        planes["ez"].append(energy(z))
        planes["ey"].append(energy(y))
        planes["eyz"].append(yz * yz)
        planes["z"].append(z)
        planes["y"].append(y)
        planes["yz"].append(yz)
    total, e_z, e_y, e_yz = (symmetric(WEIGHTS, planes[k]) for k in ("total", "ez", "ey", "eyz"))
    x_z = [symmetric(TOP, [planes["z"][a][b] for a in range(5)]) for b in range(5)]
    x_y = [symmetric(TOP, [planes["y"][a][c] for a in range(5)]) for c in range(5)]
    x_yz = symmetric(TOP, planes["yz"])
    e_x = symmetric(WEIGHTS, [energy([top_x[b, c] for c in range(5)]) for b in range(5)])
    high = e_x + (e_y - energy(x_y)) + ((e_z - energy(x_z)) - (e_yz - x_yz * x_yz))
    level = jnp.log(jnp.maximum(high / (total + ENERGY_EPS), RATIO_FLOOR)) * (1.0 / math.log(10.0))
    ramp = jnp.clip((level - SENSOR_CENTRE) / SENSOR_WIDTH, -1.0, 1.0)
    return EPS_SCALE * 0.5 * (1.0 + jnp.sin(0.5 * math.pi * ramp))


def rolled(value, shift, axis):
    size = value.shape[axis]
    return pltpu.roll(value, shift % size, axis)


LOWER = [float((1.0 - x) / 2.0) for x in NODES]
UPPER = [float((1.0 + x) / 2.0) for x in NODES]


def along_lanes(line):
    lanes = line.shape[1]
    lane = lax.broadcasted_iota(jnp.int32, line.shape, 1)
    before = jnp.where(lane == 0, 0.0, rolled(line, 1, 1))
    after = jnp.where(lane == lanes - 1, 0.0, rolled(line, -1, 1))
    return jnp.maximum(line, before), jnp.maximum(line, after)


def interpolate(neighbours, nu):
    corner = {}
    for x in range(2):
        for y in range(2):
            line = jnp.maximum(
                jnp.maximum(neighbours[x][y], neighbours[x + 1][y]),
                jnp.maximum(neighbours[x][y + 1], neighbours[x + 1][y + 1]),
            )
            corner[x, y, 0], corner[x, y, 1] = along_lanes(line)
    lower, upper = LOWER, UPPER
    for a in range(5):
        face = {
            (y, z): lower[a] * corner[0, y, z] + upper[a] * corner[1, y, z]
            for y in range(2)
            for z in range(2)
        }
        for b in range(5):
            edge = [lower[b] * face[0, z] + upper[b] * face[1, z] for z in range(2)]
            for c in range(5):
                nu[25 * a + 5 * b + c] = lower[c] * edge[0] + upper[c] * edge[1]


def row_masks(axis, chords, spans, lanes):
    row = lax.broadcasted_iota(jnp.int32, (chords * spans, lanes), 0)
    if axis == 0:
        return row < spans, row >= (chords - 1) * spans
    place = row % spans
    return place == 0, place == spans - 1


def closed_rows(chord_size, chords, spans, lanes):
    rows = chords * spans
    me_c = lax.axis_index("chord")
    row = lax.broadcasted_iota(jnp.int32, (rows, lanes), 0)
    have_low = jnp.where(me_c > 0, spans, 0)
    have_high = jnp.where(me_c + 1 < chord_size, rows, rows - spans)
    return row < spans - have_low, row >= have_high


def boundary_lifts(masks, closed):
    lifts = [
        [
            jnp.where(low, float(HALF_LEFT[i]), jnp.where(high, float(HALF_RIGHT[i]), 0.0))
            for i in range(5)
        ]
        for low, high in masks
    ]
    edges = [(low | high) for low, high in masks]
    edges[0] = edges[0] & jnp.logical_not(closed)
    return lifts, edges


def masked_edge(value, axis, edges, spans):
    return value if axis == 1 and spans <= 2 else jnp.where(edges[axis], value, 0.0)


def add_fluxes(flux, lifts, store):
    for c in range(5):
        along = [[flux(axis, 5 * m + c) for m in range(5)] for axis in range(2)]
        for a in range(5):
            for b in range(5):
                store(25 * a + 5 * b + c, lifts[0][a] * along[0][b] + lifts[1][b] * along[1][a])


def local_kernel(sizes, count, chords, spans, *refs):
    state_hbm = refs[0]
    nu, acc = refs[1:3]
    state, around, tally = refs[5:8]
    grads = refs[8:11]
    faces = (refs[11:13], refs[13:15])
    ghosts = (refs[15:17], refs[3:5])
    load_sem, eps_sem, send_sem, state_sem, flux_sem, chord_sem, answer = refs[17:]
    rows, lanes = nu.shape[1:]
    chord_size, span_size = sizes
    me_c, me_s = lax.axis_index("chord"), lax.axis_index("span")
    mesh_id = pl.DeviceIdType.MESH

    def whole(ref):
        return ref.reshape(count, 25, rows, lanes)

    all_eps = around.reshape(3, 3, rows, lanes)

    def reachable(dx):
        if dx == 0:
            return None
        return me_c + 1 < chord_size if dx == 1 else me_c > 0

    def guarded(cond, run):
        if cond is None:
            run()
        else:
            pl.when(cond)(run)

    def partner(dx, dy):
        return (me_c + dx, lax.rem(me_s + dy + span_size, span_size))

    level = ((0, -1), (0, 1))
    lower, upper = (tuple((dx, dy) for dy in (0, -1, 1)) for dx in (-1, 1))

    def greet(sem, offsets):
        for dx, dy in offsets:
            pl.semaphore_signal(sem, inc=1, device_id=partner(dx, dy), device_id_type=mesh_id)

    barrier = pltpu.get_barrier_semaphore()
    def load(k, *part):
        return pltpu.make_async_copy(state_hbm.at[part], state.at[part], load_sem.at[k])

    start, remainder = load(0, 0, pl.ds(0, 75)), load(1, 0, pl.ds(75, 50))
    second, others = load(2, pl.ds(1, 1)), load(3, pl.ds(2, count - 2))
    for copy in (start, remainder, second, others):
        copy.start()

    greet(barrier, level)

    guarded(reachable(1), lambda: greet(barrier, upper))

    def edge_of(step, size):
        return pl.ds(0, size) if step == 0 else (size - 1 if step == 1 else 0)

    def eps_copy(dx, dy):
        part = (edge_of(dx, chords), edge_of(dy, spans))
        return pltpu.make_async_remote_copy(
            src_ref=around.at[(1, 1) + part], dst_ref=around.at[(1 - dx, 1 - dy) + part],
            send_sem=eps_sem.at[0], recv_sem=eps_sem.at[1 if dx == 0 else 2],
            device_id=partner(dx, dy), device_id_type=mesh_id,
        )

    def column_copy():
        return pltpu.make_async_remote_copy(
            src_ref=around.at[1, :, chords - 1], dst_ref=around.at[0, :, chords - 1],
            send_sem=eps_sem.at[0], recv_sem=eps_sem.at[2],
            device_id=partner(1, 0), device_id_type=mesh_id,
        )

    ways = ((1, 0), (-1, 0), (0, 1), (0, -1))

    def side(ref, axis, v, last, part):
        if axis == 0:
            return ref.at[v, part, chords - 1 if last else 0]
        return ref.at[v, part, :, spans - 1 if last else 0]

    def recv_sem(stage, axis, v):
        if stage == 0:
            return state_sem.at[axis, v]
        return chord_sem if axis == 0 else flux_sem.at[jnp.where(v < count - 1, 0, 1)]

    def send_eps(offsets):
        for dx, dy in offsets:
            eps_copy(dx, dy).start()

    def launch(stage, axis, v, sides=(0, 1), part=pl.ds(0, 25), only=None):
        for k in (2 * axis + i for i in sides):
            dx, dy = ways[k]
            up = k % 2 == 0

            def start():
                pltpu.make_async_remote_copy(
                    src_ref=side(faces[stage][axis], axis, v, up, part),
                    dst_ref=side(ghosts[stage][axis], axis, v, not up, part),
                    send_sem=send_sem.at[stage, axis], recv_sem=recv_sem(stage, axis, v),
                    device_id=partner(dx, dy), device_id_type=mesh_id,
                ).start()

            allowed = reachable(dx) if only is None else only(partner(dx, dy)[1])
            guarded(allowed, start)

    def first_half(s):
        return s < span_size // 2

    def second_half(s):
        return s >= span_size // 2

    def by_one_link(s):
        return (s % 4 == 1) | (s % 4 == 2)

    two_sided = (me_c > 0) & (me_c + 1 < chord_size)

    def await_bytes(ref, sem):
        pltpu.make_async_copy(ref, ref, sem).wait()

    def await_chord(ref, part, sem):
        pl.when(two_sided)(lambda: await_bytes(ref.at[part, :, pl.ds(0, 2)], sem))
        pl.when(jnp.logical_not(two_sided))(lambda: await_bytes(ref.at[part, :, pl.ds(0, 1)], sem))

    def await_eps(sem, base, below, above):
        has_below, has_above = me_c > 0, me_c + 1 < chord_size
        for use_below in (False, True):
            for use_above in (False, True):
                size = base + use_below * below + use_above * above
                if size:
                    case = (has_below == use_below) & (has_above == use_above)
                    pl.when(case)(lambda size=size: await_bytes(tally.at[pl.ds(0, size)], sem))

    every = pl.ds(0, count)

    def all_sent(stage):
        await_chord(faces[stage][0], every, send_sem.at[stage, 0])
        await_bytes(faces[stage][1].at[:, :, :, pl.ds(0, 2)], send_sem.at[stage, 1])

    masks = [row_masks(axis, chords, spans, lanes) for axis in range(2)]

    def form_traces(axis, v, lines=range(5)):
        low = masks[axis][0]
        ends = [jnp.where(low, float(LEFT[i]), float(RIGHT[i])) for i in range(5)]
        out = whole(faces[0][axis])
        for q in lines:
            for j in range(5):
                pts = points(axis, q, j)
                out[v, 5 * q + j] = total_of([e * state[v, p] for e, p in zip(ends, pts)])

    with jax.named_scope("load0"):
        start.wait()
    form_traces(1, 0, range(3))
    with jax.named_scope("barrier"):
        pl.semaphore_wait(barrier, 2 + jnp.where(me_c > 0, 3, 0))
    launch(0, 1, 0, part=pl.ds(0, 15))
    guarded(reachable(-1), lambda: greet(answer, ((-1, 0),)))
    with jax.named_scope("sensor"):
        remainder.wait()
        eps = sensor(lambda p: state[0, p])
        all_eps[1, 1] = eps
    send_eps(level)
    guarded(reachable(-1), lambda: send_eps(lower))
    form_traces(1, 0, range(3, 5))
    launch(0, 1, 0, part=pl.ds(15, 10))
    with jax.named_scope("later"):
        def span_traces(v, carry):
            form_traces(1, v)
            early = v < count - held
            launch(0, 1, v, only=lambda s: jnp.logical_not(by_one_link(s)) | early)
            return carry

        held = min(HELD, count - 1)
        second.wait()
        span_traces(1, 0)
        others.wait()
        lax.fori_loop(2, count, span_traces, 0)

        def chord_traces(v, carry):
            form_traces(0, v)
            launch(0, 0, v, (1,))
            return carry

        lax.fori_loop(0, count, chord_traces, 0)

    lane = lax.broadcasted_iota(jnp.int32, (rows, lanes), 1)
    first, last = lane == 0, lane == lanes - 1
    low_s, high_s = masks[1]
    low_c, high_c = masks[0]
    closed_low, closed_high = closed_rows(sizes[0], chords, spans, lanes)
    closed = closed_low | closed_high
    shut = jnp.where(closed, 1.0, 0.0)

    def normal_gradient(v, carry):
        grad = grads[2]
        for q in range(5):
            for j in range(5):
                pts = points(2, q, j)
                parts = fold([state[v, p] for p in pts])
                left, right = traces(parts)
                before = jnp.where(first, left, rolled(right, 1, 1))
                after = jnp.where(last, right, rolled(left, -1, 1))
                for p, value in zip(pts, slope(parts, before, after)):
                    grad[v, p] = value
        return carry

    def across_gradient(axis):
        low, high = masks[axis]
        step = spans if axis == 0 else 1
        mine, grad = whole(faces[0][axis]), grads[axis]

        def body(v, carry):
            for q in range(5):
                for j in range(5):
                    pts = points(axis, q, j)
                    parts = fold([state[v, p] for p in pts])
                    left, right = traces(parts)
                    beyond = shut * mine[v, 5 * q + j] if axis == 0 else 0.0
                    before = jnp.where(low, beyond, rolled(right, step, 0))
                    after = jnp.where(high, beyond, rolled(left, -step, 0))
                    for p, value in zip(pts, slope(parts, before, after)):
                        grad[v, p] = value
            return carry

        return body

    with jax.named_scope("ngrad"):
        lax.fori_loop(0, count, normal_gradient, 0)
    with jax.named_scope("sgrad"):
        lax.fori_loop(0, count, across_gradient(1), 0)

    with jax.named_scope("level"):
        await_bytes(tally.at[pl.ds(0, 2 * chords)], eps_sem.at[1])
    with jax.named_scope("answer"):

        @pl.when(reachable(1))
        def _():
            pl.semaphore_wait(answer, 1)
            column_copy().start()

        def chord_up(v, carry):
            launch(0, 0, v, (0,))
            return carry

        lax.fori_loop(0, count, chord_up, 0)

    def launch_held(v, carry):
        launch(0, 1, v, only=by_one_link)
        return carry

    lax.fori_loop(count - held, count, launch_held, 0)

    with jax.named_scope("cgrad"):
        lax.fori_loop(0, count, across_gradient(0), 0)

    with jax.named_scope("epswait"):
        await_eps(eps_sem.at[2], 0, 3 * spans, spans + 2)

    column = []
    for x in range(3):
        mine, left, right = all_eps[x, 1], all_eps[x, 0], all_eps[x, 2]
        column.append([
            jnp.where(low_s, rolled(left, 1 - spans, 0), rolled(mine, 1, 0)),
            mine,
            jnp.where(high_s, rolled(right, spans - 1, 0), rolled(mine, -1, 0)),
        ])
    neighbours = [[], [], []]
    for y in range(3):
        inner = column[1][y]
        below = jnp.where(low_c, rolled(column[0][y], spans, 0), rolled(inner, spans, 0))
        above = jnp.where(high_c, rolled(column[2][y], -spans, 0), rolled(inner, -spans, 0))
        neighbours[0].append(jnp.where(closed_low, 0.0, below))
        neighbours[1].append(inner)
        neighbours[2].append(jnp.where(closed_high, 0.0, above))
    interpolate(neighbours, nu)

    lifts, edges = boundary_lifts(masks, closed)

    def outside(ref, axis, v, f):
        return masked_edge(ref[v, f], axis, edges, spans)

    def across(axis, v):
        low, high = masks[axis]
        step = spans if axis == 0 else 1
        grad, ghost, out = grads[axis], whole(ghosts[0][axis]), whole(faces[1][axis])
        for q in range(5):
            for j in range(5):
                f = 5 * q + j
                pts = points(axis, q, j)
                beyond = outside(ghost, axis, v, f)
                gradient = [grad[v, p] + lift * beyond for p, lift in zip(pts, lifts[axis])]
                parts = fold([nu[p] * g for p, g in zip(pts, gradient)])
                left, right = traces(parts)
                ends = jnp.where(low, left, right)
                out[v, f] = ends
                beyond = -shut * ends if axis == 0 else 0.0
                before = jnp.where(low, beyond, rolled(right, step, 0))
                after = jnp.where(high, beyond, rolled(left, -step, 0))
                for p, value in zip(pts, slope(parts, before, after)):
                    if axis == 1:
                        acc[v, p] = value
                    else:
                        acc[v, p] += value

    def normal(v):
        for q in range(5):
            for j in range(5):
                pts = points(2, q, j)
                parts = fold([nu[p] * grads[2][v, p] for p in pts])
                left, right = traces(parts)
                before = jnp.where(first, -left, rolled(right, 1, 1))
                after = jnp.where(last, -right, rolled(left, -1, 1))
                for p, value in zip(pts, slope(parts, before, after)):
                    acc[v, p] += value

    lag = min(LAG, count)

    def variable(v, carry):
        with jax.named_scope("wait_u1"):
            await_bytes(ghosts[0][1].at[v, :, :, pl.ds(0, 2)], state_sem.at[1, v])
        with jax.named_scope("span"):
            across(1, v)
            launch(1, 1, v, only=first_half)
        with jax.named_scope("wait_u0"):
            await_chord(ghosts[0][0], v, state_sem.at[0, v])
        with jax.named_scope("chord"):
            across(0, v)
            launch(1, 0, v)
            due = v >= lag
            launch(1, 1, jnp.maximum(v - lag, 0), only=lambda s: second_half(s) & due)
        return carry

    with jax.named_scope("fluxes"):
        lax.fori_loop(0, count, variable, 0)

    def launch_rest(v, carry):
        launch(1, 1, v, only=second_half)
        return carry

    lax.fori_loop(count - lag, count, launch_rest, 0)

    def rest(v, carry):
        normal(v)
        return carry

    with jax.named_scope("normal"):
        lax.fori_loop(0, count, rest, 0)

    with jax.named_scope("sent0"):
        await_eps(eps_sem.at[0], 2 * chords, spans + 2, 3 * spans)
        all_sent(0)

    def correct(v, carry):
        add_fluxes(
            lambda axis, f: outside(whole(ghosts[1][axis]), axis, v, f), lifts,
            lambda p, value: acc.__setitem__((v, p), acc[v, p] + value),
        )
        return carry

    with jax.named_scope("wait_f0"):
        await_chord(ghosts[1][0], every, chord_sem)
    with jax.named_scope("correct"):
        await_bytes(
            ghosts[1][1].at[pl.ds(0, count - 1), :, :, pl.ds(0, 2)], flux_sem.at[0]
        )
        lax.fori_loop(0, count - 1, correct, 0)
        await_bytes(ghosts[1][1].at[count - 1, :, :, pl.ds(0, 2)], flux_sem.at[1])
    with jax.named_scope("sent1"):
        all_sent(1)


def finish_kernel(chord_size, acc, nu, flux_c, flux_s, residual_out, nu_out, last, sems):
    count, chords, spans, lanes = flux_c.shape[0], *flux_c.shape[2:]
    v = count - 1
    copies = (
        pltpu.make_async_copy(acc.at[pl.ds(0, v)], residual_out.at[pl.ds(0, v)], sems.at[0]),
        pltpu.make_async_copy(nu, nu_out, sems.at[1]),
        pltpu.make_async_copy(last, residual_out.at[v], sems.at[2]),
    )
    copies[0].start()
    copies[1].start()
    masks = [row_masks(axis, chords, spans, lanes) for axis in range(2)]
    closed_low, closed_high = closed_rows(chord_size, chords, spans, lanes)
    lifts, edges = boundary_lifts(masks, closed_low | closed_high)
    whole = [ref.reshape(count, 25, chords * spans, lanes) for ref in (flux_c, flux_s)]

    def store(p, value):
        last[p] = acc[v, p] + value

    add_fluxes(
        lambda axis, f: masked_edge(whole[axis][v, f], axis, edges, spans), lifts, store
    )
    copies[2].start()
    for copy in copies:
        copy.wait()


def shards(state):
    count, npts, chords, spans, lanes = state.shape
    rows = chords * spans
    flat = state.reshape(count, npts, rows, lanes)
    f32 = jnp.float32
    sizes = (lax.axis_size("chord"), lax.axis_size("span"))

    def full(*shape):
        return jax.ShapeDtypeStruct(shape, f32)

    vmem = pl.BlockSpec(memory_space=pltpu.VMEM)
    faces = (count, 25, chords, spans, lanes)
    nu, residual, flux_c, flux_s = pl.pallas_call(
        functools.partial(local_kernel, sizes, count, chords, spans),
        in_specs=[pl.BlockSpec(memory_space=pltpu.HBM)],
        out_specs=[vmem] * 4,
        out_shape=[
            full(npts, rows, lanes), full(count, npts, rows, lanes), full(*faces), full(*faces)
        ],
        scratch_shapes=[
            pltpu.VMEM(shape, f32)
            for shape in [
                (count, npts, rows, lanes),
                (3, 3, chords, spans, lanes),
                (2 * chords + 4 * spans + 2, 1, lanes),
                (count, npts, rows, lanes),
                (count, npts, rows, lanes),
                (count, npts, rows, lanes),
            ]
            + [faces] * 6
        ]
        + [
            pltpu.SemaphoreType.DMA((4,)),
            pltpu.SemaphoreType.DMA((3,)),
            pltpu.SemaphoreType.DMA((2, 2)),
            pltpu.SemaphoreType.DMA((2, count)),
            pltpu.SemaphoreType.DMA((2,)),
            pltpu.SemaphoreType.DMA,
            pltpu.SemaphoreType.REGULAR,
        ],
        compiler_params=pltpu.CompilerParams(
            collective_id=0, has_side_effects=True, vmem_limit_bytes=VMEM_BYTES
        ),
    )(flat)
    hbm = pl.BlockSpec(memory_space=pltpu.HBM)
    residual, nu = pl.pallas_call(
        functools.partial(finish_kernel, sizes[0]),
        in_specs=[vmem] * 4,
        out_specs=[hbm, hbm],
        out_shape=[full(count, npts, rows, lanes), full(npts, rows, lanes)],
        scratch_shapes=[pltpu.VMEM((npts, rows, lanes), f32), pltpu.SemaphoreType.DMA((3,))],
        compiler_params=pltpu.CompilerParams(vmem_limit_bytes=FINISH_BYTES),
    )(residual, nu, flux_c, flux_s)
    return residual.reshape(state.shape), nu.reshape(npts, chords, spans, lanes)


def solution(mesh):
    in_specs = (P(None, None, "chord", "span", None),)
    out_specs = (P(None, None, "chord", "span", None), P(None, "chord", "span", None))
    return jax.shard_map(shards, mesh=mesh, in_specs=in_specs, out_specs=out_specs, check_vma=False)
```

```python
import functools
import math

import jax
import jax.numpy as jnp
import numpy as np
from jax import lax
from jax.experimental import pallas as pl
from jax.experimental.pallas import tpu as pltpu
from jax.sharding import PartitionSpec as P

VMEM_BYTES = 50_750_000
FINISH_BYTES = 8_000_000
HELD = 2
LAG = 3
EPS_SCALE = 0.01
SENSOR_CENTRE = -3.0
SENSOR_WIDTH = 1.5
RATIO_FLOOR = 1e-06
ENERGY_EPS = 1e-06
GAUSS_NODES = [-0.906179845938664, -0.5384693101056831, 0.0, 0.5384693101056831, 0.906179845938664]
GAUSS_WEIGHTS = [
    0.2369268850561891,
    0.4786286704993665,
    0.5688888888888889,
    0.4786286704993665,
    0.2369268850561891,
]


def legendre_values(points):
    values = [np.ones(points.shape), np.array(points)]
    for order in range(1, 5):
        values.append(
            ((2 * order + 1) * points * values[order] - order * values[order - 1]) / (order + 1)
        )
    return values


def line_tables():
    line_nodes = np.array(GAUSS_NODES)
    quadrature_weights = np.array(GAUSS_WEIGHTS)
    barycentric = np.array(
        [
            1.0 / np.prod([line_nodes[j] - line_nodes[k] for k in range(5) if k != j])
            for j in range(5)
        ]
    )
    derivative = np.zeros((5, 5))
    for i in range(5):
        for j in range(5):
            if i != j:
                derivative[i, j] = barycentric[j] / barycentric[i] / (line_nodes[i] - line_nodes[j])
        derivative[i, i] = -np.sum(derivative[i])
    left_values = np.ones(5)
    right_values = np.ones(5)
    for j in range(5):
        for k in range(5):
            if k != j:
                left_values[j] *= (-1.0 - line_nodes[k]) / (line_nodes[j] - line_nodes[k])
                right_values[j] *= (1.0 - line_nodes[k]) / (line_nodes[j] - line_nodes[k])
    legendre = legendre_values(line_nodes)
    fourth_slope = 7.0 * legendre[3] + 3.0 * legendre[1]
    fifth_slope = 9.0 * legendre[4] + 5.0 * legendre[2] + legendre[0]
    left_corr = 0.5 * (fourth_slope - fifth_slope)
    right_corr = 0.5 * (fourth_slope + fifth_slope)
    modal = np.zeros((5, 5))
    for k in range(5):
        modal[k, :] = quadrature_weights * math.sqrt((2 * k + 1) / 2.0) * legendre[k]
    return (line_nodes, derivative, left_values, right_values, left_corr, right_corr, modal)


NODES, DERIV, LEFT, RIGHT, LIFT_LEFT, LIFT_RIGHT, MODAL = line_tables()
HALF_LEFT = 0.5 * LIFT_LEFT
HALF_RIGHT = 0.5 * LIFT_RIGHT


def fold(u):
    return (u[0] + u[4], u[1] + u[3], u[2], u[0] - u[4], u[1] - u[3])


def traces(parts):
    s0, s1, mid, d0, d1 = parts
    r = [float(x) for x in RIGHT]
    even = 0.5 * (r[0] + r[4]) * s0 + 0.5 * (r[1] + r[3]) * s1 + r[2] * mid
    odd = 0.5 * (r[0] - r[4]) * d0 + 0.5 * (r[1] - r[3]) * d1
    return even - odd, even + odd


def slope(parts, before, after):
    s0, s1, mid, d0, d1 = parts
    h = [float(x) for x in HALF_LEFT]
    r = [float(x) for x in RIGHT]
    if before is not None:
        diff, both = before - after, before + after
    even, odd = [], []
    for i in range(3):
        lift = 0.5 * (h[i] + h[4 - i])
        value = (
            float(0.5 * (DERIV[i, 0] - DERIV[i, 4]) + lift * (r[0] - r[4])) * d0
            + float(0.5 * (DERIV[i, 1] - DERIV[i, 3]) + lift * (r[1] - r[3])) * d1
        )
        even.append(value if before is None else value + lift * diff)
    for i in range(2):
        lift = 0.5 * (h[i] - h[4 - i])
        value = (
            float(0.5 * (DERIV[i, 0] + DERIV[i, 4]) - lift * (r[0] + r[4])) * s0
            + float(0.5 * (DERIV[i, 1] + DERIV[i, 3]) - lift * (r[1] + r[3])) * s1
            + float(DERIV[i, 2] - 2.0 * lift * r[2]) * mid
        )
        odd.append(value if before is None else value + lift * both)
    return [even[0] + odd[0], even[1] + odd[1], even[2], even[1] - odd[1], even[0] - odd[0]]


def points(axis, q, j):
    if axis == 0:
        return [25 * i + 5 * q + j for i in range(5)]
    if axis == 1:
        return [25 * q + 5 * i + j for i in range(5)]
    return [25 * q + 5 * j + i for i in range(5)]


TOP = [float(x) for x in MODAL[4]]
WEIGHTS = [float(x) for x in GAUSS_WEIGHTS]


def total_of(values):
    out = values[0]
    for value in values[1:]:
        out = out + value
    return out


def symmetric(coefficients, u):
    c = coefficients
    return c[0] * (u[0] + u[4]) + c[1] * (u[1] + u[3]) + c[2] * u[2]


def energy(values):
    return symmetric(WEIGHTS, [x * x for x in values])


def sensor(load):
    planes = {"y": [], "z": [], "yz": [], "total": [], "ez": [], "ey": [], "eyz": []}
    top_x = {}
    for a in range(5):
        u = [[load(25 * a + 5 * b + c) for c in range(5)] for b in range(5)]
        for b in range(5):
            for c in range(5):
                term = TOP[a] * u[b][c]
                top_x[b, c] = term if a == 0 else top_x[b, c] + term
        z = [symmetric(TOP, u[b]) for b in range(5)]
        y = [symmetric(TOP, [u[b][c] for b in range(5)]) for c in range(5)]
        yz = symmetric(TOP, z)
        planes["total"].append(symmetric(WEIGHTS, [energy(u[b]) for b in range(5)]))
        planes["ez"].append(energy(z))
        planes["ey"].append(energy(y))
        planes["eyz"].append(yz * yz)
        planes["z"].append(z)
        planes["y"].append(y)
        planes["yz"].append(yz)
    total, e_z, e_y, e_yz = (symmetric(WEIGHTS, planes[k]) for k in ("total", "ez", "ey", "eyz"))
    x_z = [symmetric(TOP, [planes["z"][a][b] for a in range(5)]) for b in range(5)]
    x_y = [symmetric(TOP, [planes["y"][a][c] for a in range(5)]) for c in range(5)]
    x_yz = symmetric(TOP, planes["yz"])
    e_x = symmetric(WEIGHTS, [energy([top_x[b, c] for c in range(5)]) for b in range(5)])
    high = e_x + (e_y - energy(x_y)) + ((e_z - energy(x_z)) - (e_yz - x_yz * x_yz))
    level = jnp.log(jnp.maximum(high / (total + ENERGY_EPS), RATIO_FLOOR)) * (1.0 / math.log(10.0))
    ramp = jnp.clip((level - SENSOR_CENTRE) / SENSOR_WIDTH, -1.0, 1.0)
    return EPS_SCALE * 0.5 * (1.0 + jnp.sin(0.5 * math.pi * ramp))


def rolled(value, shift, axis):
    size = value.shape[axis]
    return pltpu.roll(value, shift % size, axis)


LOWER = [float((1.0 - x) / 2.0) for x in NODES]
UPPER = [float((1.0 + x) / 2.0) for x in NODES]


def along_lanes(line):
    lanes = line.shape[1]
    lane = lax.broadcasted_iota(jnp.int32, line.shape, 1)
    before = jnp.where(lane == 0, 0.0, rolled(line, 1, 1))
    after = jnp.where(lane == lanes - 1, 0.0, rolled(line, -1, 1))
    return jnp.maximum(line, before), jnp.maximum(line, after)


def interpolate(neighbours, nu):
    corner = {}
    for x in range(2):
        for y in range(2):
            line = jnp.maximum(
                jnp.maximum(neighbours[x][y], neighbours[x + 1][y]),
                jnp.maximum(neighbours[x][y + 1], neighbours[x + 1][y + 1]),
            )
            corner[x, y, 0], corner[x, y, 1] = along_lanes(line)
    lower, upper = LOWER, UPPER
    for a in range(5):
        face = {
            (y, z): lower[a] * corner[0, y, z] + upper[a] * corner[1, y, z]
            for y in range(2)
            for z in range(2)
        }
        for b in range(5):
            edge = [lower[b] * face[0, z] + upper[b] * face[1, z] for z in range(2)]
            for c in range(5):
                nu[25 * a + 5 * b + c] = lower[c] * edge[0] + upper[c] * edge[1]


def row_masks(axis, chords, spans, lanes):
    row = lax.broadcasted_iota(jnp.int32, (chords * spans, lanes), 0)
    if axis == 0:
        return row < spans, row >= (chords - 1) * spans
    place = row % spans
    return place == 0, place == spans - 1


def closed_rows(chord_size, chords, spans, lanes):
    rows = chords * spans
    me_c = lax.axis_index("chord")
    row = lax.broadcasted_iota(jnp.int32, (rows, lanes), 0)
    have_low = jnp.where(me_c > 0, spans, 0)
    have_high = jnp.where(me_c + 1 < chord_size, rows, rows - spans)
    return row < spans - have_low, row >= have_high


def boundary_lifts(masks, closed):
    lifts = [
        [
            jnp.where(low, float(HALF_LEFT[i]), jnp.where(high, float(HALF_RIGHT[i]), 0.0))
            for i in range(5)
        ]
        for low, high in masks
    ]
    edges = [(low | high) for low, high in masks]
    edges[0] = edges[0] & jnp.logical_not(closed)
    return lifts, edges


def masked_edge(value, axis, edges, spans):
    return value if axis == 1 and spans <= 2 else jnp.where(edges[axis], value, 0.0)


def add_fluxes(flux, lifts, store):
    for c in range(5):
        along = [[flux(axis, 5 * m + c) for m in range(5)] for axis in range(2)]
        for a in range(5):
            for b in range(5):
                store(25 * a + 5 * b + c, lifts[0][a] * along[0][b] + lifts[1][b] * along[1][a])


def local_kernel(sizes, count, chords, spans, *refs):
    state_hbm = refs[0]
    nu, acc = refs[1:3]
    state, around, tally = refs[5:8]
    grads = refs[8:11]
    faces = (refs[11:13], refs[13:15])
    ghosts = (refs[15:17], refs[3:5])
    load_sem, eps_sem, send_sem, state_sem, flux_sem, chord_sem, answer = refs[17:]
    rows, lanes = nu.shape[1:]
    chord_size, span_size = sizes
    me_c, me_s = lax.axis_index("chord"), lax.axis_index("span")
    mesh_id = pl.DeviceIdType.MESH

    def whole(ref):
        return ref.reshape(count, 25, rows, lanes)

    all_eps = around.reshape(3, 3, rows, lanes)

    def reachable(dx):
        if dx == 0:
            return None
        return me_c + 1 < chord_size if dx == 1 else me_c > 0

    def guarded(cond, run):
        if cond is None:
            run()
        else:
            pl.when(cond)(run)

    def partner(dx, dy):
        return (me_c + dx, lax.rem(me_s + dy + span_size, span_size))

    level = ((0, -1), (0, 1))
    lower, upper = (tuple((dx, dy) for dy in (0, -1, 1)) for dx in (-1, 1))

    def greet(sem, offsets):
        for dx, dy in offsets:
            pl.semaphore_signal(sem, inc=1, device_id=partner(dx, dy), device_id_type=mesh_id)

    barrier = pltpu.get_barrier_semaphore()
    def load(k, *part):
        return pltpu.make_async_copy(state_hbm.at[part], state.at[part], load_sem.at[k])

    start, remainder = load(0, 0, pl.ds(0, 75)), load(1, 0, pl.ds(75, 50))
    others = load(2, pl.ds(1, count - 1))
    for copy in (start, remainder, others):
        copy.start()

    greet(barrier, level)

    guarded(reachable(1), lambda: greet(barrier, upper))

    def edge_of(step, size):
        return pl.ds(0, size) if step == 0 else (size - 1 if step == 1 else 0)

    def eps_copy(dx, dy):
        part = (edge_of(dx, chords), edge_of(dy, spans))
        return pltpu.make_async_remote_copy(
            src_ref=around.at[(1, 1) + part], dst_ref=around.at[(1 - dx, 1 - dy) + part],
            send_sem=eps_sem.at[0], recv_sem=eps_sem.at[1 if dx == 0 else 2],
            device_id=partner(dx, dy), device_id_type=mesh_id,
        )

    def column_copy():
        return pltpu.make_async_remote_copy(
            src_ref=around.at[1, :, chords - 1], dst_ref=around.at[0, :, chords - 1],
            send_sem=eps_sem.at[0], recv_sem=eps_sem.at[2],
            device_id=partner(1, 0), device_id_type=mesh_id,
        )

    ways = ((1, 0), (-1, 0), (0, 1), (0, -1))

    def side(ref, axis, v, last, part):
        if axis == 0:
            return ref.at[v, part, chords - 1 if last else 0]
        return ref.at[v, part, :, spans - 1 if last else 0]

    def recv_sem(stage, axis, v):
        if stage == 0:
            return state_sem.at[axis, v]
        return chord_sem if axis == 0 else flux_sem.at[jnp.where(v < count - 1, 0, 1)]

    def send_eps(offsets):
        for dx, dy in offsets:
            eps_copy(dx, dy).start()

    def launch(stage, axis, v, sides=(0, 1), part=pl.ds(0, 25), only=None):
        for k in (2 * axis + i for i in sides):
            dx, dy = ways[k]
            up = k % 2 == 0

            def start():
                pltpu.make_async_remote_copy(
                    src_ref=side(faces[stage][axis], axis, v, up, part),
                    dst_ref=side(ghosts[stage][axis], axis, v, not up, part),
                    send_sem=send_sem.at[stage if axis == 0 else 2], recv_sem=recv_sem(stage, axis, v),
                    device_id=partner(dx, dy), device_id_type=mesh_id,
                ).start()

            allowed = reachable(dx) if only is None else only(partner(dx, dy)[1])
            guarded(allowed, start)

    def first_half(s):
        return s < span_size // 2

    def second_half(s):
        return s >= span_size // 2

    def by_one_link(s):
        return (s % 4 == 1) | (s % 4 == 2)

    two_sided = (me_c > 0) & (me_c + 1 < chord_size)

    def await_bytes(ref, sem):
        pltpu.make_async_copy(ref, ref, sem).wait()

    def await_chord(ref, part, sem):
        pl.when(two_sided)(lambda: await_bytes(ref.at[part, :, pl.ds(0, 2)], sem))
        pl.when(jnp.logical_not(two_sided))(lambda: await_bytes(ref.at[part, :, pl.ds(0, 1)], sem))

    def await_eps(sem, base, below, above):
        has_below, has_above = me_c > 0, me_c + 1 < chord_size
        for use_below in (False, True):
            for use_above in (False, True):
                size = base + use_below * below + use_above * above
                if size:
                    case = (has_below == use_below) & (has_above == use_above)
                    pl.when(case)(lambda size=size: await_bytes(tally.at[pl.ds(0, size)], sem))

    every = pl.ds(0, count)

    def all_sent(stage):
        await_chord(faces[stage][0], every, send_sem.at[stage])
        if stage == 1:
            await_bytes(state.at[:, pl.ds(0, 100 // spans)], send_sem.at[2])

    masks = [row_masks(axis, chords, spans, lanes) for axis in range(2)]

    def form_traces(axis, v, lines=range(5)):
        low = masks[axis][0]
        ends = [jnp.where(low, float(LEFT[i]), float(RIGHT[i])) for i in range(5)]
        out = whole(faces[0][axis])
        for q in lines:
            for j in range(5):
                pts = points(axis, q, j)
                out[v, 5 * q + j] = total_of([e * state[v, p] for e, p in zip(ends, pts)])

    with jax.named_scope("load0"):
        start.wait()
    form_traces(1, 0, range(3))
    with jax.named_scope("barrier"):
        pl.semaphore_wait(barrier, 2 + jnp.where(me_c > 0, 3, 0))
    launch(0, 1, 0, part=pl.ds(0, 15))
    guarded(reachable(-1), lambda: greet(answer, ((-1, 0),)))
    with jax.named_scope("sensor"):
        remainder.wait()
        eps = sensor(lambda p: state[0, p])
        all_eps[1, 1] = eps
    send_eps(level)
    guarded(reachable(-1), lambda: send_eps(lower))
    form_traces(1, 0, range(3, 5))
    launch(0, 1, 0, part=pl.ds(15, 10))
    with jax.named_scope("later"):
        def span_traces(v, carry):
            form_traces(1, v)
            early = v < count - held
            launch(0, 1, v, only=lambda s: jnp.logical_not(by_one_link(s)) | early)
            return carry

        held = min(HELD, count - 1)
        others.wait()
        lax.fori_loop(1, count, span_traces, 0)

        def chord_traces(v, carry):
            form_traces(0, v)
            launch(0, 0, v, (1,))
            return carry

        lax.fori_loop(0, count, chord_traces, 0)

    lane = lax.broadcasted_iota(jnp.int32, (rows, lanes), 1)
    first, last = lane == 0, lane == lanes - 1
    low_s, high_s = masks[1]
    low_c, high_c = masks[0]
    closed_low, closed_high = closed_rows(sizes[0], chords, spans, lanes)
    closed = closed_low | closed_high
    shut = jnp.where(closed, 1.0, 0.0)

    def normal_gradient(v, carry):
        grad = grads[2]
        for q in range(5):
            for j in range(5):
                pts = points(2, q, j)
                parts = fold([state[v, p] for p in pts])
                left, right = traces(parts)
                before = jnp.where(first, left, rolled(right, 1, 1))
                after = jnp.where(last, right, rolled(left, -1, 1))
                for p, value in zip(pts, slope(parts, before, after)):
                    grad[v, p] = value
        return carry

    def across_gradient(axis):
        low, high = masks[axis]
        step = spans if axis == 0 else 1
        mine, grad = whole(faces[0][axis]), grads[axis]

        def body(v, carry):
            for q in range(5):
                for j in range(5):
                    pts = points(axis, q, j)
                    parts = fold([state[v, p] for p in pts])
                    left, right = traces(parts)
                    beyond = shut * mine[v, 5 * q + j] if axis == 0 else 0.0
                    before = jnp.where(low, beyond, rolled(right, step, 0))
                    after = jnp.where(high, beyond, rolled(left, -step, 0))
                    for p, value in zip(pts, slope(parts, before, after)):
                        grad[v, p] = value
            return carry

        return body

    with jax.named_scope("ngrad"):
        lax.fori_loop(0, count, normal_gradient, 0)
    with jax.named_scope("sgrad"):
        lax.fori_loop(0, count, across_gradient(1), 0)

    with jax.named_scope("level"):
        await_bytes(tally.at[pl.ds(0, 2 * chords)], eps_sem.at[1])
    with jax.named_scope("answer"):

        @pl.when(reachable(1))
        def _():
            pl.semaphore_wait(answer, 1)
            column_copy().start()

        def chord_up(v, carry):
            launch(0, 0, v, (0,))
            return carry

        lax.fori_loop(0, count, chord_up, 0)

    def launch_held(v, carry):
        launch(0, 1, v, only=by_one_link)
        return carry

    lax.fori_loop(count - held, count, launch_held, 0)

    with jax.named_scope("cgrad"):
        lax.fori_loop(0, count, across_gradient(0), 0)

    with jax.named_scope("epswait"):
        await_eps(eps_sem.at[2], 0, 3 * spans, spans + 2)

    column = []
    for x in range(3):
        mine, left, right = all_eps[x, 1], all_eps[x, 0], all_eps[x, 2]
        column.append([
            jnp.where(low_s, rolled(left, 1 - spans, 0), rolled(mine, 1, 0)),
            mine,
            jnp.where(high_s, rolled(right, spans - 1, 0), rolled(mine, -1, 0)),
        ])
    neighbours = [[], [], []]
    for y in range(3):
        inner = column[1][y]
        below = jnp.where(low_c, rolled(column[0][y], spans, 0), rolled(inner, spans, 0))
        above = jnp.where(high_c, rolled(column[2][y], -spans, 0), rolled(inner, -spans, 0))
        neighbours[0].append(jnp.where(closed_low, 0.0, below))
        neighbours[1].append(inner)
        neighbours[2].append(jnp.where(closed_high, 0.0, above))
    interpolate(neighbours, nu)

    lifts, edges = boundary_lifts(masks, closed)

    def outside(ref, axis, v, f):
        return masked_edge(ref[v, f], axis, edges, spans)

    def across(axis, v):
        low, high = masks[axis]
        step = spans if axis == 0 else 1
        grad, ghost, out = grads[axis], whole(ghosts[0][axis]), whole(faces[1][axis])
        for q in range(5):
            for j in range(5):
                f = 5 * q + j
                pts = points(axis, q, j)
                beyond = outside(ghost, axis, v, f)
                gradient = [grad[v, p] + lift * beyond for p, lift in zip(pts, lifts[axis])]
                parts = fold([nu[p] * g for p, g in zip(pts, gradient)])
                left, right = traces(parts)
                ends = jnp.where(low, left, right)
                out[v, f] = ends
                beyond = -shut * ends if axis == 0 else 0.0
                before = jnp.where(low, beyond, rolled(right, step, 0))
                after = jnp.where(high, beyond, rolled(left, -step, 0))
                for p, value in zip(pts, slope(parts, before, after)):
                    if axis == 1:
                        acc[v, p] = value
                    else:
                        acc[v, p] += value

    def normal(v):
        for q in range(5):
            for j in range(5):
                pts = points(2, q, j)
                parts = fold([nu[p] * grads[2][v, p] for p in pts])
                left, right = traces(parts)
                before = jnp.where(first, -left, rolled(right, 1, 1))
                after = jnp.where(last, -right, rolled(left, -1, 1))
                for p, value in zip(pts, slope(parts, before, after)):
                    acc[v, p] += value

    lag = min(LAG, count)

    def variable(v, carry):
        with jax.named_scope("wait_u1"):
            await_bytes(ghosts[0][1].at[v, :, :, pl.ds(0, 2)], state_sem.at[1, v])
        with jax.named_scope("span"):
            across(1, v)
            launch(1, 1, v, only=first_half)
        with jax.named_scope("wait_u0"):
            await_chord(ghosts[0][0], v, state_sem.at[0, v])
        with jax.named_scope("chord"):
            across(0, v)
            launch(1, 0, v)
            due = v >= lag
            launch(1, 1, jnp.maximum(v - lag, 0), only=lambda s: second_half(s) & due)
        return carry

    with jax.named_scope("fluxes"):
        lax.fori_loop(0, count, variable, 0)

    def launch_rest(v, carry):
        launch(1, 1, v, only=second_half)
        return carry

    lax.fori_loop(count - lag, count, launch_rest, 0)

    def rest(v, carry):
        normal(v)
        return carry

    with jax.named_scope("normal"):
        lax.fori_loop(0, count, rest, 0)

    with jax.named_scope("sent0"):
        await_eps(eps_sem.at[0], 2 * chords, spans + 2, 3 * spans)
        all_sent(0)

    def correct(v, carry):
        add_fluxes(
            lambda axis, f: outside(whole(ghosts[1][axis]), axis, v, f), lifts,
            lambda p, value: acc.__setitem__((v, p), acc[v, p] + value),
        )
        return carry

    with jax.named_scope("wait_f0"):
        await_chord(ghosts[1][0], every, chord_sem)
    with jax.named_scope("correct"):
        await_bytes(
            ghosts[1][1].at[pl.ds(0, count - 1), :, :, pl.ds(0, 2)], flux_sem.at[0]
        )
        lax.fori_loop(0, count - 1, correct, 0)
        await_bytes(ghosts[1][1].at[count - 1, :, :, pl.ds(0, 2)], flux_sem.at[1])
    with jax.named_scope("sent1"):
        all_sent(1)


def finish_kernel(chord_size, acc, nu, flux_c, flux_s, residual_out, nu_out, last, sems):
    count, chords, spans, lanes = flux_c.shape[0], *flux_c.shape[2:]
    v = count - 1
    copies = (
        pltpu.make_async_copy(acc.at[pl.ds(0, v)], residual_out.at[pl.ds(0, v)], sems.at[0]),
        pltpu.make_async_copy(nu, nu_out, sems.at[1]),
        pltpu.make_async_copy(last, residual_out.at[v], sems.at[2]),
    )
    copies[0].start()
    copies[1].start()
    masks = [row_masks(axis, chords, spans, lanes) for axis in range(2)]
    closed_low, closed_high = closed_rows(chord_size, chords, spans, lanes)
    lifts, edges = boundary_lifts(masks, closed_low | closed_high)
    whole = [ref.reshape(count, 25, chords * spans, lanes) for ref in (flux_c, flux_s)]

    def store(p, value):
        last[p] = acc[v, p] + value

    add_fluxes(
        lambda axis, f: masked_edge(whole[axis][v, f], axis, edges, spans), lifts, store
    )
    copies[2].start()
    for copy in copies:
        copy.wait()


def shards(state):
    count, npts, chords, spans, lanes = state.shape
    rows = chords * spans
    flat = state.reshape(count, npts, rows, lanes)
    f32 = jnp.float32
    sizes = (lax.axis_size("chord"), lax.axis_size("span"))

    def full(*shape):
        return jax.ShapeDtypeStruct(shape, f32)

    vmem = pl.BlockSpec(memory_space=pltpu.VMEM)
    faces = (count, 25, chords, spans, lanes)
    nu, residual, flux_c, flux_s = pl.pallas_call(
        functools.partial(local_kernel, sizes, count, chords, spans),
        in_specs=[pl.BlockSpec(memory_space=pltpu.HBM)],
        out_specs=[vmem] * 4,
        out_shape=[
            full(npts, rows, lanes), full(count, npts, rows, lanes), full(*faces), full(*faces)
        ],
        scratch_shapes=[
            pltpu.VMEM(shape, f32)
            for shape in [
                (count, npts, rows, lanes),
                (3, 3, chords, spans, lanes),
                (2 * chords + 4 * spans + 2, 1, lanes),
                (count, npts, rows, lanes),
                (count, npts, rows, lanes),
                (count, npts, rows, lanes),
            ]
            + [faces] * 6
        ]
        + [
            pltpu.SemaphoreType.DMA((3,)),
            pltpu.SemaphoreType.DMA((3,)),
            pltpu.SemaphoreType.DMA((3,)),
            pltpu.SemaphoreType.DMA((2, count)),
            pltpu.SemaphoreType.DMA((2,)),
            pltpu.SemaphoreType.DMA,
            pltpu.SemaphoreType.REGULAR,
        ],
        compiler_params=pltpu.CompilerParams(
            collective_id=0, has_side_effects=True, vmem_limit_bytes=VMEM_BYTES
        ),
    )(flat)
    hbm = pl.BlockSpec(memory_space=pltpu.HBM)
    residual, nu = pl.pallas_call(
        functools.partial(finish_kernel, sizes[0]),
        in_specs=[vmem] * 4,
        out_specs=[hbm, hbm],
        out_shape=[full(count, npts, rows, lanes), full(npts, rows, lanes)],
        scratch_shapes=[pltpu.VMEM((npts, rows, lanes), f32), pltpu.SemaphoreType.DMA((3,))],
        compiler_params=pltpu.CompilerParams(vmem_limit_bytes=FINISH_BYTES),
    )(residual, nu, flux_c, flux_s)
    return residual.reshape(state.shape), nu.reshape(npts, chords, spans, lanes)


def solution(mesh):
    in_specs = (P(None, None, "chord", "span", None),)
    out_specs = (P(None, None, "chord", "span", None), P(None, "chord", "span", None))
    return jax.shard_map(shards, mesh=mesh, in_specs=in_specs, out_specs=out_specs, check_vma=False)
```
